16 devices in a mesh: tp: 2 (over z), dp: 8 (over y, x, core).
Axes of the slice: x: 2, y: 2, z: 2, core: 2. Of those that a mesh axis runs over, the one named last changes fastest.
Arguments:
- tokens: int32 [128, 512], P('dp')
- cotangent: bfloat16 [128, 512, 768], P('dp')
- emb_table: bfloat16 [30592, 768], P('tp')
- w_qkv: bfloat16 [768, 2304], P(None, 'tp')
- b_qkv: bfloat16 [12, 192], P('tp')
- w_out: bfloat16 [768, 768], P('tp')
- b_out: bfloat16 [768], replicated
- ln1_gain: bfloat16 [768], replicated
- ln1_bias: bfloat16 [768], replicated
- w_gate: bfloat16 [768, 3072], P(None, 'tp')
- b_gate: bfloat16 [3072], P('tp')
- w_lin: bfloat16 [768, 3072], P(None, 'tp')
- b_lin: bfloat16 [3072], P('tp')
- w_down: bfloat16 [3072, 768], P('tp')
- b_down: bfloat16 [768], replicated
- ln2_gain: bfloat16 [768], replicated
Outputs:
- output 1: float32 [30592, 768], P('tp')
- output 2: float32 [768, 2304], P(None, 'tp')
- output 3: float32 [12, 192], P('tp')
- output 4: float32 [768, 768], P('tp')
- output 5: float32 [768], replicated
- output 6: float32 [768], replicated
- output 7: float32 [768], replicated
- output 8: float32 [768, 3072], P(None, 'tp')
- output 9: float32 [3072], P('tp')
- output 10: float32 [768, 3072], P(None, 'tp')
- output 11: float32 [3072], P('tp')
- output 12: float32 [3072, 768], P('tp')
- output 13: float32 [768], replicated
- output 14: float32 [768], replicated
All inputs are finite; a program needn't handle non-finite values.
Results may differ from the reference program's by a relative error of at most 0.0151514.
Values sent between devices are 32-bit elements.
A program may use at most 1 GiB of HBM per device.

```python
import jax
import jax.numpy as jnp
from jax import lax

VOCAB_SIZE = 30592
D_MODEL = 768
NUM_HEADS = 12
FFN_DIM = 3072
GLOBAL_BATCH = 128
SEQ_LEN = 512
HEAD_DIM = D_MODEL // NUM_HEADS
ALPHA = 140.0 ** 0.5
EPS = 1e-5
SHRINK = 0.1
ROPE_BASE = 10000.0


def setup_inputs(seed: int = 0) -> dict:
    root_key = jax.random.key(seed)
    key_list = jax.random.split(root_key, 16)
    id_keys = jax.random.split(key_list[0], 2)
    first_ids = jax.random.randint(id_keys[0], (GLOBAL_BATCH, SEQ_LEN), 0, VOCAB_SIZE, dtype=jnp.int32)
    second_ids = jax.random.randint(id_keys[1], (GLOBAL_BATCH, SEQ_LEN), 0, VOCAB_SIZE, dtype=jnp.int32)
    tokens = jnp.minimum(first_ids, second_ids)
    tokens = tokens.at[0, 0].set(0).at[0, SEQ_LEN - 1].set(VOCAB_SIZE - 1)

    def draw(index, shape, scale, offset):
        return (jax.random.normal(key_list[index], shape, jnp.float32) * scale + offset).astype(jnp.bfloat16)

    return {
        'tokens': tokens,
        'cotangent': draw(1, (GLOBAL_BATCH, SEQ_LEN, D_MODEL), 1.0, 0.0),
        'emb_table': draw(2, (VOCAB_SIZE, D_MODEL), 1.0, 0.0),
        'w_qkv': draw(3, (D_MODEL, 3 * D_MODEL), D_MODEL ** -0.5, 0.0),
        'b_qkv': draw(4, (NUM_HEADS, 3 * HEAD_DIM), 0.3, 0.0),
        'w_out': draw(5, (D_MODEL, D_MODEL), ALPHA * D_MODEL ** -0.5, 0.0),
        'b_out': draw(6, (D_MODEL,), 1.0, 0.0),
        'ln1_gain': draw(7, (D_MODEL,), 0.3, 1.0),
        'ln1_bias': draw(8, (D_MODEL,), 0.3, 0.0),
        'w_gate': draw(9, (D_MODEL, FFN_DIM), D_MODEL ** -0.5, 0.0),
        'b_gate': draw(10, (FFN_DIM,), 0.3, 0.0),
        'w_lin': draw(11, (D_MODEL, FFN_DIM), D_MODEL ** -0.5, 0.0),
        'b_lin': draw(12, (FFN_DIM,), 0.3, 0.0),
        'w_down': draw(13, (FFN_DIM, D_MODEL), ALPHA * FFN_DIM ** -0.5, 0.0),
        'b_down': draw(14, (D_MODEL,), 2.0, 0.0),
        'ln2_gain': draw(15, (D_MODEL,), 0.3, 1.0),
    }


def to_bf16(values):
    return values.astype(jnp.bfloat16).astype(jnp.float32)


def norm_scaled(values, gain):
    mean_val = jnp.mean(values, axis=-1, keepdims=True)
    centered = values - mean_val
    variance = jnp.mean(centered * centered, axis=-1, keepdims=True)
    return centered * lax.rsqrt(variance + EPS) * gain


def rope_tables():
    half_dim = HEAD_DIM // 2
    inv_freq = ROPE_BASE ** (-2.0 * jnp.arange(half_dim, dtype=jnp.float32) / HEAD_DIM)
    angles = jnp.arange(SEQ_LEN, dtype=jnp.float32)[:, None] * inv_freq[None, :]
    return jnp.cos(angles)[:, None, :], jnp.sin(angles)[:, None, :]


def apply_rope(values, cos_tab, sin_tab):
    half_dim = values.shape[-1] // 2
    first_half = values[..., :half_dim]
    second_half = values[..., half_dim:]
    return jnp.concatenate([first_half * cos_tab - second_half * sin_tab, second_half * cos_tab + first_half * sin_tab], axis=-1)


def seq_loss(params, emb_rows, seq_cot):
    (w_qkv, b_qkv, w_out, b_out, ln1_gain, ln1_bias, w_gate, b_gate, w_lin, b_lin, w_down, b_down, ln2_gain) = params
    embedded = SHRINK * emb_rows + (1.0 - SHRINK) * lax.stop_gradient(emb_rows)
    qkv_pre = jnp.dot(embedded, w_qkv, preferred_element_type=jnp.float32) + b_qkv.reshape(-1)
    qkv_all = to_bf16(qkv_pre).reshape(SEQ_LEN, NUM_HEADS, 3, HEAD_DIM)
    cos_tab, sin_tab = rope_tables()
    queries = to_bf16(apply_rope(qkv_all[:, :, 0], cos_tab, sin_tab))
    keys_rot = to_bf16(apply_rope(qkv_all[:, :, 1], cos_tab, sin_tab))
    values = qkv_all[:, :, 2]
    scores = jnp.einsum('qhd,khd->hqk', queries, keys_rot) * HEAD_DIM ** -0.5
    causal = jnp.arange(SEQ_LEN)[:, None] >= jnp.arange(SEQ_LEN)[None, :]
    attn_probs = to_bf16(jax.nn.softmax(jnp.where(causal, scores, -1e30), axis=-1))
    context = to_bf16(jnp.einsum('hqk,khd->qhd', attn_probs, values)).reshape(SEQ_LEN, D_MODEL)
    attn_out = jnp.dot(context, w_out, preferred_element_type=jnp.float32) + b_out
    hidden = to_bf16(norm_scaled(ALPHA * embedded + attn_out, ln1_gain) + ln1_bias)
    gate_pre = jnp.dot(hidden, w_gate, preferred_element_type=jnp.float32) + b_gate
    lin_pre = jnp.dot(hidden, w_lin, preferred_element_type=jnp.float32) + b_lin
    inner_act = to_bf16(jax.nn.gelu(gate_pre, approximate=False) * lin_pre)
    ffn_out = jnp.dot(inner_act, w_down, preferred_element_type=jnp.float32) + b_down
    final_out = norm_scaled(ALPHA * hidden + ffn_out, ln2_gain)
    return jnp.sum(final_out * seq_cot)


def reference(tokens, cotangent, emb_table, w_qkv, b_qkv, w_out, b_out, ln1_gain, ln1_bias, w_gate, b_gate, w_lin, b_lin, w_down, b_down, ln2_gain):
    params = tuple(weight.astype(jnp.float32) for weight in (w_qkv, b_qkv, w_out, b_out, ln1_gain, ln1_bias, w_gate, b_gate, w_lin, b_lin, w_down, b_down, ln2_gain))

    def one_sequence(grad_acc, seq_item):
        seq_tokens, seq_cot = seq_item
        emb_rows = jnp.take(emb_table, seq_tokens, axis=0).astype(jnp.float32)

        def loss_of(prm_all, rows_in):
            return seq_loss(prm_all, rows_in, seq_cot.astype(jnp.float32))

        pull_back = jax.vjp(loss_of, params, emb_rows)[1]
        grad_params, grad_rows = pull_back(jnp.ones((), jnp.float32))
        new_acc = jax.tree.map(lambda acc_val, new_val: acc_val + new_val, grad_acc, grad_params)
        return new_acc, grad_rows

    init_acc = jax.tree.map(lambda prm_item: prm_item * 0.0, params)
    grad_params, grad_rows = lax.scan(one_sequence, init_acc, (tokens, cotangent))
    d_table = jax.ops.segment_sum(grad_rows.reshape(-1, D_MODEL), tokens.reshape(-1), num_segments=VOCAB_SIZE)
    (d_w_qkv, d_b_qkv, d_w_out, d_b_out, d_ln1_gain, d_ln1_bias, d_w_gate, d_b_gate, d_w_lin, d_b_lin, d_w_down, d_b_down, d_ln2_gain) = grad_params
    return (d_table, d_w_qkv, d_b_qkv, d_w_out, d_b_out, d_ln1_gain, d_ln1_bias, d_w_gate, d_b_gate, d_w_lin, d_b_lin, d_w_down, d_b_down, d_ln2_gain)
```

```python
import functools

import jax
import jax.numpy as jnp
from jax import lax
from jax.experimental import pallas as pl
from jax.experimental.pallas import tpu as pltpu
from jax.sharding import PartitionSpec as P

ALPHA = 140.0 ** 0.5
EPS = 1e-5
SHRINK = 0.1
ROPE_BASE = 10000.0
WEIGHT_SPECS = (P(None, 'tp'), P('tp', None), P('tp', None), P(), P(), P(), P(None, 'tp'), P('tp'), P(None, 'tp'), P('tp'), P('tp', None), P(), P())

F32 = jnp.float32
BF16 = jnp.bfloat16
LANES = 128
HALF_Q = 256
CHUNK = 512
VMEM_LIMIT = 66 * 1024 * 1024 - 512 * 1024
LOG2E = 1.4426950408889634
MASKED = -8e30
NT = (((1,), (1,)), ((), ()))
NN = (((1,), (0,)), ((), ()))
SWAP = ((0, 1), (1, 0))


def dot_nn(left, right):
    return lax.dot_general(left, right, NN, preferred_element_type=F32)


def dot_nt(left, right):
    return lax.dot_general(left, right, NT, preferred_element_type=F32)


def row_sums(values):
    return jnp.sum(values.reshape(values.shape[0] // 8, 8, values.shape[1]), axis=0)


def rope(values, cos_tab, sin_tab, first_half):
    partner = jnp.where(first_half, pltpu.roll(values, 96, 1), pltpu.roll(values, 32, 1))
    return values * cos_tab + partner * sin_tab


def lane_masks():
    lane = lax.broadcasted_iota(jnp.int32, (1, LANES), 1)
    low = lane < 64
    return low, low.astype(F32).astype(BF16), (1.0 - low.astype(F32)).astype(BF16), (lane % 64) < 32


def attn_forward_kernel(head_dim, alias_count, *refs):
    (emb_ref, wqkv_ref, bqkv_ref, wo_ref, bo_ref, gain_ref, bias_ref, cos_ref, sin_ref) = refs[:9]
    (qkv_ref, prob_ref, ctx_ref, hat_ref, rstd_ref, hid_ref) = refs[9 + alias_count:]
    seq_len, width = emb_ref.shape[1], emb_ref.shape[2]
    low, mask_low, mask_high, first_half = lane_masks()
    score_scale = head_dim ** -0.5 * LOG2E
    causal = lax.broadcasted_iota(jnp.int32, (HALF_Q, HALF_Q), 0) <= lax.broadcasted_iota(jnp.int32, (HALF_Q, HALF_Q), 1)
    step = 4 * 3 * head_dim

    def quad(index, carry):
        col = pl.multiple_of(index * step, step)
        pre = dot_nn(emb_ref[0], wqkv_ref[:, pl.ds(col, step)]) + bqkv_ref[:, pl.ds(col, step)]
        pre = pre.astype(BF16).astype(F32)
        for half in range(2):
            parts = [pre[:, (half * 3 + part) * LANES:(half * 3 + part + 1) * LANES] for part in range(3)]
            pair = index * 2 + half
            pair_col = pl.multiple_of(pair * LANES, LANES)
            q_pair = jnp.where(low, parts[0], parts[1])
            k_pair = pltpu.roll(jnp.where(low, parts[2], parts[0]), 64, 1)
            v_pair = jnp.where(low, parts[1], parts[2])
            q_rot = rope(q_pair, cos_ref[...], sin_ref[...], first_half).astype(BF16)
            k_rot = rope(k_pair, cos_ref[...], sin_ref[...], first_half).astype(BF16)
            qkv_ref[0, :, pl.ds(pair_col, LANES)] = q_rot
            qkv_ref[0, :, pl.ds(width + pair_col, LANES)] = k_rot
            qkv_ref[0, :, pl.ds(2 * width + pair_col, LANES)] = v_pair.astype(BF16)
            v_trans = v_pair.T.astype(BF16)
            ctx_rows = []
            for head in range(2):
                k_one = k_rot * (mask_low if head == 0 else mask_high)
                v_one = v_trans[head * 64:(head + 1) * 64]
                blocks = []
                for block in range(2):
                    q_block = q_rot[block * HALF_Q:(block + 1) * HALF_Q]
                    diag = jnp.where(causal, dot_nt(k_one[block * HALF_Q:(block + 1) * HALF_Q], q_block), MASKED)
                    pieces = [diag] if block == 0 else [dot_nt(k_one[:HALF_Q], q_block), diag]
                    peak = functools.reduce(jnp.maximum, [jnp.max(piece, axis=0, keepdims=True) for piece in pieces])
                    exps = [jnp.exp2((piece - peak) * score_scale) for piece in pieces]
                    total = functools.reduce(jnp.add, [jnp.sum(piece, axis=0, keepdims=True) for piece in exps])
                    inverse = 1.0 / total
                    ctx = None
                    for num, piece in enumerate(exps):
                        prob = (piece * inverse).astype(BF16)
                        prob_ref[0, pair * 2 + head, (block + num) * HALF_Q:(block + num + 1) * HALF_Q, :] = prob
                        term = dot_nn(v_one[:, num * HALF_Q:(num + 1) * HALF_Q], prob)
                        ctx = term if ctx is None else ctx + term
                    blocks.append(ctx)
                ctx_rows.append(jnp.concatenate(blocks, axis=1))
            ctx_pair = jnp.concatenate(ctx_rows, axis=0)
            ctx_ref[0, :, pl.ds(pair_col, LANES)] = ctx_pair.T.astype(BF16)
        return carry

    lax.fori_loop(0, wqkv_ref.shape[1] // step, quad, 0)
    attn = dot_nn(ctx_ref[0], wo_ref[...]) + bo_ref[...]
    resid = ALPHA * emb_ref[0].astype(F32) + attn
    centered = resid - jnp.mean(resid, axis=-1, keepdims=True)
    variance = jnp.mean(centered * centered, axis=-1, keepdims=True)
    rstd = lax.rsqrt(variance + EPS)
    hat = centered * rstd
    hat_ref[0] = hat
    rstd_ref[0] = jnp.broadcast_to(rstd, (seq_len, LANES))
    hid_ref[0] = (hat * gain_ref[...] + bias_ref[...]).astype(BF16)


def ffn_kernel(hid_ref, cot_ref, hat_ref, rstd_ref, wg_ref, wl_ref, wd_ref, bg_ref, bl_ref, bd_ref, gain1_ref, gain2_ref,
               inner_out, gate_out, lin_out, dffn_ref, dres_ref, narrow_ref, wide_ref,
               act_buf, slope_buf, inner_buf, gate_buf, lin_buf, acc_buf, sems):
    step = pl.program_id(0)
    last = pl.num_programs(0) - 1
    rows, width = hid_ref.shape[1], hid_ref.shape[2]
    chunks = wg_ref.shape[1] // CHUNK

    def copy_out(buf, out, kind, chunk, block):
        cols = pl.ds(pl.multiple_of(chunk * CHUNK, CHUNK), CHUNK)
        return pltpu.make_async_copy(buf.at[:, cols], out.at[pl.ds(block * rows, rows), cols], sems.at[kind, chunk])

    @pl.when(step == 0)
    def _():
        narrow_ref[...] = jnp.zeros_like(narrow_ref)
        wide_ref[...] = jnp.zeros_like(wide_ref)

    acc_buf[...] = jnp.zeros_like(acc_buf)

    def forward(chunk, carry):
        cols = pl.ds(pl.multiple_of(chunk * CHUNK, CHUNK), CHUNK)
        gate_pre = dot_nn(hid_ref[0], wg_ref[:, cols]) + bg_ref[:, cols]
        lin_pre = dot_nn(hid_ref[0], wl_ref[:, cols]) + bl_ref[:, cols]
        cdf = 0.5 + 0.5 * lax.erf(gate_pre * (0.5 ** 0.5))
        act = gate_pre * cdf
        pdf = jnp.exp2(gate_pre * gate_pre * (-0.5 * LOG2E)) * 0.3989422804014327
        act_buf[:, cols] = act
        slope_buf[:, cols] = lin_pre * (cdf + gate_pre * pdf)

        @pl.when(step > 0)
        def _():
            copy_out(inner_buf, inner_out, 0, chunk, step - 1).wait()

        inner = (act * lin_pre).astype(BF16)
        inner_buf[:, cols] = inner
        acc_buf[...] += dot_nn(inner, wd_ref[cols, :])
        copy_out(inner_buf, inner_out, 0, chunk, step).start()
        return carry

    lax.fori_loop(0, chunks, forward, 0)
    resid = ALPHA * hid_ref[0].astype(F32) + (acc_buf[...] + bd_ref[...])
    centered = resid - jnp.mean(resid, axis=-1, keepdims=True)
    variance = jnp.mean(centered * centered, axis=-1, keepdims=True)
    rstd = lax.rsqrt(variance + EPS)
    hat = centered * rstd
    cot = cot_ref[0].astype(F32)
    narrow_ref[0:8] += row_sums(cot * hat)
    d_hat = cot * gain2_ref[...]
    d_resid = rstd * (d_hat - jnp.mean(d_hat, axis=-1, keepdims=True) - hat * jnp.mean(d_hat * hat, axis=-1, keepdims=True))
    narrow_ref[8:16] += row_sums(d_resid)
    dffn_ref[0] = d_resid.astype(BF16)
    acc_buf[...] = ALPHA * d_resid

    def backward(chunk, carry):
        cols = pl.ds(pl.multiple_of(chunk * CHUNK, CHUNK), CHUNK)
        d_inner = dot_nt(dffn_ref[0], wd_ref[cols, :]).astype(BF16).astype(F32)
        d_gate = d_inner * slope_buf[:, cols]
        d_lin = d_inner * act_buf[:, cols]
        wide_ref[0:8, cols] += row_sums(d_gate)
        wide_ref[8:16, cols] += row_sums(d_lin)

        @pl.when(step > 0)
        def _():
            copy_out(gate_buf, gate_out, 1, chunk, step - 1).wait()
            copy_out(lin_buf, lin_out, 2, chunk, step - 1).wait()

        d_gate = d_gate.astype(BF16)
        d_lin = d_lin.astype(BF16)
        gate_buf[:, cols] = d_gate
        lin_buf[:, cols] = d_lin
        acc_buf[...] += dot_nt(d_gate, wg_ref[:, cols]) + dot_nt(d_lin, wl_ref[:, cols])
        copy_out(gate_buf, gate_out, 1, chunk, step).start()
        copy_out(lin_buf, lin_out, 2, chunk, step).start()
        return carry

    lax.fori_loop(0, chunks, backward, 0)
    d_hid = acc_buf[...]
    hat = hat_ref[0]
    narrow_ref[16:24] += row_sums(d_hid)
    narrow_ref[24:32] += row_sums(d_hid * hat)
    d_hat = d_hid * gain1_ref[...]
    d_resid = rstd_ref[0][:, :1] * (d_hat - jnp.mean(d_hat, axis=-1, keepdims=True) - hat * jnp.mean(d_hat * hat, axis=-1, keepdims=True))
    narrow_ref[32:40] += row_sums(d_resid)
    dres_ref[0] = d_resid

    @pl.when(step == last)
    def _():
        def drain(chunk, carry):
            copy_out(inner_buf, inner_out, 0, chunk, step).wait()
            copy_out(gate_buf, gate_out, 1, chunk, step).wait()
            copy_out(lin_buf, lin_out, 2, chunk, step).wait()
            return carry

        lax.fori_loop(0, chunks, drain, 0)


def attn_backward_kernel(head_dim, alias_count, *refs):
    (dres_ref, qkv_ref, prob_ref, wqkv_ref, wo_ref, cos_ref, sin_ref) = refs[:7]
    (demb_ref, dqkv_ref, acc_ref) = refs[7 + alias_count:]
    width = dres_ref.shape[2]
    low, mask_low, mask_high, first_half = lane_masks()
    attn_scale = head_dim ** -0.5
    step = 4 * 3 * head_dim

    @pl.when(pl.program_id(0) == 0)
    def _():
        acc_ref[...] = jnp.zeros_like(acc_ref)

    d_attn = dres_ref[0].astype(BF16)

    def quad(index, carry):
        col = pl.multiple_of(index * step, step)
        ctx_row = pl.multiple_of(index * 4 * head_dim, 4 * head_dim)
        d_ctx_quad = dot_nt(d_attn, wo_ref[pl.ds(ctx_row, 4 * head_dim), :]).astype(BF16)
        pieces = []
        for half in range(2):
            pair = index * 2 + half
            pair_col = pl.multiple_of(pair * LANES, LANES)
            d_ctx = d_ctx_quad[:, half * LANES:(half + 1) * LANES]
            q_rot = qkv_ref[0, :, pl.ds(pair_col, LANES)]
            k_rot = qkv_ref[0, :, pl.ds(width + pair_col, LANES)]
            v_pair = qkv_ref[0, :, pl.ds(2 * width + pair_col, LANES)]
            k_trans = k_rot.astype(F32).T.astype(BF16)
            dq_rows, dk_heads, dv_heads = [], [], []
            for head in range(2):
                v_one = v_pair * (mask_low if head == 0 else mask_high)
                k_one = k_trans[head * 64:(head + 1) * 64]
                d_v, d_k, d_q = [None, None], [None, None], []
                for block in range(2):
                    rows = slice(block * HALF_Q, (block + 1) * HALF_Q)
                    keys = range(block + 1)
                    probs = [prob_ref[0, pair * 2 + head, (block + num) * HALF_Q:(block + num + 1) * HALF_Q, :] for num in keys]
                    d_probs = [dot_nt(v_one[num * HALF_Q:(num + 1) * HALF_Q], d_ctx[rows]) for num in keys]
                    wide = [prob.astype(F32) for prob in probs]
                    inner = functools.reduce(jnp.add, [jnp.sum(d_prob * prob, axis=0, keepdims=True) for d_prob, prob in zip(d_probs, wide)])
                    d_q_block = None
                    for num in keys:
                        d_score = (wide[num] * (d_probs[num] - inner) * attn_scale).astype(BF16)
                        terms = (dot_nn(probs[num], d_ctx[rows]), dot_nn(d_score, q_rot[rows]), dot_nn(k_one[:, num * HALF_Q:(num + 1) * HALF_Q], d_score))
                        d_v[num] = terms[0] if d_v[num] is None else d_v[num] + terms[0]
                        d_k[num] = terms[1] if d_k[num] is None else d_k[num] + terms[1]
                        d_q_block = terms[2] if d_q_block is None else d_q_block + terms[2]
                    d_q.append(d_q_block)
                dq_rows.append(jnp.concatenate(d_q, axis=1))
                dk_heads.append(jnp.concatenate(d_k, axis=0))
                dv_heads.append(jnp.concatenate(d_v, axis=0))
            d_q = rope(jnp.concatenate(dq_rows, axis=0).T, cos_ref[...], -sin_ref[...], first_half)
            d_k = rope(jnp.where(low, dk_heads[0], dk_heads[1]), cos_ref[...], -sin_ref[...], first_half)
            d_v = jnp.where(low, dv_heads[0], dv_heads[1])
            d_k = pltpu.roll(d_k, 64, 1)
            pieces += [jnp.where(low, d_q, d_k), jnp.where(low, d_v, d_q), jnp.where(low, d_k, d_v)]
        for num, piece in enumerate(pieces):
            lanes = pl.ds(col + num * LANES, LANES)
            acc_ref[:, lanes] += row_sums(piece)
            dqkv_ref[0, :, lanes] = piece.astype(BF16)
        return carry

    lax.fori_loop(0, wqkv_ref.shape[1] // step, quad, 0)
    demb_ref[0] = SHRINK * (ALPHA * dres_ref[0] + dot_nt(dqkv_ref[0], wqkv_ref[...]))


def whole(shape):
    return pl.BlockSpec(shape, lambda i: (0,) * len(shape), pipeline_mode=pl.Buffered(1))


def per_seq(shape, base=0):
    return pl.BlockSpec((1,) + tuple(shape), lambda i: (i + base,) + (0,) * len(shape))


def params():
    return pltpu.CompilerParams(dimension_semantics=('arbitrary',), vmem_limit_bytes=VMEM_LIMIT)


def attn_forward(base, total, emb, weights, tables, previous, head_dim):
    count, seq_len, width = emb.shape
    wqkv = weights[0]
    heads = width // head_dim
    shapes = [((seq_len, 3 * width), BF16), ((heads, seq_len * 3 // 2, HALF_Q), BF16), ((seq_len, width), BF16),
              ((seq_len, width), F32), ((seq_len, LANES), F32), ((seq_len, width), BF16)]
    operands = (emb,) + tuple(weights) + tuple(tables)
    specs = [per_seq((seq_len, width))] + [whole(item.shape) for item in operands[1:]]
    extra = tuple(previous) if previous is not None else ()
    specs += [pl.BlockSpec(memory_space=pl.ANY)] * len(extra)
    flops = count * (2 * seq_len * width * (wqkv.shape[1] + width) + 4 * heads * seq_len * seq_len * 64)
    return pl.pallas_call(
        functools.partial(attn_forward_kernel, head_dim, len(extra)),
        grid=(count,),
        in_specs=specs,
        out_specs=[per_seq(shape, base) for shape, _ in shapes],
        out_shape=[jax.ShapeDtypeStruct((total,) + shape, dtype) for shape, dtype in shapes],
        input_output_aliases={len(operands) + num: num for num in range(len(extra))},
        compiler_params=params(),
        cost_estimate=pl.CostEstimate(flops=2 * flops, bytes_accessed=count * 12_000_000, transcendentals=0),
        name='attn_forward',
    )(*operands, *extra)


def ffn(hidden, cotangent, hat, rstd, weights):
    count, seq_len, width = hidden.shape
    wide = weights[0].shape[1]
    rows = count * seq_len
    operands = (hidden, cotangent, hat, rstd) + tuple(weights)
    specs = [per_seq(item.shape[1:]) for item in operands[:4]] + [whole(item.shape) for item in operands[4:]]
    anywhere = pl.BlockSpec(memory_space=pl.ANY)
    big = jax.ShapeDtypeStruct((rows, wide), BF16)
    flops = 12 * rows * width * wide
    return pl.pallas_call(
        ffn_kernel,
        grid=(count,),
        in_specs=specs,
        out_specs=[anywhere] * 3 + [per_seq((seq_len, width))] * 2 + [pl.BlockSpec((40, width), lambda i: (0, 0)), pl.BlockSpec((16, wide), lambda i: (0, 0))],
        out_shape=[big] * 3 + [jax.ShapeDtypeStruct((count, seq_len, width), BF16), jax.ShapeDtypeStruct((count, seq_len, width), F32),
                               jax.ShapeDtypeStruct((40, width), F32), jax.ShapeDtypeStruct((16, wide), F32)],
        scratch_shapes=[pltpu.VMEM((seq_len, wide), F32)] * 2 + [pltpu.VMEM((seq_len, wide), BF16)] * 3
        + [pltpu.VMEM((seq_len, width), F32), pltpu.SemaphoreType.DMA((3, wide // CHUNK))],
        compiler_params=params(),
        cost_estimate=pl.CostEstimate(flops=int(1.5 * flops), bytes_accessed=count * 14_000_000, transcendentals=0),
        name='ffn',
    )(*operands)


def attn_backward(base, count, total, d_resid, qkv, probs, weights, tables, previous, head_dim):
    seq_len, width = d_resid.shape[1:]
    wqkv, wout = weights
    heads = width // head_dim
    operands = (d_resid, qkv, probs, wqkv, wout) + tuple(tables)
    specs = [per_seq(item.shape[1:], base) for item in operands[:3]] + [whole(item.shape) for item in operands[3:]]
    extra = (previous,) if previous is not None else ()
    specs += [pl.BlockSpec(memory_space=pl.ANY)] * len(extra)
    flops = count * (2 * seq_len * width * (wqkv.shape[1] + width) + 8 * heads * seq_len * seq_len * 64)
    return pl.pallas_call(
        functools.partial(attn_backward_kernel, head_dim, len(extra)),
        grid=(count,),
        in_specs=specs,
        out_specs=[per_seq((seq_len, width)), per_seq((seq_len, wqkv.shape[1]), base), pl.BlockSpec((8, wqkv.shape[1]), lambda i: (0, 0))],
        out_shape=[jax.ShapeDtypeStruct((count, seq_len, width), F32), jax.ShapeDtypeStruct((total, seq_len, wqkv.shape[1]), BF16),
                   jax.ShapeDtypeStruct((8, wqkv.shape[1]), F32)],
        input_output_aliases={len(operands): 1} if extra else {},
        compiler_params=params(),
        cost_estimate=pl.CostEstimate(flops=2 * flops, bytes_accessed=count * 12_000_000, transcendentals=0),
        name='attn_backward',
    )(*operands, *extra)


def groups_of(total, size):
    return [(base, min(size, total - base)) for base in range(0, total, size)]


def join_kernel(axis, blocks, own_ref, peer_ref, out_ref):
    if axis == 1:
        split = own_ref.shape[1]
        out_ref[:, :split] = own_ref[...]
        out_ref[:, split:] = peer_ref[...].astype(BF16)
    else:
        @pl.when(pl.program_id(0) < blocks)
        def _():
            out_ref[...] = own_ref[...]

        @pl.when(pl.program_id(0) >= blocks)
        def _():
            out_ref[...] = peer_ref[...].astype(BF16)


def with_peer_half(own, axis, index, parts):
    rows = own.shape[0] // parts
    piece = lax.dynamic_slice_in_dim(own, index * rows, rows, 0).astype(F32)
    piece = lax.ppermute(piece, 'tp', SWAP)
    peer = lax.all_gather(piece, 'dp', axis=0, tiled=True)
    blocks = 4
    shape = (own.shape[0] // blocks, own.shape[1])
    if axis == 1:
        grid, out_block, out_shape = (blocks,), (shape[0], 2 * shape[1]), (own.shape[0], 2 * own.shape[1])
        own_map = peer_map = lambda i: (i, 0)
    else:
        grid, out_block, out_shape = (2 * blocks,), shape, (2 * own.shape[0], own.shape[1])
        own_map, peer_map = (lambda i: (jnp.minimum(i, blocks - 1), 0)), (lambda i: (jnp.maximum(i - blocks, 0), 0))
    return pl.pallas_call(
        functools.partial(join_kernel, axis, blocks),
        grid=grid,
        in_specs=[pl.BlockSpec(shape, own_map), pl.BlockSpec(shape, peer_map)],
        out_specs=pl.BlockSpec(out_block, lambda i: (i, 0)),
        out_shape=jax.ShapeDtypeStruct(out_shape, BF16),
        compiler_params=params(),
        cost_estimate=pl.CostEstimate(flops=own.size * 64, bytes_accessed=own.size * 10, transcendentals=0),
        name='join_weight',
    )(own, peer)


def reduce_weight(grad, parts):
    piece = lax.psum_scatter(grad, 'dp', scatter_dimension=1, tiled=True)
    mine = piece[0] + lax.ppermute(piece[1], 'tp', SWAP)
    return lax.all_gather(mine, 'dp', axis=0, tiled=True)


def solution(mesh):
    in_specs = (P('dp', None), P('dp', None, None), P('tp', None)) + WEIGHT_SPECS
    out_specs = (P('tp', None),) + WEIGHT_SPECS
    parts = mesh.shape['dp']

    def device_step(tokens, cotangent, emb_table, *weights):
        (w_qkv, b_qkv, w_out, b_out, ln1_gain, ln1_bias, w_gate, b_gate, w_lin, b_lin, w_down, b_down, ln2_gain) = weights
        tp_index, dp_index = lax.axis_index('tp'), lax.axis_index('dp')
        vocab_loc, width = emb_table.shape
        head_dim = b_qkv.shape[1] // 3
        seq_len = tokens.shape[1]
        total = tokens.shape[0] // 2

        local_ids = tokens - tp_index * vocab_loc
        in_shard = (local_ids >= 0) & (local_ids < vocab_loc)
        own_ids = lax.dynamic_slice_in_dim(local_ids, tp_index * total, total, 0)
        own_in = lax.dynamic_slice_in_dim(in_shard, tp_index * total, total, 0)
        peer_ids = lax.dynamic_slice_in_dim(local_ids, (1 - tp_index) * total, total, 0)
        peer_in = lax.dynamic_slice_in_dim(in_shard, (1 - tp_index) * total, total, 0)
        own_cot = lax.dynamic_slice_in_dim(cotangent, tp_index * total, total, 0)

        def rows_of(ids, inside):
            rows = jnp.take(emb_table, jnp.where(inside, ids, 0), axis=0)
            return jnp.where(inside[:, :, None], rows, 0.0).astype(F32)

        def small_of(own):
            return jnp.concatenate([own, lax.ppermute(own, 'tp', SWAP)])

        fwd_groups = groups_of(total, 2)
        arrived = []
        for base, count in fwd_groups:
            arrived.append(lax.ppermute(rows_of(peer_ids[base:base + count], peer_in[base:base + count]), 'tp', SWAP))
            if base == 0:
                wqkv_full = with_peer_half(w_qkv, 1, dp_index, parts)
                wout_full = with_peer_half(w_out, 0, dp_index, parts)
                packed = small_of(jnp.concatenate([b_qkv.astype(F32).reshape(-1), b_gate.astype(F32), b_lin.astype(F32)]).reshape(1, -1))
                own_size = b_qkv.size
                wide_loc = b_gate.shape[0]
                bqkv_full = packed[:, :own_size].reshape(1, -1)
                bgate_full = packed[:, own_size:own_size + wide_loc].reshape(1, -1)
                blin_full = packed[:, own_size + wide_loc:].reshape(1, -1)
        wgate_full = with_peer_half(w_gate, 1, dp_index, parts)
        wlin_full = with_peer_half(w_lin, 1, dp_index, parts)
        wdown_full = with_peer_half(w_down, 0, dp_index, parts)

        half_dim = head_dim // 2
        inv_freq = ROPE_BASE ** (-2.0 * jnp.arange(half_dim, dtype=F32) / head_dim)
        angles = jnp.arange(seq_len, dtype=F32)[:, None] * inv_freq[None, :]
        cos_half, sin_half = jnp.cos(angles), jnp.sin(angles)
        tables = (jnp.concatenate([cos_half] * 4, axis=1), jnp.concatenate([-sin_half, sin_half] * 2, axis=1))

        def row_of(vector):
            return vector.astype(F32).reshape(1, -1)

        front = (wqkv_full, bqkv_full, wout_full, row_of(b_out), row_of(ln1_gain), row_of(ln1_bias))
        saved, embs = None, []
        for (base, count), other in zip(fwd_groups, arrived):
            emb = (rows_of(own_ids[base:base + count], own_in[base:base + count]) + other).astype(BF16)
            embs.append(emb)
            saved = attn_forward(base, total, emb, front, tables, saved, head_dim)
        qkv, probs, context, hat, rstd, hidden = saved
        emb_rows = jnp.concatenate(embs, axis=0).reshape(-1, width)

        (inner, d_gate, d_lin, d_ffn, d_resid, narrow, wide) = ffn(
            hidden, own_cot, hat, rstd, (wgate_full, wlin_full, wdown_full, bgate_full, blin_full, row_of(b_down), row_of(ln1_gain), row_of(ln2_gain)))

        def outer(left, right):
            return lax.dot_general(left, right, (((0,), (0,)), ((), ())), preferred_element_type=F32)

        hid_rows, ffn_rows = hidden.reshape(-1, width), d_ffn.reshape(-1, width)
        wide_loc = w_gate.shape[1]
        d_w_down = reduce_weight(outer(inner, ffn_rows).reshape(2, wide_loc, width), parts)
        d_w_gate = reduce_weight(jnp.stack([outer(hid_rows, d_gate[:, :wide_loc]), outer(hid_rows, d_gate[:, wide_loc:])]), parts)
        d_w_lin = reduce_weight(jnp.stack([outer(hid_rows, d_lin[:, :wide_loc]), outer(hid_rows, d_lin[:, wide_loc:])]), parts)

        d_qkv, bias_parts, d_own, d_peer = None, [], [], []
        for base, count in groups_of(total, 2):
            d_emb, d_qkv, bias_part = attn_backward(base, count, total, d_resid, qkv, probs, (wqkv_full, wout_full), tables, d_qkv, head_dim)
            bias_parts.append(bias_part)
            d_own.append(d_emb)
            d_peer.append(lax.ppermute(d_emb, 'tp', SWAP))

        d_rows = jnp.concatenate(d_own + d_peer, axis=0).reshape(-1, width)
        row_ids = jnp.concatenate([jnp.where(own_in, own_ids, vocab_loc), jnp.where(peer_in, peer_ids, vocab_loc)], axis=0).reshape(-1)
        d_table = jnp.zeros((vocab_loc, width), F32).at[row_ids].add(d_rows, mode='drop')
        d_table = lax.psum(d_table, 'dp')

        qkv_rows = d_qkv.reshape(-1, d_qkv.shape[-1])
        qkv_loc = w_qkv.shape[1]
        d_w_qkv = reduce_weight(jnp.stack([outer(emb_rows, qkv_rows[:, :qkv_loc]), outer(emb_rows, qkv_rows[:, qkv_loc:])]), parts)
        d_w_out = reduce_weight(outer(context.reshape(-1, width), d_resid.astype(BF16).reshape(-1, width)).reshape(2, w_out.shape[0], width), parts)

        d_bqkv = jnp.sum(sum(bias_parts), axis=0).reshape(2, -1)
        d_bwide = jnp.sum(wide.reshape(2, 8, -1), axis=1).reshape(2, 2, -1)
        split = jnp.concatenate([d_bqkv, d_bwide[0], d_bwide[1]], axis=1)
        split = jnp.where(tp_index == 0, split, split[::-1])
        flat = jnp.concatenate([split.reshape(-1), jnp.sum(narrow.reshape(5, 8, -1), axis=1).reshape(-1)])
        flat = lax.psum(flat, ('tp', 'dp'))
        split_size = split.shape[1]
        own_split = lax.dynamic_slice_in_dim(flat, tp_index * split_size, split_size, 0)
        d_b_qkv = own_split[:qkv_loc].reshape(b_qkv.shape)
        d_b_gate = own_split[qkv_loc:qkv_loc + wide_loc]
        d_b_lin = own_split[qkv_loc + wide_loc:]
        d_ln2_gain, d_b_down, d_ln1_bias, d_ln1_gain, d_b_out = flat[2 * split_size:].reshape(5, width)
        return (d_table, d_w_qkv, d_b_qkv, d_w_out, d_b_out, d_ln1_gain, d_ln1_bias, d_w_gate, d_b_gate, d_w_lin, d_b_lin, d_w_down, d_b_down, d_ln2_gain)

    return jax.shard_map(device_step, mesh=mesh, in_specs=in_specs, out_specs=out_specs, check_vma=False)
```

```python
import functools

import jax
import jax.numpy as jnp
from jax import lax
from jax.experimental import pallas as pl
from jax.experimental.pallas import tpu as pltpu
from jax.sharding import PartitionSpec as P


ALPHA = 140.0 ** 0.5
EPS = 1e-5
SHRINK = 0.1
ROPE_BASE = 10000.0
WEIGHT_SPECS = (P(None, 'tp'), P('tp', None), P('tp', None), P(), P(), P(), P(None, 'tp'), P('tp'), P(None, 'tp'), P('tp'), P('tp', None), P(), P())

F32 = jnp.float32
BF16 = jnp.bfloat16
LANES = 128
HALF_Q = 256
CHUNK = 512
VMEM_LIMIT = 66 * 1024 * 1024 - 512 * 1024
LOG2E = 1.4426950408889634
MASKED = -8e30
NT = (((1,), (1,)), ((), ()))
NN = (((1,), (0,)), ((), ()))
SWAP = ((0, 1), (1, 0))


def dot_nn(left, right):
    return lax.dot_general(left, right, NN, preferred_element_type=F32)


def dot_nt(left, right):
    return lax.dot_general(left, right, NT, preferred_element_type=F32)


def row_sums(values):
    return jnp.sum(values.reshape(values.shape[0] // 8, 8, values.shape[1]), axis=0)


def rope(values, cos_tab, sin_tab, first_half):
    partner = jnp.where(first_half, pltpu.roll(values, 96, 1), pltpu.roll(values, 32, 1))
    return values * cos_tab + partner * sin_tab


def lane_masks():
    lane = lax.broadcasted_iota(jnp.int32, (1, LANES), 1)
    low = lane < 64
    return low, low.astype(F32).astype(BF16), (1.0 - low.astype(F32)).astype(BF16), (lane % 64) < 32


def attn_forward_kernel(head_dim, alias_count, *refs):
    (own_ref, other_ref, wqkv_ref, bqkv_ref, wo_ref, bo_ref, gain_ref, bias_ref, cos_ref, sin_ref) = refs[:10]
    (emb_ref, qkv_ref, prob_ref, ctx_ref, hat_ref, rstd_ref, hid_ref, token_ref) = refs[10 + alias_count:]
    seq_len, width = own_ref.shape[1], own_ref.shape[2]
    token_ref[...] = jnp.zeros_like(token_ref)
    emb_ref[0] = (own_ref[0].astype(F32) + other_ref[0]).astype(BF16)
    low, mask_low, mask_high, first_half = lane_masks()
    score_scale = head_dim ** -0.5 * LOG2E
    causal = lax.broadcasted_iota(jnp.int32, (HALF_Q, HALF_Q), 0) <= lax.broadcasted_iota(jnp.int32, (HALF_Q, HALF_Q), 1)
    step = 4 * 3 * head_dim

    def quad(index, carry):
        col = pl.multiple_of(index * step, step)
        pre = dot_nn(emb_ref[0], wqkv_ref[:, pl.ds(col, step)]) + bqkv_ref[:, pl.ds(col, step)]
        pre = pre.astype(BF16).astype(F32)
        for half in range(2):
            parts = [pre[:, (half * 3 + part) * LANES:(half * 3 + part + 1) * LANES] for part in range(3)]
            pair = index * 2 + half
            pair_col = pl.multiple_of(pair * LANES, LANES)
            q_pair = jnp.where(low, parts[0], parts[1])
            k_pair = pltpu.roll(jnp.where(low, parts[2], parts[0]), 64, 1)
            v_pair = jnp.where(low, parts[1], parts[2])
            q_rot = rope(q_pair, cos_ref[...], sin_ref[...], first_half).astype(BF16)
            k_rot = rope(k_pair, cos_ref[...], sin_ref[...], first_half).astype(BF16)
            qkv_ref[0, :, pl.ds(pair_col, LANES)] = q_rot
            qkv_ref[0, :, pl.ds(width + pair_col, LANES)] = k_rot
            qkv_ref[0, :, pl.ds(2 * width + pair_col, LANES)] = v_pair.astype(BF16)
            v_trans = v_pair.T.astype(BF16)
            ctx_rows = []
            for head in range(2):
                k_one = k_rot * (mask_low if head == 0 else mask_high)
                v_one = v_trans[head * 64:(head + 1) * 64]
                blocks = []
                for block in range(2):
                    q_block = q_rot[block * HALF_Q:(block + 1) * HALF_Q]
                    diag = jnp.where(causal, dot_nt(k_one[block * HALF_Q:(block + 1) * HALF_Q], q_block), MASKED)
                    pieces = [diag] if block == 0 else [dot_nt(k_one[:HALF_Q], q_block), diag]
                    peak = functools.reduce(jnp.maximum, [jnp.max(piece, axis=0, keepdims=True) for piece in pieces])
                    exps = [jnp.exp2((piece - peak) * score_scale) for piece in pieces]
                    total = functools.reduce(jnp.add, [jnp.sum(piece, axis=0, keepdims=True) for piece in exps])
                    inverse = 1.0 / total
                    ctx = None
                    for num, piece in enumerate(exps):
                        prob = (piece * inverse).astype(BF16)
                        prob_ref[0, pair * 2 + head, (block + num) * HALF_Q:(block + num + 1) * HALF_Q, :] = prob
                        term = dot_nn(v_one[:, num * HALF_Q:(num + 1) * HALF_Q], prob)
                        ctx = term if ctx is None else ctx + term
                    blocks.append(ctx)
                ctx_rows.append(jnp.concatenate(blocks, axis=1))
            ctx_pair = jnp.concatenate(ctx_rows, axis=0)
            ctx_ref[0, :, pl.ds(pair_col, LANES)] = ctx_pair.T.astype(BF16)
        return carry

    lax.fori_loop(0, wqkv_ref.shape[1] // step, quad, 0)
    attn = dot_nn(ctx_ref[0], wo_ref[...]) + bo_ref[...]
    resid = ALPHA * emb_ref[0].astype(F32) + attn
    centered = resid - jnp.mean(resid, axis=-1, keepdims=True)
    variance = jnp.mean(centered * centered, axis=-1, keepdims=True)
    rstd = lax.rsqrt(variance + EPS)
    hat = centered * rstd
    hat_ref[0] = hat
    rstd_ref[0] = jnp.broadcast_to(rstd, (seq_len, LANES))
    hid_ref[0] = (hat * gain_ref[...] + bias_ref[...]).astype(BF16)


def ffn_kernel(base, chunk_size, hid_ref, cot_ref, hat_ref, rstd_ref, wg_ref, wl_ref, wd_ref, bg_ref, bl_ref, bd_ref, gain1_ref, gain2_ref,
               *refs):
    (inner_out, gate_out, lin_out, dffn_ref, dres_ref, dattn_ref, narrow_ref, wide_ref, token_ref,
     act_buf, slope_buf, inner_buf, gate_buf, lin_buf, acc_buf, sems) = refs[-16:]
    step = pl.program_id(0)
    last = pl.num_programs(0) - 1
    token_ref[...] = jnp.zeros_like(token_ref)
    rows = hid_ref.shape[1]
    chunks = wg_ref.shape[1] // chunk_size

    def copy_out(buf, out, kind, chunk, block):
        cols = pl.ds(pl.multiple_of(chunk * chunk_size, chunk_size), chunk_size)
        return pltpu.make_async_copy(buf.at[:, cols], out.at[pl.ds((block + base) * rows, rows), cols], sems.at[kind, chunk])

    @pl.when(step == 0)
    def _():
        narrow_ref[...] = jnp.zeros_like(narrow_ref)
        wide_ref[...] = jnp.zeros_like(wide_ref)

    acc_buf[...] = jnp.zeros_like(acc_buf)

    def forward(chunk, carry):
        cols = pl.ds(pl.multiple_of(chunk * chunk_size, chunk_size), chunk_size)
        gate_pre = dot_nn(hid_ref[0], wg_ref[:, cols]) + bg_ref[:, cols]
        lin_pre = dot_nn(hid_ref[0], wl_ref[:, cols]) + bl_ref[:, cols]
        cdf = 0.5 + 0.5 * lax.erf(gate_pre * (0.5 ** 0.5))
        act = gate_pre * cdf
        pdf = jnp.exp2(gate_pre * gate_pre * (-0.5 * LOG2E)) * 0.3989422804014327
        act_buf[:, cols] = act
        slope_buf[:, cols] = lin_pre * (cdf + gate_pre * pdf)

        @pl.when(step > 0)
        def _():
            copy_out(inner_buf, inner_out, 0, chunk, step - 1).wait()

        inner = (act * lin_pre).astype(BF16)
        inner_buf[:, cols] = inner
        acc_buf[...] += dot_nn(inner, wd_ref[cols, :])
        copy_out(inner_buf, inner_out, 0, chunk, step).start()
        return carry

    lax.fori_loop(0, chunks, forward, 0)
    resid = ALPHA * hid_ref[0].astype(F32) + (acc_buf[...] + bd_ref[...])
    centered = resid - jnp.mean(resid, axis=-1, keepdims=True)
    variance = jnp.mean(centered * centered, axis=-1, keepdims=True)
    rstd = lax.rsqrt(variance + EPS)
    hat = centered * rstd
    cot = cot_ref[0].astype(F32)
    narrow_ref[0:8] += row_sums(cot * hat)
    d_hat = cot * gain2_ref[...]
    d_resid = rstd * (d_hat - jnp.mean(d_hat, axis=-1, keepdims=True) - hat * jnp.mean(d_hat * hat, axis=-1, keepdims=True))
    narrow_ref[8:16] += row_sums(d_resid)
    dffn_ref[0] = d_resid.astype(BF16)
    acc_buf[...] = ALPHA * d_resid

    def backward(chunk, carry):
        cols = pl.ds(pl.multiple_of(chunk * chunk_size, chunk_size), chunk_size)
        d_inner = dot_nt(dffn_ref[0], wd_ref[cols, :]).astype(BF16).astype(F32)
        d_gate = d_inner * slope_buf[:, cols]
        d_lin = d_inner * act_buf[:, cols]
        wide_ref[0:8, cols] += row_sums(d_gate)
        wide_ref[8:16, cols] += row_sums(d_lin)

        @pl.when(step > 0)
        def _():
            copy_out(gate_buf, gate_out, 1, chunk, step - 1).wait()
            copy_out(lin_buf, lin_out, 2, chunk, step - 1).wait()

        d_gate = d_gate.astype(BF16)
        d_lin = d_lin.astype(BF16)
        gate_buf[:, cols] = d_gate
        lin_buf[:, cols] = d_lin
        acc_buf[...] += dot_nt(d_gate, wg_ref[:, cols]) + dot_nt(d_lin, wl_ref[:, cols])
        copy_out(gate_buf, gate_out, 1, chunk, step).start()
        copy_out(lin_buf, lin_out, 2, chunk, step).start()
        return carry

    lax.fori_loop(0, chunks, backward, 0)
    d_hid = acc_buf[...]
    hat = hat_ref[0]
    narrow_ref[16:24] += row_sums(d_hid)
    narrow_ref[24:32] += row_sums(d_hid * hat)
    d_hat = d_hid * gain1_ref[...]
    d_resid = rstd_ref[0][:, :1] * (d_hat - jnp.mean(d_hat, axis=-1, keepdims=True) - hat * jnp.mean(d_hat * hat, axis=-1, keepdims=True))
    narrow_ref[32:40] += row_sums(d_resid)
    dres_ref[0] = d_resid
    dattn_ref[0] = d_resid.astype(BF16)

    @pl.when(step == last)
    def _():
        def drain(chunk, carry):
            copy_out(inner_buf, inner_out, 0, chunk, step).wait()
            copy_out(gate_buf, gate_out, 1, chunk, step).wait()
            copy_out(lin_buf, lin_out, 2, chunk, step).wait()
            return carry

        lax.fori_loop(0, chunks, drain, 0)


def attn_backward_kernel(head_dim, alias_count, *refs):
    (dres_ref, dattn_ref, qkv_ref, prob_ref, wqkv_ref, wo_ref, cos_ref, sin_ref) = refs[:8]
    (demb_ref, dqkv_ref, dall_ref, acc_ref, token_ref) = refs[8 + alias_count:]
    token_ref[...] = jnp.zeros_like(token_ref)
    width = dres_ref.shape[2]
    low, mask_low, mask_high, first_half = lane_masks()
    attn_scale = head_dim ** -0.5
    step = 4 * 3 * head_dim

    @pl.when(pl.program_id(0) == 0)
    def _():
        acc_ref[...] = jnp.zeros_like(acc_ref)

    def quad(index, carry):
        col = pl.multiple_of(index * step, step)
        ctx_row = pl.multiple_of(index * 4 * head_dim, 4 * head_dim)
        d_ctx_quad = dot_nt(dattn_ref[0], wo_ref[pl.ds(ctx_row, 4 * head_dim), :]).astype(BF16)
        pieces = []
        for half in range(2):
            pair = index * 2 + half
            pair_col = pl.multiple_of(pair * LANES, LANES)
            d_ctx = d_ctx_quad[:, half * LANES:(half + 1) * LANES]
            q_rot = qkv_ref[0, :, pl.ds(pair_col, LANES)]
            k_rot = qkv_ref[0, :, pl.ds(width + pair_col, LANES)]
            v_pair = qkv_ref[0, :, pl.ds(2 * width + pair_col, LANES)]
            k_trans = k_rot.astype(F32).T.astype(BF16)
            dq_rows, dk_heads, dv_heads = [], [], []
            for head in range(2):
                v_one = v_pair * (mask_low if head == 0 else mask_high)
                k_one = k_trans[head * 64:(head + 1) * 64]
                d_v, d_k, d_q = [None, None], [None, None], []
                for block in range(2):
                    rows = slice(block * HALF_Q, (block + 1) * HALF_Q)
                    keys = range(block + 1)
                    probs = [prob_ref[0, pair * 2 + head, (block + num) * HALF_Q:(block + num + 1) * HALF_Q, :] for num in keys]
                    d_probs = [dot_nt(v_one[num * HALF_Q:(num + 1) * HALF_Q], d_ctx[rows]) for num in keys]
                    wide = [prob.astype(F32) for prob in probs]
                    inner = functools.reduce(jnp.add, [jnp.sum(d_prob * prob, axis=0, keepdims=True) for d_prob, prob in zip(d_probs, wide)])
                    d_q_block = None
                    for num in keys:
                        d_score = (wide[num] * (d_probs[num] - inner) * attn_scale).astype(BF16)
                        terms = (dot_nn(probs[num], d_ctx[rows]), dot_nn(d_score, q_rot[rows]), dot_nn(k_one[:, num * HALF_Q:(num + 1) * HALF_Q], d_score))
                        d_v[num] = terms[0] if d_v[num] is None else d_v[num] + terms[0]
                        d_k[num] = terms[1] if d_k[num] is None else d_k[num] + terms[1]
                        d_q_block = terms[2] if d_q_block is None else d_q_block + terms[2]
                    d_q.append(d_q_block)
                dq_rows.append(jnp.concatenate(d_q, axis=1))
                dk_heads.append(jnp.concatenate(d_k, axis=0))
                dv_heads.append(jnp.concatenate(d_v, axis=0))
            d_q = rope(jnp.concatenate(dq_rows, axis=0).T, cos_ref[...], -sin_ref[...], first_half)
            d_k = rope(jnp.where(low, dk_heads[0], dk_heads[1]), cos_ref[...], -sin_ref[...], first_half)
            d_v = jnp.where(low, dv_heads[0], dv_heads[1])
            d_k = pltpu.roll(d_k, 64, 1)
            pieces += [jnp.where(low, d_q, d_k), jnp.where(low, d_v, d_q), jnp.where(low, d_k, d_v)]
        for num, piece in enumerate(pieces):
            lanes = pl.ds(col + num * LANES, LANES)
            acc_ref[:, lanes] += row_sums(piece)
            dqkv_ref[0, :, lanes] = piece.astype(BF16)
        return carry

    lax.fori_loop(0, wqkv_ref.shape[1] // step, quad, 0)
    d_emb = SHRINK * (ALPHA * dres_ref[0] + dot_nt(dqkv_ref[0], wqkv_ref[...]))
    demb_ref[0] = d_emb
    dall_ref[0] = d_emb


def whole(shape):
    return pl.BlockSpec(shape, lambda i: (0,) * len(shape), pipeline_mode=pl.Buffered(1))


def per_seq(shape, base=0):
    return pl.BlockSpec((1,) + tuple(shape), lambda i: (i + base,) + (0,) * len(shape))


def params():
    return pltpu.CompilerParams(dimension_semantics=('arbitrary',), vmem_limit_bytes=VMEM_LIMIT)


TOKEN = (8, LANES)
ANYWHERE = pl.BlockSpec(memory_space=pl.ANY)


def token_spec():
    return pl.BlockSpec(TOKEN, lambda i: (0, 0))


def attn_forward(base, count, total, own, other, offset, weights, tables, previous, deps, head_dim):
    seq_len, width = own.shape[1:]
    wqkv = weights[0]
    heads = width // head_dim
    shapes = [((seq_len, width), BF16), ((seq_len, 3 * width), BF16), ((heads, seq_len * 3 // 2, HALF_Q), BF16), ((seq_len, width), BF16),
              ((seq_len, width), F32), ((seq_len, LANES), F32), ((seq_len, width), BF16)]
    operands = (own, other) + tuple(weights) + tuple(tables)
    specs = [per_seq((seq_len, width), base), per_seq((seq_len, width), offset)] + [whole(item.shape) for item in operands[2:]]
    extra = tuple(previous) if previous is not None else ()
    specs += [ANYWHERE] * (len(extra) + len(deps))
    flops = count * (2 * seq_len * width * (wqkv.shape[1] + width) + 4 * heads * seq_len * seq_len * 64)
    return pl.pallas_call(
        functools.partial(attn_forward_kernel, head_dim, len(extra) + len(deps)),
        grid=(count,),
        in_specs=specs,
        out_specs=[per_seq(shape, base) for shape, _ in shapes] + [token_spec()],
        out_shape=[jax.ShapeDtypeStruct((total,) + shape, dtype) for shape, dtype in shapes] + [jax.ShapeDtypeStruct(TOKEN, F32)],
        input_output_aliases={len(operands) + num: num for num in range(len(extra))},
        compiler_params=params(),
        cost_estimate=pl.CostEstimate(flops=2 * flops, bytes_accessed=count * 12_000_000, transcendentals=0),
        name='attn_forward',
    )(*operands, *extra, *deps)


def ffn(base, count, chunk_size, hidden, cotangent, hat, rstd, weights, previous, deps):
    total, seq_len, width = hidden.shape
    wide = weights[0].shape[1]
    operands = (hidden, cotangent, hat, rstd) + tuple(weights)
    extra = tuple(previous) if previous is not None else ()
    specs = [per_seq(item.shape[1:], base) for item in operands[:4]] + [whole(item.shape) for item in operands[4:]]
    specs += [ANYWHERE] * (len(extra) + len(deps))
    big = jax.ShapeDtypeStruct((total * seq_len, wide), BF16)
    narrow = jax.ShapeDtypeStruct((total, seq_len, width), BF16)
    flops = 12 * count * seq_len * width * wide
    return pl.pallas_call(
        functools.partial(ffn_kernel, base, chunk_size),
        grid=(count,),
        in_specs=specs,
        out_specs=[ANYWHERE] * 3 + [per_seq((seq_len, width), base)] * 3 + [pl.BlockSpec((40, width), lambda i: (0, 0)), pl.BlockSpec((16, wide), lambda i: (0, 0)), token_spec()],
        out_shape=[big] * 3 + [narrow, jax.ShapeDtypeStruct((total, seq_len, width), F32), narrow,
                               jax.ShapeDtypeStruct((40, width), F32), jax.ShapeDtypeStruct((16, wide), F32), jax.ShapeDtypeStruct(TOKEN, F32)],
        scratch_shapes=[pltpu.VMEM((seq_len, wide), F32)] * 2 + [pltpu.VMEM((seq_len, wide), BF16)] * 3
        + [pltpu.VMEM((seq_len, width), F32), pltpu.SemaphoreType.DMA((3, wide // chunk_size))],
        input_output_aliases={len(operands) + num: num for num in range(len(extra))},
        compiler_params=params(),
        cost_estimate=pl.CostEstimate(flops=int(1.5 * flops), bytes_accessed=count * 14_000_000, transcendentals=0),
        name='ffn',
    )(*operands, *extra, *deps)


def attn_backward(base, count, total, d_resid, d_attn, qkv, probs, weights, tables, previous, deps, head_dim):
    seq_len, width = d_resid.shape[1:]
    wqkv, wout = weights
    heads = width // head_dim
    operands = (d_resid, d_attn, qkv, probs, wqkv, wout) + tuple(tables)
    specs = [per_seq(item.shape[1:], base) for item in operands[:4]] + [whole(item.shape) for item in operands[4:]]
    extra = tuple(previous) if previous is not None else ()
    specs += [ANYWHERE] * (len(extra) + len(deps))
    flops = count * (2 * seq_len * width * (wqkv.shape[1] + width) + 8 * heads * seq_len * seq_len * 64)
    return pl.pallas_call(
        functools.partial(attn_backward_kernel, head_dim, len(extra) + len(deps)),
        grid=(count,),
        in_specs=specs,
        out_specs=[per_seq((seq_len, width)), per_seq((seq_len, wqkv.shape[1]), base), per_seq((seq_len, width), base), pl.BlockSpec((8, wqkv.shape[1]), lambda i: (0, 0)), token_spec()],
        out_shape=[jax.ShapeDtypeStruct((count, seq_len, width), F32), jax.ShapeDtypeStruct((total, seq_len, wqkv.shape[1]), BF16),
                   jax.ShapeDtypeStruct((total, seq_len, width), F32),
                   jax.ShapeDtypeStruct((8, wqkv.shape[1]), F32), jax.ShapeDtypeStruct(TOKEN, F32)],
        input_output_aliases={len(operands) + num: 1 + num for num in range(len(extra))},
        compiler_params=params(),
        cost_estimate=pl.CostEstimate(flops=2 * flops, bytes_accessed=count * 12_000_000, transcendentals=0),
        name='attn_backward',
    )(*operands, *extra, *deps)


def outer_kernel(flip, left_ref, right_ref, *refs):
    out_ref, token_ref, left_t = refs[-3:]
    token_ref[...] = jnp.zeros_like(token_ref)

    @pl.when(pl.program_id(0) == 0)
    def _():
        def turn(index, carry):
            rows = pl.ds(pl.multiple_of(index * CHUNK, CHUNK), CHUNK)
            left_t[:, rows] = left_ref[rows, :].astype(F32).T.astype(BF16)
            return carry

        lax.fori_loop(0, left_ref.shape[0] // CHUNK, turn, 0)

    result = dot_nn(left_t[...], right_ref[...])
    out_ref[...] = result.T if flip else result


def outer(left, right, block, flip, deps):
    rows, width = left.shape
    wide = right.shape[1]
    shape = (wide, width) if flip else (width, wide)
    return pl.pallas_call(
        functools.partial(outer_kernel, flip),
        grid=(wide // block,),
        in_specs=[whole((rows, width)), pl.BlockSpec((rows, block), lambda i: (0, i))] + [ANYWHERE] * len(deps),
        out_specs=[pl.BlockSpec((block, width), lambda i: (i, 0)) if flip else pl.BlockSpec((width, block), lambda i: (0, i)), token_spec()],
        out_shape=[jax.ShapeDtypeStruct(shape, F32), jax.ShapeDtypeStruct(TOKEN, F32)],
        scratch_shapes=[pltpu.VMEM((width, rows), BF16)],
        compiler_params=params(),
        cost_estimate=pl.CostEstimate(flops=2 * rows * width * wide, bytes_accessed=4 * width * wide + 2 * rows * (width + wide), transcendentals=0),
        name='outer',
    )(left, right, *deps)


def join_kernel(axis, blocks, own_ref, peer_ref, out_ref):
    if axis == 1:
        split = own_ref.shape[1]
        out_ref[:, :split] = own_ref[...]
        out_ref[:, split:] = peer_ref[...].astype(BF16)
    else:
        @pl.when(pl.program_id(0) < blocks)
        def _():
            out_ref[...] = own_ref[...]

        @pl.when(pl.program_id(0) >= blocks)
        def _():
            out_ref[...] = peer_ref[...].astype(BF16)


def with_peer_half(own, axis, index, parts):
    rows = own.shape[0] // parts
    piece = lax.dynamic_slice_in_dim(own, index * rows, rows, 0).astype(F32)
    piece = lax.ppermute(piece, 'tp', SWAP)
    peer = lax.all_gather(piece, 'dp', axis=0, tiled=True)
    blocks = 4
    shape = (own.shape[0] // blocks, own.shape[1])
    if axis == 1:
        grid, out_block, out_shape = (blocks,), (shape[0], 2 * shape[1]), (own.shape[0], 2 * own.shape[1])
        own_map = peer_map = lambda i: (i, 0)
    else:
        grid, out_block, out_shape = (2 * blocks,), shape, (2 * own.shape[0], own.shape[1])
        own_map, peer_map = (lambda i: (jnp.minimum(i, blocks - 1), 0)), (lambda i: (jnp.maximum(i - blocks, 0), 0))
    return pl.pallas_call(
        functools.partial(join_kernel, axis, blocks),
        grid=grid,
        in_specs=[pl.BlockSpec(shape, own_map), pl.BlockSpec(shape, peer_map)],
        out_specs=pl.BlockSpec(out_block, lambda i: (i, 0)),
        out_shape=jax.ShapeDtypeStruct(out_shape, BF16),
        compiler_params=params(),
        cost_estimate=pl.CostEstimate(flops=own.size * 64, bytes_accessed=own.size * 10, transcendentals=0),
        name='join_weight',
    )(own, peer)


def reduce_columns(grad):
    piece = lax.psum_scatter(grad, 'dp', scatter_dimension=0, tiled=True)
    half = piece.shape[1] // 2
    mine = piece[:, :half] + lax.ppermute(piece[:, half:], 'tp', SWAP)
    return lax.all_gather(mine, 'dp', axis=0, tiled=True)


def reduce_rows(grad):
    piece = lax.psum_scatter(grad.reshape(2, grad.shape[0] // 2, grad.shape[1]), 'dp', scatter_dimension=1, tiled=True)
    mine = piece[0] + lax.ppermute(piece[1], 'tp', SWAP)
    return lax.all_gather(mine, 'dp', axis=0, tiled=True)


def tie(value, token):
    return lax.optimization_barrier((value, token))[0]


def solution(mesh):
    in_specs = (P('dp', None), P('dp', None, None), P('tp', None)) + WEIGHT_SPECS
    out_specs = (P('tp', None),) + WEIGHT_SPECS
    parts = mesh.shape['dp']

    def device_step(tokens, cotangent, emb_table, *weights):
        (w_qkv, b_qkv, w_out, b_out, ln1_gain, ln1_bias, w_gate, b_gate, w_lin, b_lin, w_down, b_down, ln2_gain) = weights
        tp_index, dp_index = lax.axis_index('tp'), lax.axis_index('dp')
        vocab_loc, width = emb_table.shape
        head_dim = b_qkv.shape[1] // 3
        seq_len = tokens.shape[1]
        total = tokens.shape[0] // 2

        local_ids = tokens - tp_index * vocab_loc
        in_shard = (local_ids >= 0) & (local_ids < vocab_loc)
        own_ids = lax.dynamic_slice_in_dim(local_ids, tp_index * total, total, 0)
        own_in = lax.dynamic_slice_in_dim(in_shard, tp_index * total, total, 0)
        peer_ids = lax.dynamic_slice_in_dim(local_ids, (1 - tp_index) * total, total, 0)
        peer_in = lax.dynamic_slice_in_dim(in_shard, (1 - tp_index) * total, total, 0)
        own_cot = lax.dynamic_slice_in_dim(cotangent, tp_index * total, total, 0)

        def rows_of(ids, inside):
            rows = jnp.take(emb_table, jnp.where(inside, ids, 0), axis=0)
            return jnp.where(inside[:, :, None], rows, 0.0).astype(F32)

        def small_of(own):
            return jnp.concatenate([own, lax.ppermute(own, 'tp', SWAP)])

        size = total // 4
        quarters = [(num * size, size) for num in range(4)]
        first = rows_of(peer_ids[:size], peer_in[:size])
        rest = rows_of(peer_ids[size:], peer_in[size:])
        wqkv_full = with_peer_half(w_qkv, 1, dp_index, parts)
        wout_full = with_peer_half(w_out, 0, dp_index, parts)
        arrived = [lax.ppermute(first, 'tp', SWAP)] + [lax.ppermute(rest[num * size:(num + 1) * size], 'tp', SWAP) for num in range(3)]
        packed = small_of(jnp.concatenate([b_qkv.astype(F32).reshape(-1), b_gate.astype(F32), b_lin.astype(F32)]).reshape(1, -1))
        own_size = b_qkv.size
        wide_loc = b_gate.shape[0]
        bqkv_full = packed[:, :own_size].reshape(1, -1)
        bgate_full = packed[:, own_size:own_size + wide_loc].reshape(1, -1)
        blin_full = packed[:, own_size + wide_loc:].reshape(1, -1)
        wgate_full = with_peer_half(w_gate, 1, dp_index, parts)
        wlin_full = with_peer_half(w_lin, 1, dp_index, parts)
        wdown_full = with_peer_half(w_down, 0, dp_index, parts)

        half_dim = head_dim // 2
        inv_freq = ROPE_BASE ** (-2.0 * jnp.arange(half_dim, dtype=F32) / head_dim)
        angles = jnp.arange(seq_len, dtype=F32)[:, None] * inv_freq[None, :]
        cos_half, sin_half = jnp.cos(angles), jnp.sin(angles)
        tables = (jnp.concatenate([cos_half] * 4, axis=1), jnp.concatenate([-sin_half, sin_half] * 2, axis=1))

        def row_of(vector):
            return vector.astype(F32).reshape(1, -1)

        own_rows = jnp.where(own_in[:, :, None], jnp.take(emb_table, jnp.where(own_in, own_ids, 0), axis=0), 0.0)
        front = (wqkv_full, bqkv_full, wout_full, row_of(b_out), row_of(ln1_gain), row_of(ln1_bias))
        middle = (wgate_full, wlin_full, wdown_full, bgate_full, blin_full, row_of(b_down), row_of(ln1_gain), row_of(ln2_gain))
        saved, ffn_saved, d_kept, deps = None, None, None, ()
        narrow_parts, wide_parts, bias_parts, d_peer = [], [], [], []

        def run_attention(num):
            nonlocal saved, deps
            base, count = quarters[num]
            out = attn_forward(base, count, total, own_rows, arrived[num], 0, front, tables, saved, deps, head_dim)
            saved, deps = out[:-1], (out[-1],)

        def run_ffn(base, count, chunk_size):
            nonlocal ffn_saved, deps
            out = ffn(base, count, chunk_size, saved[6], own_cot, saved[4], saved[5], middle, ffn_saved, deps)
            ffn_saved, deps = out[:6], (out[-1],)
            narrow_parts.append(out[6])
            wide_parts.append(out[7])

        def run_backward(base, count):
            nonlocal d_kept, deps
            d_emb, d_qkv, d_all, bias_part, token = attn_backward(base, count, total, ffn_saved[4], ffn_saved[5], saved[1], saved[2], (wqkv_full, wout_full), tables, d_kept, deps, head_dim)
            d_kept, deps = (d_qkv, d_all), (token,)
            bias_parts.append(bias_part)
            d_peer.append(lax.ppermute(d_emb, 'tp', SWAP))

        def run_outer(left, right, block, flip=False):
            nonlocal deps
            out, token = outer(left.reshape(-1, left.shape[-1]), right.reshape(-1, right.shape[-1]), block, flip, deps)
            deps = (token,)
            return out

        for num in range(4):
            run_attention(num)
        run_ffn(0, 2 * size, CHUNK)
        run_backward(0, 2 * size)
        run_ffn(2 * size, 2 * size, 768)
        d_w_gate = reduce_columns(run_outer(saved[6], ffn_saved[1], CHUNK))
        d_w_lin = reduce_columns(run_outer(saved[6], ffn_saved[2], CHUNK))
        d_w_down = reduce_rows(run_outer(ffn_saved[3], ffn_saved[0], CHUNK, True))
        run_backward(2 * size, size)
        run_backward(3 * size, size)
        d_w_out = reduce_rows(run_outer(saved[3], ffn_saved[5], width))
        d_w_qkv = reduce_columns(run_outer(saved[0], d_kept[0], width))

        own_row_ids = jnp.where(own_in, own_ids, vocab_loc)
        peer_row_ids = jnp.where(peer_in, peer_ids, vocab_loc)

        def add_rows(grad, ids, rows):
            return grad.at[ids.reshape(-1)].add(rows.reshape(-1, width), mode='drop')

        d_table = add_rows(jnp.zeros((vocab_loc, width), F32), tie(own_row_ids, deps[0]), d_kept[1])
        d_table = add_rows(d_table, peer_row_ids, jnp.concatenate(d_peer, axis=0))
        d_table = lax.psum(d_table, 'dp')

        narrow, wide = sum(narrow_parts), sum(wide_parts)
        qkv_loc = own_size
        d_bqkv = jnp.sum(sum(bias_parts), axis=0).reshape(2, -1)
        d_bwide = jnp.sum(wide.reshape(2, 8, -1), axis=1).reshape(2, 2, -1)
        split = jnp.concatenate([d_bqkv, d_bwide[0], d_bwide[1]], axis=1)
        split = jnp.where(tp_index == 0, split, split[::-1])
        flat = jnp.concatenate([split.reshape(-1), jnp.sum(narrow.reshape(5, 8, -1), axis=1).reshape(-1)])
        flat = lax.psum(flat, ('tp', 'dp'))
        split_size = split.shape[1]
        own_split = lax.dynamic_slice_in_dim(flat, tp_index * split_size, split_size, 0)
        d_b_qkv = own_split[:qkv_loc].reshape(b_qkv.shape)
        d_b_gate = own_split[qkv_loc:qkv_loc + wide_loc]
        d_b_lin = own_split[qkv_loc + wide_loc:]
        d_ln2_gain, d_b_down, d_ln1_bias, d_ln1_gain, d_b_out = flat[2 * split_size:].reshape(5, width)
        return (d_table, d_w_qkv, d_b_qkv, d_w_out, d_b_out, d_ln1_gain, d_ln1_bias, d_w_gate, d_b_gate, d_w_lin, d_b_lin, d_w_down, d_b_down, d_ln2_gain)

    return shard(device_step, mesh, in_specs, out_specs)


def shard(step, mesh, in_specs, out_specs):
    return jax.shard_map(step, mesh=mesh, in_specs=in_specs, out_specs=out_specs, check_vma=False)
```

```python
import functools

import jax
import jax.numpy as jnp
from jax import lax
from jax.experimental import pallas as pl
from jax.experimental.pallas import tpu as pltpu
from jax.sharding import PartitionSpec as P


ALPHA = 140.0 ** 0.5
EPS = 1e-5
SHRINK = 0.1
ROPE_BASE = 10000.0
COLS, ROWS, ALL = P(None, 'tp'), P('tp'), P()
WEIGHT_SPECS = (COLS, ROWS, ROWS, ALL, ALL, ALL, COLS, ROWS, COLS, ROWS, ROWS, ALL, ALL)

F32 = jnp.float32
BF16 = jnp.bfloat16
LANES = 128
HALF_Q = 256
CHUNK = 512
FFN_CHUNK = 768
TILE = 8
PIECES = 3
VMEM_LIMIT = 66 * 1024 * 1024 - 512 * 1024
LOG2E = 1.4426950408889634
MASKED = -8e30
NT = (((1,), (1,)), ((), ()))
NN = (((1,), (0,)), ((), ()))
SWAP = ((0, 1), (1, 0))


def dot_nn(left, right):
    return lax.dot_general(left, right, NN, preferred_element_type=F32)


def dot_nt(left, right):
    return lax.dot_general(left, right, NT, preferred_element_type=F32)


def row_sums(values):
    return jnp.sum(values.reshape(-1, TILE, values.shape[1]), axis=0)


def row_mean(values):
    return jnp.mean(values, axis=-1, keepdims=True)


def col_sum(values):
    return jnp.sum(values, axis=0, keepdims=True)


def add_sums(ref, slot, values):
    ref[slot * TILE:(slot + 1) * TILE] += row_sums(values)


def full(ref):
    return ref[...]


def clear(ref):
    ref[...] = jnp.zeros_like(ref)


def normalize(values):
    centered = values - row_mean(values)
    rstd = lax.rsqrt(row_mean(centered * centered) + EPS)
    return centered * rstd, rstd


def normalize_back(d_hat, hat, rstd):
    return rstd * (d_hat - row_mean(d_hat) - hat * row_mean(d_hat * hat))


def rope(values, cos_tab, sin_tab, first_half):
    partner = jnp.where(first_half, pltpu.roll(values, 96, 1), pltpu.roll(values, 32, 1))
    return values * cos_tab + partner * sin_tab


def lane_masks():
    lane = lax.broadcasted_iota(jnp.int32, (1, LANES), 1)
    low = lane < 64
    return low, low.astype(F32).astype(BF16), (1.0 - low.astype(F32)).astype(BF16), (lane % 64) < 32


def attn_forward_kernel(head_dim, alias_count, *refs):
    (own_ref, other_ref, wqkv_ref, bqkv_ref, wo_ref, bo_ref, gain_ref, bias_ref, cos_ref, sin_ref) = refs[:10]
    (emb_ref, qkv_ref, prob_ref, ctx_ref, hat_ref, rstd_ref, hid_ref, token_ref) = refs[10 + alias_count:]
    seq_len, width = own_ref.shape
    clear(token_ref)
    emb_ref[...] = (full(own_ref).astype(F32) + full(other_ref)).astype(BF16)
    low, mask_low, mask_high, first_half = lane_masks()
    score_scale = head_dim ** -0.5 * LOG2E
    causal = lax.broadcasted_iota(jnp.int32, (HALF_Q, HALF_Q), 0) <= lax.broadcasted_iota(jnp.int32, (HALF_Q, HALF_Q), 1)
    step = 4 * 3 * head_dim

    def quad(index, carry):
        col = pl.multiple_of(index * step, step)
        pre = dot_nn(full(emb_ref), wqkv_ref[:, pl.ds(col, step)]) + bqkv_ref[:, pl.ds(col, step)]
        pre = pre.astype(BF16).astype(F32)
        for half in range(2):
            parts = [pre[:, (half * 3 + part) * LANES:(half * 3 + part + 1) * LANES] for part in range(3)]
            pair = index * 2 + half
            pair_col = pl.multiple_of(pair * LANES, LANES)
            q_pair = jnp.where(low, parts[0], parts[1])
            k_pair = pltpu.roll(jnp.where(low, parts[2], parts[0]), 64, 1)
            v_pair = jnp.where(low, parts[1], parts[2])
            q_rot = rope(q_pair, full(cos_ref), full(sin_ref), first_half).astype(BF16)
            k_rot = rope(k_pair, full(cos_ref), full(sin_ref), first_half).astype(BF16)
            qkv_ref[:, pl.ds(pair_col, LANES)] = q_rot
            qkv_ref[:, pl.ds(width + pair_col, LANES)] = k_rot
            qkv_ref[:, pl.ds(2 * width + pair_col, LANES)] = v_pair.astype(BF16)
            v_trans = v_pair.T.astype(BF16)
            ctx_rows = []
            for head in range(2):
                k_one = k_rot * (mask_low if head == 0 else mask_high)
                v_one = v_trans[head * 64:(head + 1) * 64]
                blocks = []
                for block in range(2):
                    q_block = q_rot[block * HALF_Q:(block + 1) * HALF_Q]
                    diag = jnp.where(causal, dot_nt(k_one[block * HALF_Q:(block + 1) * HALF_Q], q_block), MASKED)
                    pieces = [diag] if block == 0 else [dot_nt(k_one[:HALF_Q], q_block), diag]
                    peak = functools.reduce(jnp.maximum, [jnp.max(piece, axis=0, keepdims=True) for piece in pieces])
                    exps = [jnp.exp2((piece - peak) * score_scale) for piece in pieces]
                    total = functools.reduce(jnp.add, [col_sum(piece) for piece in exps])
                    inverse = 1.0 / total
                    ctx = None
                    for num, piece in enumerate(exps):
                        prob = (piece * inverse).astype(BF16)
                        prob_ref[pair * 2 + head, (block + num) * HALF_Q:(block + num + 1) * HALF_Q, :] = prob
                        term = dot_nn(v_one[:, num * HALF_Q:(num + 1) * HALF_Q], prob)
                        ctx = term if ctx is None else ctx + term
                    blocks.append(ctx)
                ctx_rows.append(jnp.concatenate(blocks, axis=1))
            ctx_pair = jnp.concatenate(ctx_rows, axis=0)
            ctx_ref[:, pl.ds(pair_col, LANES)] = ctx_pair.T.astype(BF16)
        return carry

    lax.fori_loop(0, wqkv_ref.shape[1] // step, quad, 0)
    attn = dot_nt(full(ctx_ref), full(wo_ref)) + full(bo_ref)
    resid = ALPHA * full(emb_ref).astype(F32) + attn
    hat, rstd = normalize(resid)
    hat_ref[...] = hat
    rstd_ref[...] = jnp.broadcast_to(rstd, (seq_len, LANES))
    hid_ref[...] = (hat * full(gain_ref) + full(bias_ref)).astype(BF16)


def ffn_kernel(base, hid_ref, cot_ref, hat_ref, rstd_ref, wg_ref, wl_ref, wd_ref, bg_ref, bl_ref, bd_ref, gain1_ref, gain2_ref,
               *refs):
    (inner_out, gate_out, lin_out, dffn_ref, dres_ref, dattn_ref, narrow_ref, wide_ref, token_ref,
     act_buf, slope_buf, inner_buf, gate_buf, lin_buf, acc_buf, sems) = refs[-16:]
    step = pl.program_id(0)
    last = pl.num_programs(0) - 1
    clear(token_ref)
    rows, _ = hid_ref.shape
    chunks = wg_ref.shape[1] // FFN_CHUNK

    def copy_out(buf, out, kind, chunk, block):
        cols = pl.ds(pl.multiple_of(chunk * FFN_CHUNK, FFN_CHUNK), FFN_CHUNK)
        return pltpu.make_async_copy(buf.at[:, cols], out.at[pl.ds((block + base) * rows, rows), cols], sems.at[kind, chunk])

    @pl.when(step == 0)
    def _():
        clear(narrow_ref)
        clear(wide_ref)

    clear(acc_buf)

    def forward(chunk, carry):
        cols = pl.ds(pl.multiple_of(chunk * FFN_CHUNK, FFN_CHUNK), FFN_CHUNK)
        gate_pre = dot_nn(full(hid_ref), wg_ref[:, cols]) + bg_ref[:, cols]
        lin_pre = dot_nn(full(hid_ref), wl_ref[:, cols]) + bl_ref[:, cols]
        cdf = 0.5 + 0.5 * lax.erf(gate_pre * (0.5 ** 0.5))
        act = gate_pre * cdf
        pdf = jnp.exp2(gate_pre * gate_pre * (-0.5 * LOG2E)) * 0.3989422804014327
        act_buf[:, cols] = act
        slope_buf[:, cols] = lin_pre * (cdf + gate_pre * pdf)

        @pl.when(step > 0)
        def _():
            copy_out(inner_buf, inner_out, 0, chunk, step - 1).wait()

        inner = (act * lin_pre).astype(BF16)
        inner_buf[:, cols] = inner
        acc_buf[...] += dot_nt(inner, wd_ref[:, cols])
        copy_out(inner_buf, inner_out, 0, chunk, step).start()
        return carry

    lax.fori_loop(0, chunks, forward, 0)
    resid = ALPHA * full(hid_ref).astype(F32) + (full(acc_buf) + full(bd_ref))
    hat, rstd = normalize(resid)
    cot = full(cot_ref).astype(F32)
    add_sums(narrow_ref, 0, cot * hat)
    d_hat = cot * full(gain2_ref)
    d_resid = normalize_back(d_hat, hat, rstd)
    add_sums(narrow_ref, 1, d_resid)
    dffn_ref[...] = d_resid.astype(BF16)
    acc_buf[...] = ALPHA * d_resid

    def backward(chunk, carry):
        cols = pl.ds(pl.multiple_of(chunk * FFN_CHUNK, FFN_CHUNK), FFN_CHUNK)
        d_inner = dot_nn(full(dffn_ref), wd_ref[:, cols]).astype(BF16).astype(F32)
        d_gate = d_inner * slope_buf[:, cols]
        d_lin = d_inner * act_buf[:, cols]
        add_sums(wide_ref.at[:, cols], 0, d_gate)
        add_sums(wide_ref.at[:, cols], 1, d_lin)

        @pl.when(step > 0)
        def _():
            copy_out(gate_buf, gate_out, 1, chunk, step - 1).wait()
            copy_out(lin_buf, lin_out, 2, chunk, step - 1).wait()

        d_gate = d_gate.astype(BF16)
        d_lin = d_lin.astype(BF16)
        gate_buf[:, cols] = d_gate
        lin_buf[:, cols] = d_lin
        acc_buf[...] += dot_nt(d_gate, wg_ref[:, cols]) + dot_nt(d_lin, wl_ref[:, cols])
        copy_out(gate_buf, gate_out, 1, chunk, step).start()
        copy_out(lin_buf, lin_out, 2, chunk, step).start()
        return carry

    lax.fori_loop(0, chunks, backward, 0)
    d_hid = full(acc_buf)
    hat = full(hat_ref)
    add_sums(narrow_ref, 2, d_hid)
    add_sums(narrow_ref, 3, d_hid * hat)
    d_hat = d_hid * full(gain1_ref)
    d_resid = normalize_back(d_hat, hat, rstd_ref[:, :1])
    add_sums(narrow_ref, 4, d_resid)
    dres_ref[...] = d_resid
    dattn_ref[...] = d_resid.astype(BF16)

    @pl.when(step == last)
    def _():
        def drain(chunk, carry):
            copy_out(inner_buf, inner_out, 0, chunk, step).wait()
            copy_out(gate_buf, gate_out, 1, chunk, step).wait()
            copy_out(lin_buf, lin_out, 2, chunk, step).wait()
            return carry

        lax.fori_loop(0, chunks, drain, 0)


def attn_backward_kernel(head_dim, alias_count, *refs):
    (dres_ref, dattn_ref, qkv_ref, prob_ref, wqkv_ref, wo_ref, cos_ref, sin_ref) = refs[:8]
    (demb_ref, dqkv_ref, dall_ref, acc_ref, token_ref) = refs[8 + alias_count:]
    clear(token_ref)
    width = dres_ref.shape[1]
    low, mask_low, mask_high, first_half = lane_masks()
    attn_scale = head_dim ** -0.5
    step = 4 * 3 * head_dim

    @pl.when(pl.program_id(0) == 0)
    def _():
        clear(acc_ref)

    def quad(index, carry):
        col = pl.multiple_of(index * step, step)
        ctx_row = pl.multiple_of(index * 4 * head_dim, 4 * head_dim)
        d_ctx_quad = dot_nn(full(dattn_ref), wo_ref[:, pl.ds(ctx_row, 4 * head_dim)]).astype(BF16)
        pieces = []
        for half in range(2):
            pair = index * 2 + half
            pair_col = pl.multiple_of(pair * LANES, LANES)
            d_ctx = d_ctx_quad[:, half * LANES:(half + 1) * LANES]
            q_rot = qkv_ref[:, pl.ds(pair_col, LANES)]
            k_rot = qkv_ref[:, pl.ds(width + pair_col, LANES)]
            v_pair = qkv_ref[:, pl.ds(2 * width + pair_col, LANES)]
            k_trans = k_rot.astype(F32).T.astype(BF16)
            dq_rows, dk_heads, dv_heads = [], [], []
            for head in range(2):
                v_one = v_pair * (mask_low if head == 0 else mask_high)
                k_one = k_trans[head * 64:(head + 1) * 64]
                d_v, d_k, d_q = [None, None], [None, None], []
                for block in range(2):
                    rows = slice(block * HALF_Q, (block + 1) * HALF_Q)
                    keys = range(block + 1)
                    probs = [prob_ref[pair * 2 + head, (block + num) * HALF_Q:(block + num + 1) * HALF_Q, :] for num in keys]
                    d_probs = [dot_nt(v_one[num * HALF_Q:(num + 1) * HALF_Q], d_ctx[rows]) for num in keys]
                    wide = [prob.astype(F32) for prob in probs]
                    inner = functools.reduce(jnp.add, [col_sum(d_prob * prob) for d_prob, prob in zip(d_probs, wide)])
                    d_q_block = None
                    for num in keys:
                        d_score = (wide[num] * (d_probs[num] - inner) * attn_scale).astype(BF16)
                        terms = (dot_nn(probs[num], d_ctx[rows]), dot_nn(d_score, q_rot[rows]), dot_nn(k_one[:, num * HALF_Q:(num + 1) * HALF_Q], d_score))
                        d_v[num] = terms[0] if d_v[num] is None else d_v[num] + terms[0]
                        d_k[num] = terms[1] if d_k[num] is None else d_k[num] + terms[1]
                        d_q_block = terms[2] if d_q_block is None else d_q_block + terms[2]
                    d_q.append(d_q_block)
                dq_rows.append(jnp.concatenate(d_q, axis=1))
                dk_heads.append(jnp.concatenate(d_k, axis=0))
                dv_heads.append(jnp.concatenate(d_v, axis=0))
            d_q = rope(jnp.concatenate(dq_rows, axis=0).T, full(cos_ref), -full(sin_ref), first_half)
            d_k = rope(jnp.where(low, dk_heads[0], dk_heads[1]), full(cos_ref), -full(sin_ref), first_half)
            d_v = jnp.where(low, dv_heads[0], dv_heads[1])
            d_k = pltpu.roll(d_k, 64, 1)
            pieces += [jnp.where(low, d_q, d_k), jnp.where(low, d_v, d_q), jnp.where(low, d_k, d_v)]
        for num, piece in enumerate(pieces):
            lanes = pl.ds(col + num * LANES, LANES)
            acc_ref[:, lanes] += row_sums(piece)
            dqkv_ref[:, lanes] = piece.astype(BF16)
        return carry

    lax.fori_loop(0, wqkv_ref.shape[1] // step, quad, 0)
    d_emb = SHRINK * (ALPHA * full(dres_ref) + dot_nt(full(dqkv_ref), full(wqkv_ref)))
    demb_ref[...] = d_emb
    dall_ref[...] = d_emb


def whole(shape):
    return pl.BlockSpec(shape, lambda i: (0,) * len(shape), pipeline_mode=pl.Buffered(1))


def per_seq(shape, base=0):
    return pl.BlockSpec((None,) + tuple(shape), lambda i: (i + base,) + (0,) * len(shape))


def cost(flops, moved):
    return pl.CostEstimate(flops=flops, bytes_accessed=moved, transcendentals=0)


def params():
    return pltpu.CompilerParams(dimension_semantics=('arbitrary',), vmem_limit_bytes=VMEM_LIMIT)


TOKEN = (8, LANES)
ANYWHERE = pl.BlockSpec(memory_space=pl.ANY)


def token_spec():
    return pl.BlockSpec(TOKEN, lambda i: (0, 0))


def attn_forward(base, count, total, own, other, weights, tables, previous, deps, head_dim):
    seq_len, width = own.shape[1:]
    wqkv = weights[0]
    heads = width // head_dim
    shapes = [((seq_len, width), BF16), ((seq_len, 3 * width), BF16), ((heads, seq_len * 3 // 2, HALF_Q), BF16), ((seq_len, width), BF16),
              ((seq_len, width), F32), ((seq_len, LANES), F32), ((seq_len, width), BF16)]
    operands = (own, other) + tuple(weights) + tuple(tables)
    specs = [per_seq((seq_len, width), base), per_seq((seq_len, width))] + [whole(item.shape) for item in operands[2:]]
    extra = tuple(previous) if previous is not None else ()
    specs += [ANYWHERE] * (len(extra) + len(deps))
    flops = count * (2 * seq_len * width * (wqkv.shape[1] + width) + 4 * heads * seq_len * seq_len * 64)
    return pl.pallas_call(
        functools.partial(attn_forward_kernel, head_dim, len(extra) + len(deps)),
        grid=(count,),
        in_specs=specs,
        out_specs=[per_seq(shape, base) for shape, _ in shapes] + [token_spec()],
        out_shape=[jax.ShapeDtypeStruct((total,) + shape, dtype) for shape, dtype in shapes] + [jax.ShapeDtypeStruct(TOKEN, F32)],
        input_output_aliases={len(operands) + num: num for num in range(len(extra))},
        compiler_params=params(),
        cost_estimate=cost(2 * flops, count * 12_000_000),
        name='attn_forward',
    )(*operands, *extra, *deps)


def ffn(base, count, hidden, cotangent, hat, rstd, weights, previous, deps):
    total, seq_len, width = hidden.shape
    wide = weights[0].shape[1]
    operands = (hidden, cotangent, hat, rstd) + tuple(weights)
    extra = tuple(previous) if previous is not None else ()
    specs = [per_seq(item.shape[1:], base) for item in operands[:4]] + [whole(item.shape) for item in operands[4:]]
    specs += [ANYWHERE] * (len(extra) + len(deps))
    big = jax.ShapeDtypeStruct((total * seq_len, wide), BF16)
    narrow = jax.ShapeDtypeStruct((total, seq_len, width), BF16)
    flops = 12 * count * seq_len * width * wide
    return pl.pallas_call(
        functools.partial(ffn_kernel, base),
        grid=(count,),
        in_specs=specs,
        out_specs=[ANYWHERE] * 3 + [per_seq((seq_len, width), base)] * 3 + [pl.BlockSpec((40, width), lambda i: (0, 0)), pl.BlockSpec((16, wide), lambda i: (0, 0)), token_spec()],
        out_shape=[big] * 3 + [narrow, jax.ShapeDtypeStruct((total, seq_len, width), F32), narrow,
                               jax.ShapeDtypeStruct((40, width), F32), jax.ShapeDtypeStruct((16, wide), F32), jax.ShapeDtypeStruct(TOKEN, F32)],
        scratch_shapes=[pltpu.VMEM((seq_len, wide), F32)] * 2 + [pltpu.VMEM((seq_len, wide), BF16)] * 3
        + [pltpu.VMEM((seq_len, width), F32), pltpu.SemaphoreType.DMA((3, wide // FFN_CHUNK))],
        input_output_aliases={len(operands) + num: num for num in range(len(extra))},
        compiler_params=params(),
        cost_estimate=cost(int(1.5 * flops), count * 14_000_000),
        name='ffn',
    )(*operands, *extra, *deps)


def attn_backward(base, count, total, d_resid, d_attn, qkv, probs, weights, tables, previous, deps, head_dim):
    seq_len, width = d_resid.shape[1:]
    wqkv, wout = weights
    heads = width // head_dim
    operands = (d_resid, d_attn, qkv, probs, wqkv, wout) + tuple(tables)
    specs = [per_seq(item.shape[1:], base) for item in operands[:4]] + [whole(item.shape) for item in operands[4:]]
    extra = tuple(previous) if previous is not None else ()
    specs += [ANYWHERE] * (len(extra) + len(deps))
    flops = count * (2 * seq_len * width * (wqkv.shape[1] + width) + 8 * heads * seq_len * seq_len * 64)
    return pl.pallas_call(
        functools.partial(attn_backward_kernel, head_dim, len(extra) + len(deps)),
        grid=(count,),
        in_specs=specs,
        out_specs=[per_seq((seq_len, width)), per_seq((seq_len, wqkv.shape[1]), base), per_seq((seq_len, width), base), pl.BlockSpec((8, wqkv.shape[1]), lambda i: (0, 0)), token_spec()],
        out_shape=[jax.ShapeDtypeStruct((count, seq_len, width), F32), jax.ShapeDtypeStruct((total, seq_len, wqkv.shape[1]), BF16),
                   jax.ShapeDtypeStruct((total, seq_len, width), F32),
                   jax.ShapeDtypeStruct((8, wqkv.shape[1]), F32), jax.ShapeDtypeStruct(TOKEN, F32)],
        input_output_aliases={len(operands) + num: 1 + num for num in range(len(extra))},
        compiler_params=params(),
        cost_estimate=cost(2 * flops, count * 12_000_000),
        name='attn_backward',
    )(*operands, *extra, *deps)


def outer_kernel(left_ref, right_ref, *refs):
    out_ref, token_ref, left_t = refs[-3:]
    clear(token_ref)

    @pl.when(pl.program_id(0) == 0)
    def _():
        def turn(index, carry):
            rows = pl.ds(pl.multiple_of(index * CHUNK, CHUNK), CHUNK)
            left_t[:, rows] = left_ref[rows, :].astype(F32).T.astype(BF16)
            return carry

        lax.fori_loop(0, left_ref.shape[0] // CHUNK, turn, 0)

    out_ref[...] = dot_nn(full(left_t), full(right_ref))


def outer(left, right, block, shape, slot, previous, deps):
    rows, width = left.shape
    wide = right.shape[1]
    per_half = wide // (2 * block)
    half_blocks = shape[1] // (2 * block)
    extra = (previous,) if previous is not None else ()
    return pl.pallas_call(
        outer_kernel,
        grid=(wide // block,),
        in_specs=[whole((rows, width)), pl.BlockSpec((rows, block), lambda i: (0, i))] + [ANYWHERE] * (len(extra) + len(deps)),
        out_specs=[pl.BlockSpec((width, block), lambda i: (0, slot + i % per_half + half_blocks * (i // per_half))), token_spec()],
        out_shape=[jax.ShapeDtypeStruct(shape, F32), jax.ShapeDtypeStruct(TOKEN, F32)],
        input_output_aliases={2 + num: num for num in range(len(extra))},
        scratch_shapes=[pltpu.VMEM((width, rows), BF16)],
        compiler_params=params(),
        cost_estimate=cost(2 * rows * width * wide, 4 * width * wide + 2 * rows * (width + wide)),
        name='outer',
    )(left, right, *extra, *deps)


def join_kernel(plain, peer_ref, *refs):
    owns, outs = refs[:len(refs) // 2], refs[len(refs) // 2:]
    start = 0
    for num, (own_ref, out_ref) in enumerate(zip(owns, outs)):
        half = out_ref.shape[1] // 2
        out_ref[:, :half] = full(own_ref) if num < plain else full(own_ref).astype(F32).T.astype(BF16)
        out_ref[:, half:] = peer_ref[:, start:start + half].astype(BF16)
        start += half


def join(peer, plain, flipped):
    owns = tuple(plain) + tuple(flipped)
    rows = peer.shape[0]
    halves = [item.shape[1] for item in plain] + [item.shape[0] for item in flipped]
    return pl.pallas_call(
        functools.partial(join_kernel, len(plain)),
        grid=(rows // LANES,),
        in_specs=[pl.BlockSpec((LANES, peer.shape[1]), lambda i: (i, 0))] + [pl.BlockSpec((LANES, item.shape[1]), lambda i: (i, 0)) for item in plain]
        + [pl.BlockSpec((item.shape[0], LANES), lambda i: (0, i)) for item in flipped],
        out_specs=[pl.BlockSpec((LANES, 2 * half), lambda i: (i, 0)) for half in halves],
        out_shape=[jax.ShapeDtypeStruct((rows, 2 * half), BF16) for half in halves],
        compiler_params=params(),
        cost_estimate=cost(peer.size * 64, peer.size * 10),
        name='join_weights',
    )(peer, *owns)


def shared_slice(plain, flipped, index, parts):
    rows = plain[0].shape[0] // parts
    pieces = [lax.dynamic_slice_in_dim(item, index * rows, rows, 0) for item in plain]
    pieces += [lax.dynamic_slice_in_dim(item, index * rows, rows, 1).T for item in flipped]
    return jnp.concatenate(pieces, axis=1).astype(F32)


def row_pieces(rows):
    tiles = rows // TILE
    cuts = [num * tiles // PIECES * TILE for num in range(PIECES + 1)]
    return [(first, last - first) for first, last in zip(cuts, cuts[1:])]


def table_kernel(src, out, away, keep, got_one, got_two, stage, load_sems, store_sems, swap_sems, one_sems, two_sems, near_sems, far_sems, back_sems):
    me = lax.axis_index('dp')
    core, col, line = me % 2, me // 2 % 2, me // 4
    partner, x_peer, y_peer = me + 1 - 2 * core, me + 2 - 4 * col, me + 4 - 8 * line
    first_peer = x_peer + core * (y_peer - x_peer)
    second_peer = y_peer + core * (x_peer - y_peer)
    one = col + core * (line - col)
    two = line + core * (col - line)
    eighth = src.shape[0] // 8
    pieces = row_pieces(eighth)
    jobs = [(part, num) for part in range(4) for num in range(PIECES)]

    barrier = pltpu.get_barrier_semaphore()
    for peer in (partner, x_peer, y_peer):
        pl.semaphore_signal(barrier, inc=1, device_id={'dp': peer}, device_id_type=pl.DeviceIdType.MESH)
    pl.semaphore_wait(barrier, 3)

    def send(source, target, sems, slot, peer):
        return pltpu.make_async_remote_copy(src_ref=source, dst_ref=target, send_sem=sems.at[0, slot], recv_sem=sems.at[1, slot],
                                            device_id={'dp': peer}, device_id_type=pl.DeviceIdType.MESH)

    def table_rows(ref, half, quarter, last, num):
        start, size = pieces[num]
        return ref.at[pl.ds(pl.multiple_of((half * 4 + quarter * 2 + last) * eighth + start, TILE), size)]

    def part_rows(ref, half, quarter, last, part, num):
        return table_rows(ref, half, 1 - quarter if part < 2 else quarter, last if part % 2 else 1 - last, num)

    def buffer_rows(ref, part, num):
        start, size = pieces[num]
        return ref.at[pl.ds(part % 2 * eighth + start, size)]

    def holder(part):
        return away if part < 2 else keep

    def add_into(target, part, source, source_part, num):
        start, size = pieces[num]
        to, of = part % 2 * eighth + start, source_part * eighth + start

        def body(index, carry):
            offset = index * TILE
            target[pl.ds(pl.multiple_of(to + offset, TILE), TILE)] += source[pl.ds(pl.multiple_of(of + offset, TILE), TILE)]
            return carry

        lax.fori_loop(0, size // TILE, body, 0)

    swaps = [send(part_rows(src, 1 - core, two, one, part, num), buffer_rows(holder(part), part, num), swap_sems, slot, partner)
             for slot, (part, num) in enumerate(jobs)]
    loads = [pltpu.make_async_copy(part_rows(src, core, one, two, part, num), stage.at[slot % 2, pl.ds(0, pieces[num][1])], load_sems.at[slot % 2])
             for slot, (part, num) in enumerate(jobs)]
    firsts = [send(buffer_rows(away, part, num), buffer_rows(got_one, part, num), one_sems, slot, first_peer)
              for slot, (part, num) in enumerate(jobs[:2 * PIECES])]
    seconds = [send(buffer_rows(keep, 0, num), buffer_rows(got_two, 0, num), two_sems, num, second_peer) for num in range(PIECES)]

    for copy in swaps:
        copy.start()
    loads[0].start()
    for slot, (part, num) in enumerate(jobs):
        if slot + 1 < len(jobs):
            loads[slot + 1].start()
        loads[slot].wait()
        swaps[slot].wait_recv()
        start, size = pieces[num]
        target, held, to = holder(part), stage.at[slot % 2], part % 2 * eighth + start

        def body(index, carry, target=target, held=held, to=to):
            offset = index * TILE
            target[pl.ds(pl.multiple_of(to + offset, TILE), TILE)] += held[pl.ds(pl.multiple_of(offset, TILE), TILE)]
            return carry

        lax.fori_loop(0, size // TILE, body, 0)
        if 0 < slot <= len(firsts):
            firsts[slot - 1].start()

    for slot in range(2 * PIECES):
        firsts[slot].wait_recv()
        add_into(keep, slot // PIECES, got_one, slot // PIECES, slot % PIECES)
        if 0 < slot <= PIECES:
            seconds[slot - 1].start()

    done = []

    def publish(num):
        mine = buffer_rows(keep, 1, num)
        place = table_rows(out, core, one, two, num)
        copies = [pltpu.make_async_copy(mine, place, store_sems.at[num]), send(mine, place, near_sems, num, second_peer),
                  send(mine, place, far_sems, num, first_peer), send(mine, place, back_sems, num, partner)]
        for copy in copies:
            copy.start()
        done.append(copies)

    for num in range(PIECES):
        seconds[num].wait_recv()
        add_into(keep, 1, got_two, 0, num)
        if num:
            publish(num - 1)
    publish(PIECES - 1)

    def forward(quarter, last, num, sems, slot, peer, start=True):
        place = table_rows(out, core, quarter, last, num)
        copy = send(place, place, sems, slot, peer)
        if start:
            copy.start()
        return copy

    relays = []
    for num in range(PIECES):
        forward(one, 1 - two, num, near_sems, num, second_peer, False).wait_recv()
        relays.append(forward(one, 1 - two, num, far_sems, PIECES + num, first_peer))
        relays.append(forward(one, 1 - two, num, back_sems, PIECES + num, partner))
        forward(1 - one, two, num, far_sems, num, first_peer, False).wait_recv()
        relays.append(forward(1 - one, two, num, back_sems, 2 * PIECES + num, partner))
    for num in range(PIECES):
        forward(1 - one, 1 - two, num, far_sems, PIECES + num, first_peer, False).wait_recv()
        relays.append(forward(1 - one, 1 - two, num, back_sems, 3 * PIECES + num, partner))
    for slot, (part, num) in enumerate(jobs):
        place = table_rows(out, 1 - core, two if part < 2 else 1 - two, 1 - one if part % 2 else one, num)
        send(place, place, back_sems, slot, partner).wait_recv()
    for copy in swaps + firsts + seconds + relays:
        copy.wait_send()
    for local, *remote in done:
        local.wait()
        for copy in remote:
            copy.wait_send()


def reduce_table(table):
    rows, width = table.shape
    eighth = rows // 8
    largest = max(size for _, size in row_pieces(eighth))
    buffers = [pltpu.VMEM((count * eighth, width), F32) for count in (2, 2, 2, 1)]
    counts = (4 * PIECES, 2 * PIECES, PIECES, PIECES, 2 * PIECES, 4 * PIECES)
    return pl.pallas_call(
        table_kernel,
        in_specs=[ANYWHERE],
        out_specs=ANYWHERE,
        out_shape=jax.ShapeDtypeStruct(table.shape, F32),
        scratch_shapes=buffers + [pltpu.VMEM((2, largest, width), F32), pltpu.SemaphoreType.DMA((2,)), pltpu.SemaphoreType.DMA((PIECES,))]
        + [pltpu.SemaphoreType.DMA((2, count)) for count in counts],
        compiler_params=pltpu.CompilerParams(collective_id=0, has_side_effects=True, vmem_limit_bytes=VMEM_LIMIT),
        cost_estimate=cost(400_000_000_000, rows * width * 8),
        name='reduce_table',
    )(table)


def reduce_gradient(grad):
    piece = lax.psum_scatter(grad, 'dp', scatter_dimension=0, tiled=True)
    half = piece.shape[1] // 2
    other = lax.ppermute(piece[:, half:], 'tp', SWAP)
    return lax.all_gather(piece[:, :half] + other, 'dp', axis=0, tiled=True)


def tie(value, token):
    return lax.optimization_barrier((value, token))[0]


def solution(mesh):
    in_specs = (P('dp'), P('dp'), ROWS) + WEIGHT_SPECS
    out_specs = (ROWS,) + WEIGHT_SPECS
    parts = mesh.shape['dp']

    def device_step(tokens, cotangent, emb_table, *weights):
        (w_qkv, b_qkv, w_out, b_out, ln1_gain, ln1_bias, w_gate, b_gate, w_lin, b_lin, w_down, b_down, ln2_gain) = weights
        tp_index, dp_index = lax.axis_index('tp'), lax.axis_index('dp')
        vocab_loc, width = emb_table.shape
        head_dim = b_qkv.shape[1] // 3
        seq_len = tokens.shape[1]
        total = tokens.shape[0] // 2

        local_ids = tokens - tp_index * vocab_loc
        in_shard = (local_ids >= 0) & (local_ids < vocab_loc)
        own_ids = lax.dynamic_slice_in_dim(local_ids, tp_index * total, total)
        own_in = lax.dynamic_slice_in_dim(in_shard, tp_index * total, total)
        peer_ids = lax.dynamic_slice_in_dim(local_ids, (1 - tp_index) * total, total)
        peer_in = lax.dynamic_slice_in_dim(in_shard, (1 - tp_index) * total, total)
        own_cot = lax.dynamic_slice_in_dim(cotangent, tp_index * total, total)

        def rows_of(ids, inside):
            rows = jnp.take(emb_table, jnp.where(inside, ids, 0), axis=0)
            return jnp.where(inside[:, :, None], rows, 0.0)

        def exchange(value):
            return lax.ppermute(value, 'tp', SWAP)

        def collect(value):
            value = exchange(value)
            return lax.all_gather(value, 'dp', axis=0, tiled=True)

        def row_of(vector):
            return vector.astype(F32).reshape(1, -1)

        size = total // 4
        qkv_loc, wide_loc = b_qkv.size, b_gate.shape[0]
        first = rows_of(peer_ids[:size], peer_in[:size]).astype(F32)
        rest = rows_of(peer_ids[size:], peer_in[size:]).astype(F32)
        own_rows = rows_of(own_ids, own_in)
        front_peer = collect(shared_slice((w_qkv,), (w_out,), dp_index, parts))
        wide_peer = collect(shared_slice((w_gate, w_lin), (w_down,), dp_index, parts))
        arrived = [exchange(first)] + [exchange(rest[num * size:(num + 1) * size]) for num in range(3)]
        own_bias = jnp.concatenate([row_of(b_qkv), row_of(b_gate), row_of(b_lin)], axis=1)
        biases = jnp.concatenate([own_bias, exchange(own_bias)])
        bqkv_full = biases[:, :qkv_loc].reshape(1, -1)
        bgate_full = biases[:, qkv_loc:qkv_loc + wide_loc].reshape(1, -1)
        blin_full = biases[:, qkv_loc + wide_loc:].reshape(1, -1)
        wqkv_full, wout_full = join(front_peer, (w_qkv,), (w_out,))
        wide_full = join(wide_peer, (w_gate, w_lin), (w_down,))

        half_dim = head_dim // 2
        inv_freq = ROPE_BASE ** (-2.0 * jnp.arange(half_dim, dtype=F32) / head_dim)
        angles = jnp.arange(seq_len, dtype=F32)[:, None] * inv_freq[None, :]
        cos_half, sin_half = jnp.cos(angles), jnp.sin(angles)
        tables = (jnp.concatenate([cos_half] * 4, axis=1), jnp.concatenate([-sin_half, sin_half] * 2, axis=1))

        front = (wqkv_full, bqkv_full, wout_full, row_of(b_out), row_of(ln1_gain), row_of(ln1_bias))
        middle = tuple(wide_full) + (bgate_full, blin_full, row_of(b_down), row_of(ln1_gain), row_of(ln2_gain))
        saved, ffn_saved, d_kept, deps = None, None, None, ()
        narrow_parts, wide_parts, bias_parts, d_peer = [], [], [], []

        def run_attention(num):
            nonlocal saved, deps
            out = attn_forward(num * size, size, total, own_rows, arrived[num], front, tables, saved, deps, head_dim)
            *kept, token = out
            saved, deps = kept, (token,)

        def run_ffn(base, count):
            nonlocal ffn_saved, deps
            *_, hat, rstd, hidden = saved
            *kept, narrow, wide, token = ffn(base, count, hidden, own_cot, hat, rstd, middle, ffn_saved, deps)
            ffn_saved, deps = kept, (token,)
            narrow_parts.append(narrow)
            wide_parts.append(wide)

        def run_backward(base, count):
            nonlocal d_kept, deps
            _, qkv, probs, *_ = saved
            *_, d_resid, d_attn = ffn_saved
            d_emb, d_qkv, d_all, bias_part, token = attn_backward(base, count, total, d_resid, d_attn, qkv, probs, (wqkv_full, wout_full), tables, d_kept, deps, head_dim)
            d_kept, deps = (d_qkv, d_all), (token,)
            bias_parts.append(bias_part)
            d_peer.append(exchange(d_emb))

        def run_outer(left, right, block, shape, slot, previous):
            nonlocal deps
            out, token = outer(left.reshape(-1, left.shape[-1]), right.reshape(-1, right.shape[-1]), block, shape, slot, previous, deps)
            deps = (token,)
            return out

        run_attention(0)
        run_attention(1)
        run_ffn(0, 2 * size)
        run_attention(2)
        run_attention(3)
        run_backward(0, 2 * size)
        run_ffn(2 * size, 2 * size)
        inner, d_gate, d_lin, d_ffn, _, d_attn = ffn_saved
        emb, _, _, context, _, _, hidden = saved
        shape = (width, 6 * wide_loc)
        step = wide_loc // CHUNK
        grads = run_outer(hidden, d_gate, CHUNK, shape, 0, None)
        grads = run_outer(hidden, d_lin, CHUNK, shape, step, grads)
        grads = run_outer(d_ffn, inner, CHUNK, shape, 2 * step, grads)
        wide_grads = reduce_gradient(grads)
        run_backward(2 * size, size)
        run_backward(3 * size, size)
        block = w_out.shape[0]
        shape = (width + parts * TILE, 2 * (qkv_loc + block))
        d_qkv, d_all = d_kept
        grads = run_outer(d_attn, context, block, shape, qkv_loc // block, None)
        grads = run_outer(emb, d_qkv, block, shape, 0, grads)

        narrow = jnp.sum(sum(narrow_parts).reshape(5, 8, -1), axis=1).reshape(1, -1)
        d_bwide = jnp.sum(sum(wide_parts).reshape(2, 8, -1), axis=1).reshape(2, 2, -1)
        small = jnp.concatenate([jnp.sum(sum(bias_parts), axis=0).reshape(2, -1), d_bwide[0], d_bwide[1], jnp.concatenate([narrow] * 2)], axis=1)
        used = small.shape[1]
        small = jnp.pad(small, ((0, 0), (0, TILE * (qkv_loc + block) - used))).reshape(2, TILE, -1)
        grads = lax.dynamic_update_slice(grads, jnp.concatenate([small[0], small[1]], axis=1), (width, 0))
        front_grads = reduce_gradient(grads)

        own_row_ids = jnp.where(own_in, own_ids, vocab_loc)
        peer_row_ids = jnp.where(peer_in, peer_ids, vocab_loc)

        def add_rows(grad, ids, rows):
            return grad.at[ids.reshape(-1)].add(rows.reshape(-1, width), mode='drop')

        d_table = add_rows(jnp.zeros((vocab_loc, width), F32), tie(own_row_ids, *deps), d_all)
        d_table = add_rows(d_table, peer_row_ids, jnp.concatenate(d_peer, axis=0))
        d_table = reduce_table(d_table)

        small = front_grads[width:width + TILE].reshape(-1)
        d_b_qkv = small[:qkv_loc].reshape(b_qkv.shape)
        d_b_gate = small[qkv_loc:qkv_loc + wide_loc]
        d_b_lin = small[qkv_loc + wide_loc:qkv_loc + 2 * wide_loc]
        d_ln2_gain, d_b_down, d_ln1_bias, d_ln1_gain, d_b_out = small[qkv_loc + 2 * wide_loc:used].reshape(5, width)
        d_w_gate, d_w_lin, d_w_down = (wide_grads[:, num * wide_loc:(num + 1) * wide_loc] for num in range(3))
        d_w_qkv, d_w_out = front_grads[:width, :qkv_loc], front_grads[:width, qkv_loc:]
        return (d_table, d_w_qkv, d_b_qkv, d_w_out.T, d_b_out, d_ln1_gain, d_ln1_bias, d_w_gate, d_b_gate, d_w_lin, d_b_lin, d_w_down.T, d_b_down, d_ln2_gain)

    return jax.shard_map(device_step, mesh=mesh, in_specs=in_specs, out_specs=out_specs, check_vma=False)
```

```python
import functools

import jax
import jax.numpy as jnp
from jax import lax
from jax.experimental import pallas as pl
from jax.experimental.pallas import tpu as pltpu
from jax.sharding import PartitionSpec as P


ALPHA = 140.0 ** 0.5
EPS = 1e-5
SHRINK = 0.1
ROPE_BASE = 10000.0
COLS, ROWS, ALL = P(None, 'tp'), P('tp'), P()
WEIGHT_SPECS = (COLS, ROWS, ROWS, ALL, ALL, ALL, COLS, ROWS, COLS, ROWS, ROWS, ALL, ALL)

F32 = jnp.float32
BF16 = jnp.bfloat16
LANES = 128
HALF_Q = 256
CHUNK = 512
FFN_CHUNK = 768
TILE = 8
PIECES = 3
VMEM_LIMIT = 66 * 1024 * 1024 - 512 * 1024
LOG2E = 1.4426950408889634
MASKED = -8e30
NT = (((1,), (1,)), ((), ()))
NN = (((1,), (0,)), ((), ()))
SWAP = ((0, 1), (1, 0))


def dot_nn(left, right):
    return lax.dot_general(left, right, NN, preferred_element_type=F32)


def dot_nt(left, right):
    return lax.dot_general(left, right, NT, preferred_element_type=F32)


def row_sums(values):
    return jnp.sum(values.reshape(-1, TILE, values.shape[1]), axis=0)


def row_mean(values):
    return jnp.mean(values, axis=-1, keepdims=True)


def col_sum(values):
    return jnp.sum(values, axis=0, keepdims=True)


def add_sums(ref, slot, values):
    ref[slot * TILE:(slot + 1) * TILE] += row_sums(values)


def full(ref):
    return ref[...]


def clear(ref):
    ref[...] = jnp.zeros_like(ref)


def normalize(values):
    centered = values - row_mean(values)
    rstd = lax.rsqrt(row_mean(centered * centered) + EPS)
    return centered * rstd, rstd


def normalize_back(d_hat, hat, rstd):
    return rstd * (d_hat - row_mean(d_hat) - hat * row_mean(d_hat * hat))


def rope(values, cos_tab, sin_tab, first_half):
    partner = jnp.where(first_half, pltpu.roll(values, 96, 1), pltpu.roll(values, 32, 1))
    return values * cos_tab + partner * sin_tab


def lane_masks():
    lane = lax.broadcasted_iota(jnp.int32, (1, LANES), 1)
    low = lane < 64
    return low, low.astype(F32).astype(BF16), (1.0 - low.astype(F32)).astype(BF16), (lane % 64) < 32


def attn_forward_kernel(head_dim, alias_count, *refs):
    (own_ref, other_ref, wqkv_ref, bqkv_ref, wo_ref, bo_ref, gain_ref, bias_ref, cos_ref, sin_ref) = refs[:10]
    (emb_ref, qkv_ref, prob_ref, ctx_ref, hat_ref, rstd_ref, hid_ref, token_ref) = refs[10 + alias_count:]
    seq_len, width = own_ref.shape
    clear(token_ref)
    emb_ref[...] = (full(own_ref).astype(F32) + full(other_ref)).astype(BF16)
    low, mask_low, mask_high, first_half = lane_masks()
    score_scale = head_dim ** -0.5 * LOG2E
    causal = lax.broadcasted_iota(jnp.int32, (HALF_Q, HALF_Q), 0) <= lax.broadcasted_iota(jnp.int32, (HALF_Q, HALF_Q), 1)
    step = 4 * 3 * head_dim

    def quad(index, carry):
        col = pl.multiple_of(index * step, step)
        pre = dot_nn(full(emb_ref), wqkv_ref[:, pl.ds(col, step)]) + bqkv_ref[:, pl.ds(col, step)]
        pre = pre.astype(BF16).astype(F32)
        for half in range(2):
            parts = [pre[:, (half * 3 + part) * LANES:(half * 3 + part + 1) * LANES] for part in range(3)]
            pair = index * 2 + half
            pair_col = pl.multiple_of(pair * LANES, LANES)
            q_pair = jnp.where(low, parts[0], parts[1])
            k_pair = pltpu.roll(jnp.where(low, parts[2], parts[0]), 64, 1)
            v_pair = jnp.where(low, parts[1], parts[2])
            q_rot = rope(q_pair, full(cos_ref), full(sin_ref), first_half).astype(BF16)
            k_rot = rope(k_pair, full(cos_ref), full(sin_ref), first_half).astype(BF16)
            qkv_ref[:, pl.ds(pair_col, LANES)] = q_rot
            qkv_ref[:, pl.ds(width + pair_col, LANES)] = k_rot
            qkv_ref[:, pl.ds(2 * width + pair_col, LANES)] = v_pair.astype(BF16)
            v_trans = v_pair.T.astype(BF16)
            ctx_rows = []
            for head in range(2):
                k_one = k_rot * (mask_low if head == 0 else mask_high)
                v_one = v_trans[head * 64:(head + 1) * 64]
                blocks = []
                for block in range(2):
                    q_block = q_rot[block * HALF_Q:(block + 1) * HALF_Q]
                    diag = jnp.where(causal, dot_nt(k_one[block * HALF_Q:(block + 1) * HALF_Q], q_block), MASKED)
                    pieces = [diag] if block == 0 else [dot_nt(k_one[:HALF_Q], q_block), diag]
                    peak = functools.reduce(jnp.maximum, [jnp.max(piece, axis=0, keepdims=True) for piece in pieces])
                    exps = [jnp.exp2((piece - peak) * score_scale) for piece in pieces]
                    total = functools.reduce(jnp.add, [col_sum(piece) for piece in exps])
                    inverse = 1.0 / total
                    ctx = None
                    for num, piece in enumerate(exps):
                        prob = (piece * inverse).astype(BF16)
                        prob_ref[pair * 2 + head, (block + num) * HALF_Q:(block + num + 1) * HALF_Q, :] = prob
                        term = dot_nn(v_one[:, num * HALF_Q:(num + 1) * HALF_Q], prob)
                        ctx = term if ctx is None else ctx + term
                    blocks.append(ctx)
                ctx_rows.append(jnp.concatenate(blocks, axis=1))
            ctx_pair = jnp.concatenate(ctx_rows, axis=0)
            ctx_ref[:, pl.ds(pair_col, LANES)] = ctx_pair.T.astype(BF16)
        return carry

    lax.fori_loop(0, wqkv_ref.shape[1] // step, quad, 0)
    attn = dot_nt(full(ctx_ref), full(wo_ref)) + full(bo_ref)
    resid = ALPHA * full(emb_ref).astype(F32) + attn
    hat, rstd = normalize(resid)
    hat_ref[...] = hat
    rstd_ref[...] = jnp.broadcast_to(rstd, (seq_len, LANES))
    hid_ref[...] = (hat * full(gain_ref) + full(bias_ref)).astype(BF16)


def ffn_kernel(base, hid_ref, cot_ref, hat_ref, rstd_ref, wg_ref, wl_ref, wd_ref, bg_ref, bl_ref, bd_ref, gain1_ref, gain2_ref,
               *refs):
    (inner_out, gate_out, lin_out, dffn_ref, dres_ref, dattn_ref, narrow_ref, wide_ref, token_ref,
     act_buf, slope_buf, inner_buf, gate_buf, lin_buf, acc_buf, sems) = refs[-16:]
    step = pl.program_id(0)
    last = pl.num_programs(0) - 1
    clear(token_ref)
    rows, _ = hid_ref.shape
    chunks = wg_ref.shape[1] // FFN_CHUNK

    def copy_out(buf, out, kind, chunk, block):
        cols = pl.ds(pl.multiple_of(chunk * FFN_CHUNK, FFN_CHUNK), FFN_CHUNK)
        return pltpu.make_async_copy(buf.at[:, cols], out.at[pl.ds((block + base) * rows, rows), cols], sems.at[kind, chunk])

    @pl.when(step == 0)
    def _():
        clear(narrow_ref)
        clear(wide_ref)

    outputs = ((inner_buf, inner_out, 0), (gate_buf, gate_out, 1), (lin_buf, lin_out, 2))

    def drain(copies, block):
        def body(chunk, carry):
            for buf, out, kind in copies:
                copy_out(buf, out, kind, chunk, block).wait()
            return carry

        lax.fori_loop(0, chunks, body, 0)

    @pl.when(step > 0)
    def _():
        drain(outputs, step - 1)

    clear(acc_buf)

    def forward(chunk, carry):
        cols = pl.ds(pl.multiple_of(chunk * FFN_CHUNK, FFN_CHUNK), FFN_CHUNK)
        gate_pre = dot_nn(full(hid_ref), wg_ref[:, cols]) + bg_ref[:, cols]
        lin_pre = dot_nn(full(hid_ref), wl_ref[:, cols]) + bl_ref[:, cols]
        cdf = 0.5 + 0.5 * lax.erf(gate_pre * (0.5 ** 0.5))
        act = gate_pre * cdf
        pdf = jnp.exp2(gate_pre * gate_pre * (-0.5 * LOG2E)) * 0.3989422804014327
        act_buf[:, cols] = act
        slope_buf[:, cols] = lin_pre * (cdf + gate_pre * pdf)

        inner = (act * lin_pre).astype(BF16)
        inner_buf[:, cols] = inner
        acc_buf[...] += dot_nt(inner, wd_ref[:, cols])
        copy_out(inner_buf, inner_out, 0, chunk, step).start()
        return carry

    lax.fori_loop(0, chunks, forward, 0)
    resid = ALPHA * full(hid_ref).astype(F32) + (full(acc_buf) + full(bd_ref))
    hat, rstd = normalize(resid)
    cot = full(cot_ref).astype(F32)
    add_sums(narrow_ref, 0, cot * hat)
    d_hat = cot * full(gain2_ref)
    d_resid = normalize_back(d_hat, hat, rstd)
    add_sums(narrow_ref, 1, d_resid)
    dffn_ref[...] = d_resid.astype(BF16)
    acc_buf[...] = ALPHA * d_resid

    def backward(chunk, carry):
        cols = pl.ds(pl.multiple_of(chunk * FFN_CHUNK, FFN_CHUNK), FFN_CHUNK)
        d_inner = dot_nn(full(dffn_ref), wd_ref[:, cols]).astype(BF16).astype(F32)
        d_gate = d_inner * slope_buf[:, cols]
        d_lin = d_inner * act_buf[:, cols]
        add_sums(wide_ref.at[:, cols], 0, d_gate)
        add_sums(wide_ref.at[:, cols], 1, d_lin)

        d_gate = d_gate.astype(BF16)
        d_lin = d_lin.astype(BF16)
        gate_buf[:, cols] = d_gate
        lin_buf[:, cols] = d_lin
        acc_buf[...] += dot_nt(d_gate, wg_ref[:, cols]) + dot_nt(d_lin, wl_ref[:, cols])
        copy_out(gate_buf, gate_out, 1, chunk, step).start()
        copy_out(lin_buf, lin_out, 2, chunk, step).start()
        return carry

    lax.fori_loop(0, chunks, backward, 0)
    d_hid = full(acc_buf)
    hat = full(hat_ref)
    add_sums(narrow_ref, 2, d_hid)
    add_sums(narrow_ref, 3, d_hid * hat)
    d_hat = d_hid * full(gain1_ref)
    d_resid = normalize_back(d_hat, hat, rstd_ref[:, :1])
    add_sums(narrow_ref, 4, d_resid)
    dres_ref[...] = d_resid
    dattn_ref[...] = d_resid.astype(BF16)

    @pl.when(step == last)
    def _():
        drain(outputs, step)


def attn_backward_kernel(head_dim, alias_count, *refs):
    (dres_ref, dattn_ref, qkv_ref, prob_ref, wqkv_ref, wo_ref, cos_ref, sin_ref) = refs[:8]
    (demb_ref, dqkv_ref, dall_ref, acc_ref, token_ref) = refs[8 + alias_count:]
    clear(token_ref)
    width = dres_ref.shape[1]
    low, mask_low, mask_high, first_half = lane_masks()
    attn_scale = head_dim ** -0.5
    step = 4 * 3 * head_dim

    @pl.when(pl.program_id(0) == 0)
    def _():
        clear(acc_ref)

    def quad(index, carry):
        col = pl.multiple_of(index * step, step)
        ctx_row = pl.multiple_of(index * 4 * head_dim, 4 * head_dim)
        d_ctx_quad = dot_nn(full(dattn_ref), wo_ref[:, pl.ds(ctx_row, 4 * head_dim)]).astype(BF16)
        pieces = []
        for half in range(2):
            pair = index * 2 + half
            pair_col = pl.multiple_of(pair * LANES, LANES)
            d_ctx = d_ctx_quad[:, half * LANES:(half + 1) * LANES]
            q_rot = qkv_ref[:, pl.ds(pair_col, LANES)]
            k_rot = qkv_ref[:, pl.ds(width + pair_col, LANES)]
            v_pair = qkv_ref[:, pl.ds(2 * width + pair_col, LANES)]
            k_trans = k_rot.astype(F32).T.astype(BF16)
            dq_rows, dk_heads, dv_heads = [], [], []
            for head in range(2):
                v_one = v_pair * (mask_low if head == 0 else mask_high)
                k_one = k_trans[head * 64:(head + 1) * 64]
                d_v, d_k, d_q = [None, None], [None, None], []
                for block in range(2):
                    rows = slice(block * HALF_Q, (block + 1) * HALF_Q)
                    keys = range(block + 1)
                    probs = [prob_ref[pair * 2 + head, (block + num) * HALF_Q:(block + num + 1) * HALF_Q, :] for num in keys]
                    d_probs = [dot_nt(v_one[num * HALF_Q:(num + 1) * HALF_Q], d_ctx[rows]) for num in keys]
                    wide = [prob.astype(F32) for prob in probs]
                    inner = functools.reduce(jnp.add, [col_sum(d_prob * prob) for d_prob, prob in zip(d_probs, wide)])
                    d_q_block = None
                    for num in keys:
                        d_score = (wide[num] * (d_probs[num] - inner) * attn_scale).astype(BF16)
                        terms = (dot_nn(probs[num], d_ctx[rows]), dot_nn(d_score, q_rot[rows]), dot_nn(k_one[:, num * HALF_Q:(num + 1) * HALF_Q], d_score))
                        d_v[num] = terms[0] if d_v[num] is None else d_v[num] + terms[0]
                        d_k[num] = terms[1] if d_k[num] is None else d_k[num] + terms[1]
                        d_q_block = terms[2] if d_q_block is None else d_q_block + terms[2]
                    d_q.append(d_q_block)
                dq_rows.append(jnp.concatenate(d_q, axis=1))
                dk_heads.append(jnp.concatenate(d_k, axis=0))
                dv_heads.append(jnp.concatenate(d_v, axis=0))
            d_q = rope(jnp.concatenate(dq_rows, axis=0).T, full(cos_ref), -full(sin_ref), first_half)
            d_k = rope(jnp.where(low, dk_heads[0], dk_heads[1]), full(cos_ref), -full(sin_ref), first_half)
            d_v = jnp.where(low, dv_heads[0], dv_heads[1])
            d_k = pltpu.roll(d_k, 64, 1)
            pieces += [jnp.where(low, d_q, d_k), jnp.where(low, d_v, d_q), jnp.where(low, d_k, d_v)]
        for num, piece in enumerate(pieces):
            lanes = pl.ds(col + num * LANES, LANES)
            acc_ref[:, lanes] += row_sums(piece)
            dqkv_ref[:, lanes] = piece.astype(BF16)
        return carry

    lax.fori_loop(0, wqkv_ref.shape[1] // step, quad, 0)
    d_emb = SHRINK * (ALPHA * full(dres_ref) + dot_nt(full(dqkv_ref), full(wqkv_ref)))
    demb_ref[...] = d_emb
    dall_ref[...] = d_emb


def whole(shape):
    return pl.BlockSpec(shape, lambda i: (0,) * len(shape), pipeline_mode=pl.Buffered(1))


def per_seq(shape, base=0):
    return pl.BlockSpec((None,) + tuple(shape), lambda i: (i + base,) + (0,) * len(shape))


def cost(flops, moved):
    return pl.CostEstimate(flops=flops, bytes_accessed=moved, transcendentals=0)


def params():
    return pltpu.CompilerParams(dimension_semantics=('arbitrary',), vmem_limit_bytes=VMEM_LIMIT)


TOKEN = (8, LANES)
ANYWHERE = pl.BlockSpec(memory_space=pl.ANY)


def token_spec():
    return pl.BlockSpec(TOKEN, lambda i: (0, 0))


def attn_forward(base, count, total, own, own_base, other, weights, tables, previous, deps, head_dim):
    seq_len, width = own.shape[1:]
    wqkv = weights[0]
    heads = width // head_dim
    shapes = [((seq_len, width), BF16), ((seq_len, 3 * width), BF16), ((heads, seq_len * 3 // 2, HALF_Q), BF16), ((seq_len, width), BF16),
              ((seq_len, width), F32), ((seq_len, LANES), F32), ((seq_len, width), BF16)]
    operands = (own, other) + tuple(weights) + tuple(tables)
    specs = [per_seq((seq_len, width), own_base), per_seq((seq_len, width))] + [whole(item.shape) for item in operands[2:]]
    extra = tuple(previous) if previous is not None else ()
    specs += [ANYWHERE] * (len(extra) + len(deps))
    flops = count * (2 * seq_len * width * (wqkv.shape[1] + width) + 4 * heads * seq_len * seq_len * 64)
    return pl.pallas_call(
        functools.partial(attn_forward_kernel, head_dim, len(extra) + len(deps)),
        grid=(count,),
        in_specs=specs,
        out_specs=[per_seq(shape, base) for shape, _ in shapes] + [token_spec()],
        out_shape=[jax.ShapeDtypeStruct((total,) + shape, dtype) for shape, dtype in shapes] + [jax.ShapeDtypeStruct(TOKEN, F32)],
        input_output_aliases={len(operands) + num: num for num in range(len(extra))},
        compiler_params=params(),
        cost_estimate=cost(2 * flops, count * 12_000_000),
        name='attn_forward',
    )(*operands, *extra, *deps)


def ffn(base, count, hidden, cotangent, hat, rstd, weights, previous, deps):
    total, seq_len, width = hidden.shape
    wide = weights[0].shape[1]
    operands = (hidden, cotangent, hat, rstd) + tuple(weights)
    extra = tuple(previous) if previous is not None else ()
    specs = [per_seq(item.shape[1:], base) for item in operands[:4]] + [whole(item.shape) for item in operands[4:]]
    specs += [ANYWHERE] * (len(extra) + len(deps))
    big = jax.ShapeDtypeStruct((total * seq_len, wide), BF16)
    narrow = jax.ShapeDtypeStruct((total, seq_len, width), BF16)
    flops = 12 * count * seq_len * width * wide
    return pl.pallas_call(
        functools.partial(ffn_kernel, base),
        grid=(count,),
        in_specs=specs,
        out_specs=[ANYWHERE] * 3 + [per_seq((seq_len, width), base)] * 3 + [pl.BlockSpec((40, width), lambda i: (0, 0)), pl.BlockSpec((16, wide), lambda i: (0, 0)), token_spec()],
        out_shape=[big] * 3 + [narrow, jax.ShapeDtypeStruct((total, seq_len, width), F32), narrow,
                               jax.ShapeDtypeStruct((40, width), F32), jax.ShapeDtypeStruct((16, wide), F32), jax.ShapeDtypeStruct(TOKEN, F32)],
        scratch_shapes=[pltpu.VMEM((seq_len, wide), F32)] * 2 + [pltpu.VMEM((seq_len, wide), BF16)] * 3
        + [pltpu.VMEM((seq_len, width), F32), pltpu.SemaphoreType.DMA((3, wide // FFN_CHUNK))],
        input_output_aliases={len(operands) + num: num for num in range(len(extra))},
        compiler_params=params(),
        cost_estimate=cost(int(1.5 * flops), count * 14_000_000),
        name='ffn',
    )(*operands, *extra, *deps)


def attn_backward(base, count, total, d_resid, d_attn, qkv, probs, weights, tables, previous, deps, head_dim):
    seq_len, width = d_resid.shape[1:]
    wqkv, wout = weights
    heads = width // head_dim
    operands = (d_resid, d_attn, qkv, probs, wqkv, wout) + tuple(tables)
    specs = [per_seq(item.shape[1:], base) for item in operands[:4]] + [whole(item.shape) for item in operands[4:]]
    extra = tuple(previous) if previous is not None else ()
    specs += [ANYWHERE] * (len(extra) + len(deps))
    flops = count * (2 * seq_len * width * (wqkv.shape[1] + width) + 8 * heads * seq_len * seq_len * 64)
    return pl.pallas_call(
        functools.partial(attn_backward_kernel, head_dim, len(extra) + len(deps)),
        grid=(count,),
        in_specs=specs,
        out_specs=[per_seq((seq_len, width)), per_seq((seq_len, wqkv.shape[1]), base), per_seq((seq_len, width), base), pl.BlockSpec((8, wqkv.shape[1]), lambda i: (0, 0)), token_spec()],
        out_shape=[jax.ShapeDtypeStruct((count, seq_len, width), F32), jax.ShapeDtypeStruct((total, seq_len, wqkv.shape[1]), BF16),
                   jax.ShapeDtypeStruct((total, seq_len, width), F32),
                   jax.ShapeDtypeStruct((8, wqkv.shape[1]), F32), jax.ShapeDtypeStruct(TOKEN, F32)],
        input_output_aliases={len(operands) + num: 1 + num for num in range(len(extra))},
        compiler_params=params(),
        cost_estimate=cost(2 * flops, count * 12_000_000),
        name='attn_backward',
    )(*operands, *extra, *deps)


def outer_kernel(left_ref, right_ref, *refs):
    out_ref, token_ref, left_t = refs[-3:]
    clear(token_ref)

    @pl.when(pl.program_id(0) == 0)
    def _():
        def turn(index, carry):
            rows = pl.ds(pl.multiple_of(index * CHUNK, CHUNK), CHUNK)
            left_t[:, rows] = left_ref[rows, :].astype(F32).T.astype(BF16)
            return carry

        lax.fori_loop(0, left_ref.shape[0] // CHUNK, turn, 0)

    out_ref[...] = dot_nn(full(left_t), full(right_ref))


def outer(left, right, block, shape, slot, previous, deps):
    rows, width = left.shape
    wide = right.shape[1]
    per_half = wide // (2 * block)
    half_blocks = shape[1] // (2 * block)
    extra = (previous,) if previous is not None else ()
    return pl.pallas_call(
        outer_kernel,
        grid=(wide // block,),
        in_specs=[whole((rows, width)), pl.BlockSpec((rows, block), lambda i: (0, i))] + [ANYWHERE] * (len(extra) + len(deps)),
        out_specs=[pl.BlockSpec((width, block), lambda i: (0, slot + i % per_half + half_blocks * (i // per_half))), token_spec()],
        out_shape=[jax.ShapeDtypeStruct(shape, F32), jax.ShapeDtypeStruct(TOKEN, F32)],
        input_output_aliases={2 + num: num for num in range(len(extra))},
        scratch_shapes=[pltpu.VMEM((width, rows), BF16)],
        compiler_params=params(),
        cost_estimate=cost(2 * rows * width * wide, 4 * width * wide + 2 * rows * (width + wide)),
        name='outer',
    )(left, right, *extra, *deps)


def groups_of(start, stop, size):
    return [(base, size) for base in range(start, stop, size)]


def join_kernel(plain, peer_ref, *refs):
    owns, outs = refs[:len(refs) // 2], refs[len(refs) // 2:]
    start = 0
    for num, (own_ref, out_ref) in enumerate(zip(owns, outs)):
        half = out_ref.shape[1] // 2
        out_ref[:, :half] = full(own_ref) if num < plain else full(own_ref).astype(F32).T.astype(BF16)
        out_ref[:, half:] = peer_ref[:, start:start + half].astype(BF16)
        start += half


def join(peer, plain, flipped):
    owns = tuple(plain) + tuple(flipped)
    rows = peer.shape[0]
    halves = [item.shape[1] for item in plain] + [item.shape[0] for item in flipped]
    return pl.pallas_call(
        functools.partial(join_kernel, len(plain)),
        grid=(rows // LANES,),
        in_specs=[pl.BlockSpec((LANES, peer.shape[1]), lambda i: (i, 0))] + [pl.BlockSpec((LANES, item.shape[1]), lambda i: (i, 0)) for item in plain]
        + [pl.BlockSpec((item.shape[0], LANES), lambda i: (0, i)) for item in flipped],
        out_specs=[pl.BlockSpec((LANES, 2 * half), lambda i: (i, 0)) for half in halves],
        out_shape=[jax.ShapeDtypeStruct((rows, 2 * half), BF16) for half in halves],
        compiler_params=params(),
        cost_estimate=cost(peer.size * 64, peer.size * 10),
        name='join_weights',
    )(peer, *owns)


def shared_slice(plain, flipped, index, parts):
    rows = plain[0].shape[0] // parts
    pieces = [lax.dynamic_slice_in_dim(item, index * rows, rows, 0) for item in plain]
    pieces += [lax.dynamic_slice_in_dim(item, index * rows, rows, 1).T for item in flipped]
    return jnp.concatenate(pieces, axis=1).astype(F32)


def row_pieces(rows):
    tiles = rows // TILE
    cuts = [num * tiles // PIECES * TILE for num in range(PIECES + 1)]
    return [(first, last - first) for first, last in zip(cuts, cuts[1:])]


def table_kernel(src, out, away, keep, got_one, got_two, stage, load_sems, store_sems, swap_sems, one_sems, two_sems, near_sems, far_sems, back_sems):
    me = lax.axis_index('dp')
    core, col, line = me % 2, me // 2 % 2, me // 4
    partner, x_peer, y_peer = me + 1 - 2 * core, me + 2 - 4 * col, me + 4 - 8 * line
    first_peer = x_peer + core * (y_peer - x_peer)
    second_peer = y_peer + core * (x_peer - y_peer)
    one = col + core * (line - col)
    two = line + core * (col - line)
    eighth = src.shape[0] // 8
    pieces = row_pieces(eighth)
    jobs = [(part, num) for part in range(4) for num in range(PIECES)]

    barrier = pltpu.get_barrier_semaphore()
    for peer in (partner, x_peer, y_peer):
        pl.semaphore_signal(barrier, inc=1, device_id={'dp': peer}, device_id_type=pl.DeviceIdType.MESH)
    pl.semaphore_wait(barrier, 3)

    def send(source, target, sems, slot, peer):
        return pltpu.make_async_remote_copy(src_ref=source, dst_ref=target, send_sem=sems.at[0, slot], recv_sem=sems.at[1, slot],
                                            device_id={'dp': peer}, device_id_type=pl.DeviceIdType.MESH)

    def table_rows(ref, half, quarter, last, num):
        start, size = pieces[num]
        return ref.at[pl.ds(pl.multiple_of((half * 4 + quarter * 2 + last) * eighth + start, TILE), size)]

    def part_rows(ref, half, quarter, last, part, num):
        return table_rows(ref, half, 1 - quarter if part < 2 else quarter, last if part % 2 else 1 - last, num)

    def buffer_rows(ref, part, num):
        start, size = pieces[num]
        return ref.at[pl.ds(part % 2 * eighth + start, size)]

    def holder(part):
        return away if part < 2 else keep

    def add_into(target, part, source, source_part, num):
        start, size = pieces[num]
        to, of = part % 2 * eighth + start, source_part * eighth + start

        def body(index, carry):
            offset = index * TILE
            target[pl.ds(pl.multiple_of(to + offset, TILE), TILE)] += source[pl.ds(pl.multiple_of(of + offset, TILE), TILE)]
            return carry

        lax.fori_loop(0, size // TILE, body, 0)

    swaps = [send(part_rows(src, 1 - core, two, one, part, num), buffer_rows(holder(part), part, num), swap_sems, slot, partner)
             for slot, (part, num) in enumerate(jobs)]
    loads = [pltpu.make_async_copy(part_rows(src, core, one, two, part, num), stage.at[slot % 2, pl.ds(0, pieces[num][1])], load_sems.at[slot % 2])
             for slot, (part, num) in enumerate(jobs)]
    firsts = [send(buffer_rows(away, part, num), buffer_rows(got_one, part, num), one_sems, slot, first_peer)
              for slot, (part, num) in enumerate(jobs[:2 * PIECES])]
    seconds = [send(buffer_rows(keep, 0, num), buffer_rows(got_two, 0, num), two_sems, num, second_peer) for num in range(PIECES)]

    for copy in swaps:
        copy.start()
    loads[0].start()
    for slot, (part, num) in enumerate(jobs):
        if slot + 1 < len(jobs):
            loads[slot + 1].start()
        loads[slot].wait()
        swaps[slot].wait_recv()
        start, size = pieces[num]
        target, held, to = holder(part), stage.at[slot % 2], part % 2 * eighth + start

        def body(index, carry, target=target, held=held, to=to):
            offset = index * TILE
            target[pl.ds(pl.multiple_of(to + offset, TILE), TILE)] += held[pl.ds(pl.multiple_of(offset, TILE), TILE)]
            return carry

        lax.fori_loop(0, size // TILE, body, 0)
        if 0 < slot <= len(firsts):
            firsts[slot - 1].start()

    for slot in range(2 * PIECES):
        firsts[slot].wait_recv()
        add_into(keep, slot // PIECES, got_one, slot // PIECES, slot % PIECES)
        if 0 < slot <= PIECES:
            seconds[slot - 1].start()

    done = []

    def publish(num):
        mine = buffer_rows(keep, 1, num)
        place = table_rows(out, core, one, two, num)
        copies = [pltpu.make_async_copy(mine, place, store_sems.at[num]), send(mine, place, near_sems, num, second_peer),
                  send(mine, place, far_sems, num, first_peer), send(mine, place, back_sems, num, partner)]
        for copy in copies:
            copy.start()
        done.append(copies)

    for num in range(PIECES):
        seconds[num].wait_recv()
        add_into(keep, 1, got_two, 0, num)
        if num:
            publish(num - 1)
    publish(PIECES - 1)

    def forward(quarter, last, num, sems, slot, peer, start=True):
        place = table_rows(out, core, quarter, last, num)
        copy = send(place, place, sems, slot, peer)
        if start:
            copy.start()
        return copy

    relays = []
    for num in range(PIECES):
        forward(one, 1 - two, num, near_sems, num, second_peer, False).wait_recv()
        relays.append(forward(one, 1 - two, num, far_sems, PIECES + num, first_peer))
        relays.append(forward(one, 1 - two, num, back_sems, PIECES + num, partner))
        forward(1 - one, two, num, far_sems, num, first_peer, False).wait_recv()
        relays.append(forward(1 - one, two, num, back_sems, 2 * PIECES + num, partner))
    for num in range(PIECES):
        forward(1 - one, 1 - two, num, far_sems, PIECES + num, first_peer, False).wait_recv()
        relays.append(forward(1 - one, 1 - two, num, back_sems, 3 * PIECES + num, partner))
    for slot, (part, num) in enumerate(jobs):
        place = table_rows(out, 1 - core, two if part < 2 else 1 - two, 1 - one if part % 2 else one, num)
        send(place, place, back_sems, slot, partner).wait_recv()
    for copy in swaps + firsts + seconds + relays:
        copy.wait_send()
    for local, *remote in done:
        local.wait()
        for copy in remote:
            copy.wait_send()


def reduce_table(table):
    rows, width = table.shape
    eighth = rows // 8
    largest = max(size for _, size in row_pieces(eighth))
    buffers = [pltpu.VMEM((count * eighth, width), F32) for count in (2, 2, 2, 1)]
    counts = (4 * PIECES, 2 * PIECES, PIECES, PIECES, 2 * PIECES, 4 * PIECES)
    return pl.pallas_call(
        table_kernel,
        in_specs=[ANYWHERE],
        out_specs=ANYWHERE,
        out_shape=jax.ShapeDtypeStruct(table.shape, F32),
        scratch_shapes=buffers + [pltpu.VMEM((2, largest, width), F32), pltpu.SemaphoreType.DMA((2,)), pltpu.SemaphoreType.DMA((PIECES,))]
        + [pltpu.SemaphoreType.DMA((2, count)) for count in counts],
        compiler_params=pltpu.CompilerParams(collective_id=0, has_side_effects=True, vmem_limit_bytes=VMEM_LIMIT),
        cost_estimate=cost(400_000_000_000, rows * width * 8),
        name='reduce_table',
    )(table)


def reduce_gradient(grad):
    piece = lax.psum_scatter(grad, 'dp', scatter_dimension=0, tiled=True)
    half = piece.shape[1] // 2
    other = lax.ppermute(piece[:, half:], 'tp', SWAP)
    return lax.all_gather(piece[:, :half] + other, 'dp', axis=0, tiled=True)


def tie(value, token):
    return lax.optimization_barrier((value, token))[0]


def solution(mesh):
    in_specs = (P('dp'), P('dp'), ROWS) + WEIGHT_SPECS
    out_specs = (ROWS,) + WEIGHT_SPECS
    parts = mesh.shape['dp']

    def device_step(tokens, cotangent, emb_table, *weights):
        (w_qkv, b_qkv, w_out, b_out, ln1_gain, ln1_bias, w_gate, b_gate, w_lin, b_lin, w_down, b_down, ln2_gain) = weights
        tp_index, dp_index = lax.axis_index('tp'), lax.axis_index('dp')
        vocab_loc, width = emb_table.shape
        head_dim = b_qkv.shape[1] // 3
        seq_len = tokens.shape[1]
        total = tokens.shape[0] // 2

        local_ids = tokens - tp_index * vocab_loc
        in_shard = (local_ids >= 0) & (local_ids < vocab_loc)
        own_ids = lax.dynamic_slice_in_dim(local_ids, tp_index * total, total)
        own_in = lax.dynamic_slice_in_dim(in_shard, tp_index * total, total)
        peer_ids = lax.dynamic_slice_in_dim(local_ids, (1 - tp_index) * total, total)
        peer_in = lax.dynamic_slice_in_dim(in_shard, (1 - tp_index) * total, total)
        own_cot = lax.dynamic_slice_in_dim(cotangent, tp_index * total, total)

        def rows_of(ids, inside):
            rows = jnp.take(emb_table, jnp.where(inside, ids, 0), axis=0)
            return jnp.where(inside[:, :, None], rows, 0.0)

        def exchange(value):
            return lax.ppermute(value, 'tp', SWAP)

        def collect(value):
            value = exchange(value)
            return lax.all_gather(value, 'dp', axis=0, tiled=True)

        def row_of(vector):
            return vector.astype(F32).reshape(1, -1)

        half = total // 2
        qkv_loc, wide_loc = b_qkv.size, b_gate.shape[0]
        groups = [(num, 1) for num in range(half)] + groups_of(half, total, 2)

        def both_halves(ids, inside, kind):
            head = rows_of(ids[:half], inside[:half]).astype(kind)
            return head, rows_of(tie(ids[half:], head), inside[half:]).astype(kind)

        peer_halves = both_halves(peer_ids, peer_in, F32)
        own_halves = both_halves(own_ids, own_in, BF16)
        front_peer = collect(shared_slice((w_qkv,), (w_out,), dp_index, parts))
        wide_peer = collect(shared_slice((w_gate, w_lin), (w_down,), dp_index, parts))
        arrived = [exchange(peer_halves[base // half][base % half:base % half + count]) for base, count in groups]
        own_bias = jnp.concatenate([row_of(b_qkv), row_of(b_gate), row_of(b_lin)], axis=1)
        biases = jnp.concatenate([own_bias, exchange(own_bias)])
        bqkv_full = biases[:, :qkv_loc].reshape(1, -1)
        bgate_full = biases[:, qkv_loc:qkv_loc + wide_loc].reshape(1, -1)
        blin_full = biases[:, qkv_loc + wide_loc:].reshape(1, -1)
        wqkv_full, wout_full = join(front_peer, (w_qkv,), (w_out,))
        wide_full = join(wide_peer, (w_gate, w_lin), (w_down,))

        half_dim = head_dim // 2
        inv_freq = ROPE_BASE ** (-2.0 * jnp.arange(half_dim, dtype=F32) / head_dim)
        angles = jnp.arange(seq_len, dtype=F32)[:, None] * inv_freq[None, :]
        cos_half, sin_half = jnp.cos(angles), jnp.sin(angles)
        tables = (jnp.concatenate([cos_half] * 4, axis=1), jnp.concatenate([-sin_half, sin_half] * 2, axis=1))

        front = (wqkv_full, bqkv_full, wout_full, row_of(b_out), row_of(ln1_gain), row_of(ln1_bias))
        middle = tuple(wide_full) + (bgate_full, blin_full, row_of(b_down), row_of(ln1_gain), row_of(ln2_gain))
        saved, ffn_saved, d_kept, deps = None, None, None, ()
        narrow_parts, wide_parts, bias_parts, d_peer = [], [], [], []

        def run_attention(num):
            nonlocal saved, deps
            base, count = groups[num]
            out = attn_forward(base, count, total, own_halves[base // half], base % half, arrived[num], front, tables, saved, deps, head_dim)
            *kept, token = out
            saved, deps = kept, (token,)

        def run_ffn(base, count):
            nonlocal ffn_saved, deps
            *_, hat, rstd, hidden = saved
            *kept, narrow, wide, token = ffn(base, count, hidden, own_cot, hat, rstd, middle, ffn_saved, deps)
            ffn_saved, deps = kept, (token,)
            narrow_parts.append(narrow)
            wide_parts.append(wide)

        def run_backward(base, count):
            nonlocal d_kept, deps
            _, qkv, probs, *_ = saved
            *_, d_resid, d_attn = ffn_saved
            d_emb, d_qkv, d_all, bias_part, token = attn_backward(base, count, total, d_resid, d_attn, qkv, probs, (wqkv_full, wout_full), tables, d_kept, deps, head_dim)
            d_kept, deps = (d_qkv, d_all), (token,)
            bias_parts.append(bias_part)
            d_peer.append(exchange(d_emb))

        def run_outer(left, right, block, shape, slot, previous):
            nonlocal deps
            out, token = outer(left.reshape(-1, left.shape[-1]), right.reshape(-1, right.shape[-1]), block, shape, slot, previous, deps)
            deps = (token,)
            return out

        for num in range(half + 2):
            run_attention(num)
            if num % 2 and num < half:
                run_ffn(num - 1, 2)
        run_backward(0, half)
        run_ffn(half, half)
        inner, d_gate, d_lin, d_ffn, _, d_attn = ffn_saved
        emb, _, _, context, _, _, hidden = saved
        shape = (width, 6 * wide_loc)
        step = wide_loc // CHUNK
        grads = run_outer(hidden, d_gate, CHUNK, shape, 0, None)
        grads = run_outer(hidden, d_lin, CHUNK, shape, step, grads)
        grads = run_outer(d_ffn, inner, CHUNK, shape, 2 * step, grads)
        wide_grads = reduce_gradient(grads)
        for base, count in groups_of(half, total, 2):
            run_backward(base, count)
        block = w_out.shape[0]
        shape = (width + parts * TILE, 2 * (qkv_loc + block))
        d_qkv, d_all = d_kept
        grads = run_outer(d_attn, context, block, shape, qkv_loc // block, None)
        grads = run_outer(emb, d_qkv, block, shape, 0, grads)

        narrow = jnp.sum(sum(narrow_parts).reshape(5, 8, -1), axis=1).reshape(1, -1)
        d_bwide = jnp.sum(sum(wide_parts).reshape(2, 8, -1), axis=1).reshape(2, 2, -1)
        small = jnp.concatenate([jnp.sum(sum(bias_parts), axis=0).reshape(2, -1), d_bwide[0], d_bwide[1], jnp.concatenate([narrow] * 2)], axis=1)
        used = small.shape[1]
        small = jnp.pad(small, ((0, 0), (0, TILE * (qkv_loc + block) - used))).reshape(2, TILE, -1)
        grads = lax.dynamic_update_slice(grads, jnp.concatenate([small[0], small[1]], axis=1), (width, 0))
        front_grads = reduce_gradient(grads)

        own_row_ids = jnp.where(own_in, own_ids, vocab_loc)
        peer_row_ids = jnp.where(peer_in, peer_ids, vocab_loc)

        def add_rows(grad, ids, rows):
            return grad.at[ids.reshape(-1)].add(rows.reshape(-1, width), mode='drop')

        d_table = add_rows(jnp.zeros((vocab_loc, width), F32), tie(own_row_ids, *deps), d_all)
        d_table = add_rows(d_table, peer_row_ids, jnp.concatenate(d_peer, axis=0))
        d_table = reduce_table(d_table)

        small = front_grads[width:width + TILE].reshape(-1)
        d_b_qkv = small[:qkv_loc].reshape(b_qkv.shape)
        d_b_gate = small[qkv_loc:qkv_loc + wide_loc]
        d_b_lin = small[qkv_loc + wide_loc:qkv_loc + 2 * wide_loc]
        d_ln2_gain, d_b_down, d_ln1_bias, d_ln1_gain, d_b_out = small[qkv_loc + 2 * wide_loc:used].reshape(5, width)
        d_w_gate, d_w_lin, d_w_down = (wide_grads[:, num * wide_loc:(num + 1) * wide_loc] for num in range(3))
        d_w_qkv, d_w_out = front_grads[:width, :qkv_loc], front_grads[:width, qkv_loc:]
        return (d_table, d_w_qkv, d_b_qkv, d_w_out.T, d_b_out, d_ln1_gain, d_ln1_bias, d_w_gate, d_b_gate, d_w_lin, d_b_lin, d_w_down.T, d_b_down, d_ln2_gain)

    return jax.shard_map(device_step, mesh=mesh, in_specs=in_specs, out_specs=out_specs, check_vma=False)
```

```python
import functools

import jax
import jax.numpy as jnp
from jax import lax
from jax.experimental import pallas as pl
from jax.experimental.pallas import tpu as pltpu
from jax.sharding import PartitionSpec as P


ALPHA = 140.0 ** 0.5
EPS = 1e-5
SHRINK = 0.1
ROPE_BASE = 10000.0
COLS, ROWS, ALL = P(None, 'tp'), P('tp'), P()
WEIGHT_SPECS = (COLS, ROWS, ROWS, ALL, ALL, ALL, COLS, ROWS, COLS, ROWS, ROWS, ALL, ALL)

F32 = jnp.float32
BF16 = jnp.bfloat16
LANES = 128
HALF_Q = 256
CHUNK = 512
FFN_CHUNK = 768
TILE = 8
PIECES = 3
VMEM_LIMIT = 66 * 1024 * 1024 - 512 * 1024
LOG2E = 1.4426950408889634
MASKED = -8e30
NT = (((1,), (1,)), ((), ()))
NN = (((1,), (0,)), ((), ()))
SWAP = ((0, 1), (1, 0))


def dot_nn(left, right):
    return lax.dot_general(left, right, NN, preferred_element_type=F32)


def dot_nt(left, right):
    return lax.dot_general(left, right, NT, preferred_element_type=F32)


def row_sums(values):
    return jnp.sum(values.reshape(-1, TILE, values.shape[1]), axis=0)


def row_mean(values):
    return jnp.mean(values, axis=-1, keepdims=True)


def col_sum(values):
    return jnp.sum(values, axis=0, keepdims=True)


def add_sums(ref, slot, values):
    ref[slot * TILE:(slot + 1) * TILE] += row_sums(values)


def full(ref):
    return ref[...]


def clear(ref):
    ref[...] = jnp.zeros_like(ref)


def normalize(values):
    centered = values - row_mean(values)
    rstd = lax.rsqrt(row_mean(centered * centered) + EPS)
    return centered * rstd, rstd


def normalize_back(d_hat, hat, rstd):
    return rstd * (d_hat - row_mean(d_hat) - hat * row_mean(d_hat * hat))


def rope(values, cos_tab, sin_tab, first_half):
    partner = jnp.where(first_half, pltpu.roll(values, 96, 1), pltpu.roll(values, 32, 1))
    return values * cos_tab + partner * sin_tab


def lane_masks():
    lane = lax.broadcasted_iota(jnp.int32, (1, LANES), 1)
    low = lane < 64
    return low, low.astype(F32).astype(BF16), (1.0 - low.astype(F32)).astype(BF16), (lane % 64) < 32


def attn_forward_kernel(head_dim, alias_count, *refs):
    (own_ref, other_ref, wqkv_ref, bqkv_ref, wo_ref, bo_ref, gain_ref, bias_ref, cos_ref, sin_ref) = refs[:10]
    (emb_ref, qkv_ref, prob_ref, ctx_ref, hat_ref, rstd_ref, hid_ref, token_ref) = refs[10 + alias_count:]
    seq_len, width = own_ref.shape
    clear(token_ref)
    emb_ref[...] = (full(own_ref).astype(F32) + full(other_ref)).astype(BF16)
    low, mask_low, mask_high, first_half = lane_masks()
    score_scale = head_dim ** -0.5 * LOG2E
    causal = lax.broadcasted_iota(jnp.int32, (HALF_Q, HALF_Q), 0) <= lax.broadcasted_iota(jnp.int32, (HALF_Q, HALF_Q), 1)
    step = 4 * 3 * head_dim

    def quad(index, carry):
        col = pl.multiple_of(index * step, step)
        pre = dot_nn(full(emb_ref), wqkv_ref[:, pl.ds(col, step)]) + bqkv_ref[:, pl.ds(col, step)]
        pre = pre.astype(BF16).astype(F32)
        for half in range(2):
            parts = [pre[:, (half * 3 + part) * LANES:(half * 3 + part + 1) * LANES] for part in range(3)]
            pair = index * 2 + half
            pair_col = pl.multiple_of(pair * LANES, LANES)
            q_pair = jnp.where(low, parts[0], parts[1])
            k_pair = pltpu.roll(jnp.where(low, parts[2], parts[0]), 64, 1)
            v_pair = jnp.where(low, parts[1], parts[2])
            q_rot = rope(q_pair, full(cos_ref), full(sin_ref), first_half).astype(BF16)
            k_rot = rope(k_pair, full(cos_ref), full(sin_ref), first_half).astype(BF16)
            qkv_ref[:, pl.ds(pair_col, LANES)] = q_rot
            qkv_ref[:, pl.ds(width + pair_col, LANES)] = k_rot
            qkv_ref[:, pl.ds(2 * width + pair_col, LANES)] = v_pair.astype(BF16)
            v_trans = v_pair.T.astype(BF16)
            ctx_rows = []
            for head in range(2):
                k_one = k_rot * (mask_low if head == 0 else mask_high)
                v_one = v_trans[head * 64:(head + 1) * 64]
                blocks = []
                for block in range(2):
                    q_block = q_rot[block * HALF_Q:(block + 1) * HALF_Q]
                    diag = jnp.where(causal, dot_nt(k_one[block * HALF_Q:(block + 1) * HALF_Q], q_block), MASKED)
                    pieces = [diag] if block == 0 else [dot_nt(k_one[:HALF_Q], q_block), diag]
                    peak = functools.reduce(jnp.maximum, [jnp.max(piece, axis=0, keepdims=True) for piece in pieces])
                    exps = [jnp.exp2((piece - peak) * score_scale) for piece in pieces]
                    total = functools.reduce(jnp.add, [col_sum(piece) for piece in exps])
                    inverse = 1.0 / total
                    ctx = None
                    for num, piece in enumerate(exps):
                        prob = (piece * inverse).astype(BF16)
                        prob_ref[pair * 2 + head, (block + num) * HALF_Q:(block + num + 1) * HALF_Q, :] = prob
                        term = dot_nn(v_one[:, num * HALF_Q:(num + 1) * HALF_Q], prob)
                        ctx = term if ctx is None else ctx + term
                    blocks.append(ctx)
                ctx_rows.append(jnp.concatenate(blocks, axis=1))
            ctx_pair = jnp.concatenate(ctx_rows, axis=0)
            ctx_ref[:, pl.ds(pair_col, LANES)] = ctx_pair.T.astype(BF16)
        return carry

    lax.fori_loop(0, wqkv_ref.shape[1] // step, quad, 0)
    attn = dot_nt(full(ctx_ref), full(wo_ref)) + full(bo_ref)
    resid = ALPHA * full(emb_ref).astype(F32) + attn
    hat, rstd = normalize(resid)
    hat_ref[...] = hat
    rstd_ref[...] = jnp.broadcast_to(rstd, (seq_len, LANES))
    hid_ref[...] = (hat * full(gain_ref) + full(bias_ref)).astype(BF16)


def ffn_kernel(base, hid_ref, cot_ref, hat_ref, rstd_ref, wg_ref, wl_ref, wd_ref, bg_ref, bl_ref, bd_ref, gain1_ref, gain2_ref,
               *refs):
    (inner_out, gate_out, lin_out, dffn_ref, dres_ref, dattn_ref, narrow_ref, wide_ref, token_ref,
     act_buf, slope_buf, inner_buf, gate_buf, lin_buf, acc_buf, sems) = refs[-16:]
    step = pl.program_id(0)
    last = pl.num_programs(0) - 1
    clear(token_ref)
    rows, _ = hid_ref.shape
    chunks = wg_ref.shape[1] // FFN_CHUNK

    def copy_out(buf, out, kind, chunk, block):
        cols = pl.ds(pl.multiple_of(chunk * FFN_CHUNK, FFN_CHUNK), FFN_CHUNK)
        return pltpu.make_async_copy(buf.at[:, cols], out.at[pl.ds((block + base) * rows, rows), cols], sems.at[kind, chunk])

    @pl.when(step == 0)
    def _():
        clear(narrow_ref)
        clear(wide_ref)

    outputs = ((inner_buf, inner_out, 0), (gate_buf, gate_out, 1), (lin_buf, lin_out, 2))

    def drain(copies, block):
        def body(chunk, carry):
            for buf, out, kind in copies:
                copy_out(buf, out, kind, chunk, block).wait()
            return carry

        lax.fori_loop(0, chunks, body, 0)

    @pl.when(step > 0)
    def _():
        drain(outputs, step - 1)

    clear(acc_buf)

    def forward(chunk, carry):
        cols = pl.ds(pl.multiple_of(chunk * FFN_CHUNK, FFN_CHUNK), FFN_CHUNK)
        gate_pre = dot_nn(full(hid_ref), wg_ref[:, cols]) + bg_ref[:, cols]
        lin_pre = dot_nn(full(hid_ref), wl_ref[:, cols]) + bl_ref[:, cols]
        cdf = 0.5 + 0.5 * lax.erf(gate_pre * (0.5 ** 0.5))
        act = gate_pre * cdf
        pdf = jnp.exp2(gate_pre * gate_pre * (-0.5 * LOG2E)) * 0.3989422804014327
        act_buf[:, cols] = act
        slope_buf[:, cols] = lin_pre * (cdf + gate_pre * pdf)

        inner = (act * lin_pre).astype(BF16)
        inner_buf[:, cols] = inner
        acc_buf[...] += dot_nt(inner, wd_ref[:, cols])
        copy_out(inner_buf, inner_out, 0, chunk, step).start()
        return carry

    lax.fori_loop(0, chunks, forward, 0)
    resid = ALPHA * full(hid_ref).astype(F32) + (full(acc_buf) + full(bd_ref))
    hat, rstd = normalize(resid)
    cot = full(cot_ref).astype(F32)
    add_sums(narrow_ref, 0, cot * hat)
    d_hat = cot * full(gain2_ref)
    d_resid = normalize_back(d_hat, hat, rstd)
    add_sums(narrow_ref, 1, d_resid)
    dffn_ref[...] = d_resid.astype(BF16)
    acc_buf[...] = ALPHA * d_resid

    def backward(chunk, carry):
        cols = pl.ds(pl.multiple_of(chunk * FFN_CHUNK, FFN_CHUNK), FFN_CHUNK)
        d_inner = dot_nn(full(dffn_ref), wd_ref[:, cols]).astype(BF16).astype(F32)
        d_gate = d_inner * slope_buf[:, cols]
        d_lin = d_inner * act_buf[:, cols]
        add_sums(wide_ref.at[:, cols], 0, d_gate)
        add_sums(wide_ref.at[:, cols], 1, d_lin)

        d_gate = d_gate.astype(BF16)
        d_lin = d_lin.astype(BF16)
        gate_buf[:, cols] = d_gate
        lin_buf[:, cols] = d_lin
        acc_buf[...] += dot_nt(d_gate, wg_ref[:, cols]) + dot_nt(d_lin, wl_ref[:, cols])
        copy_out(gate_buf, gate_out, 1, chunk, step).start()
        copy_out(lin_buf, lin_out, 2, chunk, step).start()
        return carry

    lax.fori_loop(0, chunks, backward, 0)
    d_hid = full(acc_buf)
    hat = full(hat_ref)
    add_sums(narrow_ref, 2, d_hid)
    add_sums(narrow_ref, 3, d_hid * hat)
    d_hat = d_hid * full(gain1_ref)
    d_resid = normalize_back(d_hat, hat, rstd_ref[:, :1])
    add_sums(narrow_ref, 4, d_resid)
    dres_ref[...] = d_resid
    dattn_ref[...] = d_resid.astype(BF16)

    @pl.when(step == last)
    def _():
        drain(outputs, step)


def attn_backward_kernel(head_dim, alias_count, *refs):
    (dres_ref, dattn_ref, qkv_ref, prob_ref, wqkv_ref, wo_ref, cos_ref, sin_ref) = refs[:8]
    (demb_ref, dqkv_ref, dall_ref, acc_ref, token_ref) = refs[8 + alias_count:]
    clear(token_ref)
    width = dres_ref.shape[1]
    low, mask_low, mask_high, first_half = lane_masks()
    attn_scale = head_dim ** -0.5
    step = 4 * 3 * head_dim

    @pl.when(pl.program_id(0) == 0)
    def _():
        clear(acc_ref)

    def quad(index, carry):
        col = pl.multiple_of(index * step, step)
        ctx_row = pl.multiple_of(index * 4 * head_dim, 4 * head_dim)
        d_ctx_quad = dot_nn(full(dattn_ref), wo_ref[:, pl.ds(ctx_row, 4 * head_dim)]).astype(BF16)
        pieces = []
        for half in range(2):
            pair = index * 2 + half
            pair_col = pl.multiple_of(pair * LANES, LANES)
            d_ctx = d_ctx_quad[:, half * LANES:(half + 1) * LANES]
            q_rot = qkv_ref[:, pl.ds(pair_col, LANES)]
            k_rot = qkv_ref[:, pl.ds(width + pair_col, LANES)]
            v_pair = qkv_ref[:, pl.ds(2 * width + pair_col, LANES)]
            k_trans = k_rot.astype(F32).T.astype(BF16)
            dq_rows, dk_heads, dv_heads = [], [], []
            for head in range(2):
                v_one = v_pair * (mask_low if head == 0 else mask_high)
                k_one = k_trans[head * 64:(head + 1) * 64]
                d_v, d_k, d_q = [None, None], [None, None], []
                for block in range(2):
                    rows = slice(block * HALF_Q, (block + 1) * HALF_Q)
                    keys = range(block + 1)
                    probs = [prob_ref[pair * 2 + head, (block + num) * HALF_Q:(block + num + 1) * HALF_Q, :] for num in keys]
                    d_probs = [dot_nt(v_one[num * HALF_Q:(num + 1) * HALF_Q], d_ctx[rows]) for num in keys]
                    wide = [prob.astype(F32) for prob in probs]
                    inner = functools.reduce(jnp.add, [col_sum(d_prob * prob) for d_prob, prob in zip(d_probs, wide)])
                    d_q_block = None
                    for num in keys:
                        d_score = (wide[num] * (d_probs[num] - inner) * attn_scale).astype(BF16)
                        terms = (dot_nn(probs[num], d_ctx[rows]), dot_nn(d_score, q_rot[rows]), dot_nn(k_one[:, num * HALF_Q:(num + 1) * HALF_Q], d_score))
                        d_v[num] = terms[0] if d_v[num] is None else d_v[num] + terms[0]
                        d_k[num] = terms[1] if d_k[num] is None else d_k[num] + terms[1]
                        d_q_block = terms[2] if d_q_block is None else d_q_block + terms[2]
                    d_q.append(d_q_block)
                dq_rows.append(jnp.concatenate(d_q, axis=1))
                dk_heads.append(jnp.concatenate(d_k, axis=0))
                dv_heads.append(jnp.concatenate(d_v, axis=0))
            d_q = rope(jnp.concatenate(dq_rows, axis=0).T, full(cos_ref), -full(sin_ref), first_half)
            d_k = rope(jnp.where(low, dk_heads[0], dk_heads[1]), full(cos_ref), -full(sin_ref), first_half)
            d_v = jnp.where(low, dv_heads[0], dv_heads[1])
            d_k = pltpu.roll(d_k, 64, 1)
            pieces += [jnp.where(low, d_q, d_k), jnp.where(low, d_v, d_q), jnp.where(low, d_k, d_v)]
        for num, piece in enumerate(pieces):
            lanes = pl.ds(col + num * LANES, LANES)
            acc_ref[:, lanes] += row_sums(piece)
            dqkv_ref[:, lanes] = piece.astype(BF16)
        return carry

    lax.fori_loop(0, wqkv_ref.shape[1] // step, quad, 0)
    d_emb = SHRINK * (ALPHA * full(dres_ref) + dot_nt(full(dqkv_ref), full(wqkv_ref)))
    demb_ref[...] = d_emb
    dall_ref[...] = d_emb


def whole(shape):
    return pl.BlockSpec(shape, lambda i: (0,) * len(shape), pipeline_mode=pl.Buffered(1))


def per_seq(shape, base=0):
    return pl.BlockSpec((None,) + tuple(shape), lambda i: (i + base,) + (0,) * len(shape))


def cost(flops, moved):
    return pl.CostEstimate(flops=flops, bytes_accessed=moved, transcendentals=0)


def params():
    return pltpu.CompilerParams(dimension_semantics=('arbitrary',), vmem_limit_bytes=VMEM_LIMIT)


TOKEN = (8, LANES)
ANYWHERE = pl.BlockSpec(memory_space=pl.ANY)


def token_spec():
    return pl.BlockSpec(TOKEN, lambda i: (0, 0))


def attn_forward(base, count, total, own, own_base, other, weights, tables, previous, deps, head_dim):
    seq_len, width = own.shape[1:]
    wqkv = weights[0]
    heads = width // head_dim
    shapes = [((seq_len, width), BF16), ((seq_len, 3 * width), BF16), ((heads, seq_len * 3 // 2, HALF_Q), BF16), ((seq_len, width), BF16),
              ((seq_len, width), F32), ((seq_len, LANES), F32), ((seq_len, width), BF16)]
    operands = (own, other) + tuple(weights) + tuple(tables)
    specs = [per_seq((seq_len, width), own_base), per_seq((seq_len, width))] + [whole(item.shape) for item in operands[2:]]
    extra = tuple(previous) if previous is not None else ()
    specs += [ANYWHERE] * (len(extra) + len(deps))
    flops = count * (2 * seq_len * width * (wqkv.shape[1] + width) + 4 * heads * seq_len * seq_len * 64)
    return pl.pallas_call(
        functools.partial(attn_forward_kernel, head_dim, len(extra) + len(deps)),
        grid=(count,),
        in_specs=specs,
        out_specs=[per_seq(shape, base) for shape, _ in shapes] + [token_spec()],
        out_shape=[jax.ShapeDtypeStruct((total,) + shape, dtype) for shape, dtype in shapes] + [jax.ShapeDtypeStruct(TOKEN, F32)],
        input_output_aliases={len(operands) + num: num for num in range(len(extra))},
        compiler_params=params(),
        cost_estimate=cost(2 * flops, count * 12_000_000),
        name='attn_forward',
    )(*operands, *extra, *deps)


def ffn(base, count, hidden, cotangent, hat, rstd, weights, previous, deps):
    total, seq_len, width = hidden.shape
    wide = weights[0].shape[1]
    operands = (hidden, cotangent, hat, rstd) + tuple(weights)
    extra = tuple(previous) if previous is not None else ()
    specs = [per_seq(item.shape[1:], base) for item in operands[:4]] + [whole(item.shape) for item in operands[4:]]
    specs += [ANYWHERE] * (len(extra) + len(deps))
    big = jax.ShapeDtypeStruct((total * seq_len, wide), BF16)
    narrow = jax.ShapeDtypeStruct((total, seq_len, width), BF16)
    flops = 12 * count * seq_len * width * wide
    return pl.pallas_call(
        functools.partial(ffn_kernel, base),
        grid=(count,),
        in_specs=specs,
        out_specs=[ANYWHERE] * 3 + [per_seq((seq_len, width), base)] * 3 + [pl.BlockSpec((40, width), lambda i: (0, 0)), pl.BlockSpec((16, wide), lambda i: (0, 0)), token_spec()],
        out_shape=[big] * 3 + [narrow, jax.ShapeDtypeStruct((total, seq_len, width), F32), narrow,
                               jax.ShapeDtypeStruct((40, width), F32), jax.ShapeDtypeStruct((16, wide), F32), jax.ShapeDtypeStruct(TOKEN, F32)],
        scratch_shapes=[pltpu.VMEM((seq_len, wide), F32)] * 2 + [pltpu.VMEM((seq_len, wide), BF16)] * 3
        + [pltpu.VMEM((seq_len, width), F32), pltpu.SemaphoreType.DMA((3, wide // FFN_CHUNK))],
        input_output_aliases={len(operands) + num: num for num in range(len(extra))},
        compiler_params=params(),
        cost_estimate=cost(int(1.5 * flops), count * 14_000_000),
        name='ffn',
    )(*operands, *extra, *deps)


def attn_backward(base, count, total, d_resid, d_attn, qkv, probs, weights, tables, previous, deps, head_dim):
    seq_len, width = d_resid.shape[1:]
    wqkv, wout = weights
    heads = width // head_dim
    operands = (d_resid, d_attn, qkv, probs, wqkv, wout) + tuple(tables)
    specs = [per_seq(item.shape[1:], base) for item in operands[:4]] + [whole(item.shape) for item in operands[4:]]
    extra = tuple(previous) if previous is not None else ()
    specs += [ANYWHERE] * (len(extra) + len(deps))
    flops = count * (2 * seq_len * width * (wqkv.shape[1] + width) + 8 * heads * seq_len * seq_len * 64)
    return pl.pallas_call(
        functools.partial(attn_backward_kernel, head_dim, len(extra) + len(deps)),
        grid=(count,),
        in_specs=specs,
        out_specs=[per_seq((seq_len, width)), per_seq((seq_len, wqkv.shape[1]), base), per_seq((seq_len, width), base), pl.BlockSpec((8, wqkv.shape[1]), lambda i: (0, 0)), token_spec()],
        out_shape=[jax.ShapeDtypeStruct((count, seq_len, width), F32), jax.ShapeDtypeStruct((total, seq_len, wqkv.shape[1]), BF16),
                   jax.ShapeDtypeStruct((total, seq_len, width), F32),
                   jax.ShapeDtypeStruct((8, wqkv.shape[1]), F32), jax.ShapeDtypeStruct(TOKEN, F32)],
        input_output_aliases={len(operands) + num: 1 + num for num in range(len(extra))},
        compiler_params=params(),
        cost_estimate=cost(2 * flops, count * 12_000_000),
        name='attn_backward',
    )(*operands, *extra, *deps)


def outer_kernel(own_ref, left_ref, right_ref, *refs):
    out_ref, token_ref, left_t = refs[-3:]
    clear(token_ref)

    @pl.when(pl.program_id(0) == 0)
    def _():
        def turn(index, carry):
            rows = pl.ds(pl.multiple_of(index * CHUNK, CHUNK), CHUNK)
            left_t[:, rows] = left_ref[rows, :].astype(F32).T.astype(BF16)
            return carry

        lax.fori_loop(0, left_ref.shape[0] // CHUNK, turn, 0)

    out_ref[...] = dot_nn(full(left_t), full(right_ref))


def outer(left, right, block, shape, slot, index, previous, deps):
    rows, width = left.shape
    wide = right.shape[1]
    per_half = wide // (2 * block)
    extra = (previous,) if previous is not None else ()
    grid_spec = pltpu.PrefetchScalarGridSpec(
        num_scalar_prefetch=1,
        grid=(wide // block,),
        in_specs=[pl.BlockSpec((rows, width), lambda i, own: (0, 0), pipeline_mode=pl.Buffered(1)), pl.BlockSpec((rows, block), lambda i, own: (0, i))]
        + [ANYWHERE] * (len(extra) + len(deps)),
        out_specs=[pl.BlockSpec((None, width, block), lambda i, own: ((i // per_half + own[0]) % 2, 0, slot + i % per_half)),
                   pl.BlockSpec(TOKEN, lambda i, own: (0, 0))],
        scratch_shapes=[pltpu.VMEM((width, rows), BF16)])
    return pl.pallas_call(
        outer_kernel,
        grid_spec=grid_spec,
        out_shape=[jax.ShapeDtypeStruct(shape, F32), jax.ShapeDtypeStruct(TOKEN, F32)],
        input_output_aliases={3 + num: num for num in range(len(extra))},
        compiler_params=params(),
        cost_estimate=cost(2 * rows * width * wide, 4 * width * wide + 2 * rows * (width + wide)),
        name='outer',
    )(index, left, right, *extra, *deps)


def groups_of(start, stop, size):
    return [(base, size) for base in range(start, stop, size)]


def join_kernel(plain, peer_ref, *refs):
    owns, outs = refs[:len(refs) // 2], refs[len(refs) // 2:]
    start = 0
    for num, (own_ref, out_ref) in enumerate(zip(owns, outs)):
        half = out_ref.shape[1] // 2
        out_ref[:, :half] = full(own_ref) if num < plain else full(own_ref).astype(F32).T.astype(BF16)
        out_ref[:, half:] = peer_ref[:, start:start + half].astype(BF16)
        start += half


def join(peer, plain, flipped):
    owns = tuple(plain) + tuple(flipped)
    rows = peer.shape[0]
    halves = [item.shape[1] for item in plain] + [item.shape[0] for item in flipped]
    return pl.pallas_call(
        functools.partial(join_kernel, len(plain)),
        grid=(rows // LANES,),
        in_specs=[pl.BlockSpec((LANES, peer.shape[1]), lambda i: (i, 0))] + [pl.BlockSpec((LANES, item.shape[1]), lambda i: (i, 0)) for item in plain]
        + [pl.BlockSpec((item.shape[0], LANES), lambda i: (0, i)) for item in flipped],
        out_specs=[pl.BlockSpec((LANES, 2 * half), lambda i: (i, 0)) for half in halves],
        out_shape=[jax.ShapeDtypeStruct((rows, 2 * half), BF16) for half in halves],
        compiler_params=params(),
        cost_estimate=cost(peer.size * 64, peer.size * 10),
        name='join_weights',
    )(peer, *owns)


def shared_slice(plain, flipped, index, parts):
    rows = plain[0].shape[0] // parts
    pieces = [lax.dynamic_slice_in_dim(item, index * rows, rows, 0) for item in plain]
    pieces += [lax.dynamic_slice_in_dim(item, index * rows, rows, 1).T for item in flipped]
    return jnp.concatenate(pieces, axis=1).astype(F32)


def row_pieces(rows):
    tiles = rows // TILE
    cuts = [num * tiles // PIECES * TILE for num in range(PIECES + 1)]
    return [(first, last - first) for first, last in zip(cuts, cuts[1:])]


def table_kernel(src, out, away, keep, got_one, got_two, stage, load_sems, store_sems, swap_sems, one_sems, two_sems, near_sems, far_sems, back_sems):
    me = lax.axis_index('dp')
    core, col, line = me % 2, me // 2 % 2, me // 4
    partner, x_peer, y_peer = me + 1 - 2 * core, me + 2 - 4 * col, me + 4 - 8 * line
    first_peer = x_peer + core * (y_peer - x_peer)
    second_peer = y_peer + core * (x_peer - y_peer)
    one = col + core * (line - col)
    two = line + core * (col - line)
    eighth = src.shape[0] // 8
    pieces = row_pieces(eighth)
    jobs = [(part, num) for part in range(4) for num in range(PIECES)]

    barrier = pltpu.get_barrier_semaphore()
    for peer in (partner, x_peer, y_peer):
        pl.semaphore_signal(barrier, inc=1, device_id={'dp': peer}, device_id_type=pl.DeviceIdType.MESH)
    pl.semaphore_wait(barrier, 3)

    def send(source, target, sems, slot, peer):
        return pltpu.make_async_remote_copy(src_ref=source, dst_ref=target, send_sem=sems.at[0, slot], recv_sem=sems.at[1, slot],
                                            device_id={'dp': peer}, device_id_type=pl.DeviceIdType.MESH)

    def table_rows(ref, half, quarter, last, num):
        start, size = pieces[num]
        return ref.at[pl.ds(pl.multiple_of((half * 4 + quarter * 2 + last) * eighth + start, TILE), size)]

    def part_rows(ref, half, quarter, last, part, num):
        return table_rows(ref, half, 1 - quarter if part < 2 else quarter, last if part % 2 else 1 - last, num)

    def buffer_rows(ref, part, num):
        start, size = pieces[num]
        return ref.at[pl.ds(part % 2 * eighth + start, size)]

    def holder(part):
        return away if part < 2 else keep

    def add_into(target, part, source, source_part, num):
        start, size = pieces[num]
        to, of = part % 2 * eighth + start, source_part * eighth + start

        def body(index, carry):
            offset = index * TILE
            target[pl.ds(pl.multiple_of(to + offset, TILE), TILE)] += source[pl.ds(pl.multiple_of(of + offset, TILE), TILE)]
            return carry

        lax.fori_loop(0, size // TILE, body, 0)

    swaps = [send(part_rows(src, 1 - core, two, one, part, num), buffer_rows(holder(part), part, num), swap_sems, slot, partner)
             for slot, (part, num) in enumerate(jobs)]
    loads = [pltpu.make_async_copy(part_rows(src, core, one, two, part, num), stage.at[slot % 2, pl.ds(0, pieces[num][1])], load_sems.at[slot % 2])
             for slot, (part, num) in enumerate(jobs)]
    firsts = [send(buffer_rows(away, part, num), buffer_rows(got_one, part, num), one_sems, slot, first_peer)
              for slot, (part, num) in enumerate(jobs[:2 * PIECES])]
    seconds = [send(buffer_rows(keep, 0, num), buffer_rows(got_two, 0, num), two_sems, num, second_peer) for num in range(PIECES)]

    for copy in swaps:
        copy.start()
    loads[0].start()
    for slot, (part, num) in enumerate(jobs):
        if slot + 1 < len(jobs):
            loads[slot + 1].start()
        loads[slot].wait()
        swaps[slot].wait_recv()
        start, size = pieces[num]
        target, held, to = holder(part), stage.at[slot % 2], part % 2 * eighth + start

        def body(index, carry, target=target, held=held, to=to):
            offset = index * TILE
            target[pl.ds(pl.multiple_of(to + offset, TILE), TILE)] += held[pl.ds(pl.multiple_of(offset, TILE), TILE)]
            return carry

        lax.fori_loop(0, size // TILE, body, 0)
        if 0 < slot <= len(firsts):
            firsts[slot - 1].start()

    for slot in range(2 * PIECES):
        firsts[slot].wait_recv()
        add_into(keep, slot // PIECES, got_one, slot // PIECES, slot % PIECES)
        if 0 < slot <= PIECES:
            seconds[slot - 1].start()

    done = []

    def publish(num):
        mine = buffer_rows(keep, 1, num)
        place = table_rows(out, core, one, two, num)
        copies = [pltpu.make_async_copy(mine, place, store_sems.at[num]), send(mine, place, near_sems, num, second_peer),
                  send(mine, place, far_sems, num, first_peer), send(mine, place, back_sems, num, partner)]
        for copy in copies:
            copy.start()
        done.append(copies)

    for num in range(PIECES):
        seconds[num].wait_recv()
        add_into(keep, 1, got_two, 0, num)
        if num:
            publish(num - 1)
    publish(PIECES - 1)

    def forward(quarter, last, num, sems, slot, peer, start=True):
        place = table_rows(out, core, quarter, last, num)
        copy = send(place, place, sems, slot, peer)
        if start:
            copy.start()
        return copy

    relays = []
    for num in range(PIECES):
        forward(one, 1 - two, num, near_sems, num, second_peer, False).wait_recv()
        relays.append(forward(one, 1 - two, num, far_sems, PIECES + num, first_peer))
        relays.append(forward(one, 1 - two, num, back_sems, PIECES + num, partner))
        forward(1 - one, two, num, far_sems, num, first_peer, False).wait_recv()
        relays.append(forward(1 - one, two, num, back_sems, 2 * PIECES + num, partner))
    for num in range(PIECES):
        forward(1 - one, 1 - two, num, far_sems, PIECES + num, first_peer, False).wait_recv()
        relays.append(forward(1 - one, 1 - two, num, back_sems, 3 * PIECES + num, partner))
    for slot, (part, num) in enumerate(jobs):
        place = table_rows(out, 1 - core, two if part < 2 else 1 - two, 1 - one if part % 2 else one, num)
        send(place, place, back_sems, slot, partner).wait_recv()
    for copy in swaps + firsts + seconds + relays:
        copy.wait_send()
    for local, *remote in done:
        local.wait()
        for copy in remote:
            copy.wait_send()


def reduce_table(table):
    rows, width = table.shape
    eighth = rows // 8
    largest = max(size for _, size in row_pieces(eighth))
    buffers = [pltpu.VMEM((count * eighth, width), F32) for count in (2, 2, 2, 1)]
    counts = (4 * PIECES, 2 * PIECES, PIECES, PIECES, 2 * PIECES, 4 * PIECES)
    return pl.pallas_call(
        table_kernel,
        in_specs=[ANYWHERE],
        out_specs=ANYWHERE,
        out_shape=jax.ShapeDtypeStruct(table.shape, F32),
        scratch_shapes=buffers + [pltpu.VMEM((2, largest, width), F32), pltpu.SemaphoreType.DMA((2,)), pltpu.SemaphoreType.DMA((PIECES,))]
        + [pltpu.SemaphoreType.DMA((2, count)) for count in counts],
        compiler_params=pltpu.CompilerParams(collective_id=0, has_side_effects=True, vmem_limit_bytes=VMEM_LIMIT),
        cost_estimate=cost(400_000_000_000, rows * width * 8),
        name='reduce_table',
    )(table)


def reduce_gradient(grad):
    piece = lax.psum_scatter(grad.reshape(-1, grad.shape[2]), ('tp', 'dp'), scatter_dimension=0, tiled=True)
    return lax.all_gather(piece, 'dp', axis=0, tiled=True)


def tie(value, token):
    return lax.optimization_barrier((value, token))[0]


def solution(mesh):
    in_specs = (P('dp'), P('dp'), ROWS) + WEIGHT_SPECS
    out_specs = (ROWS,) + WEIGHT_SPECS
    parts = mesh.shape['dp']

    def device_step(tokens, cotangent, emb_table, *weights):
        (w_qkv, b_qkv, w_out, b_out, ln1_gain, ln1_bias, w_gate, b_gate, w_lin, b_lin, w_down, b_down, ln2_gain) = weights
        tp_index, dp_index = lax.axis_index('tp'), lax.axis_index('dp')
        vocab_loc, width = emb_table.shape
        head_dim = b_qkv.shape[1] // 3
        seq_len = tokens.shape[1]
        total = tokens.shape[0] // 2

        local_ids = tokens - tp_index * vocab_loc
        in_shard = (local_ids >= 0) & (local_ids < vocab_loc)
        own_ids = lax.dynamic_slice_in_dim(local_ids, tp_index * total, total)
        own_in = lax.dynamic_slice_in_dim(in_shard, tp_index * total, total)
        peer_ids = lax.dynamic_slice_in_dim(local_ids, (1 - tp_index) * total, total)
        peer_in = lax.dynamic_slice_in_dim(in_shard, (1 - tp_index) * total, total)
        own_cot = lax.dynamic_slice_in_dim(cotangent, tp_index * total, total)

        def rows_of(part, head):
            ids = jnp.concatenate([peer_ids[part], own_ids[part]])
            rows = jnp.take(emb_table, tie(jnp.where((ids >= 0) & (ids < vocab_loc), ids, 0), head), axis=0)
            peer_rows, own_rows = (jnp.where(inside[part][:, :, None], piece, 0.0) for inside, piece in zip((peer_in, own_in), jnp.split(rows, 2)))
            return peer_rows.astype(F32), own_rows

        def exchange(value):
            return lax.ppermute(value, 'tp', SWAP)

        def collect(value):
            value = exchange(value)
            return lax.all_gather(value, 'dp', axis=0, tiled=True)

        def row_of(vector):
            return vector.astype(F32).reshape(1, -1)

        half = total // 2
        qkv_loc, wide_loc = b_qkv.size, b_gate.shape[0]
        groups = [(num, 1) for num in range(half)] + groups_of(half, total, 2)

        first_rows = rows_of(slice(half), tp_index)
        rest_rows = rows_of(slice(half, total), first_rows)
        peer_halves, own_halves = zip(first_rows, rest_rows)
        front_peer = collect(shared_slice((w_qkv,), (w_out,), dp_index, parts))
        own_bias = jnp.concatenate([row_of(b_qkv), row_of(b_gate), row_of(b_lin)], axis=1)
        biases = jnp.concatenate([own_bias, exchange(own_bias)])
        wide_peer = collect(shared_slice((w_gate, w_lin), (w_down,), dp_index, parts))
        arrived = [exchange(peer_halves[base // half][base % half:base % half + count]) for base, count in groups]
        bqkv_full = biases[:, :qkv_loc].reshape(1, -1)
        bgate_full = biases[:, qkv_loc:qkv_loc + wide_loc].reshape(1, -1)
        blin_full = biases[:, qkv_loc + wide_loc:].reshape(1, -1)
        wqkv_full, wout_full = join(front_peer, (w_qkv,), (w_out,))
        wide_full = join(wide_peer, (w_gate, w_lin), (w_down,))

        half_dim = head_dim // 2
        inv_freq = ROPE_BASE ** (-2.0 * jnp.arange(half_dim, dtype=F32) / head_dim)
        angles = jnp.arange(seq_len, dtype=F32)[:, None] * inv_freq[None, :]
        cos_half, sin_half = jnp.cos(angles), jnp.sin(angles)
        tables = (jnp.concatenate([cos_half] * 4, axis=1), jnp.concatenate([-sin_half, sin_half] * 2, axis=1))

        front = (wqkv_full, bqkv_full, wout_full, row_of(b_out), row_of(ln1_gain), row_of(ln1_bias))
        middle = tuple(wide_full) + (bgate_full, blin_full, row_of(b_down), row_of(ln1_gain), row_of(ln2_gain))
        saved, ffn_saved, d_kept, deps = None, None, None, ()
        narrow_parts, wide_parts, bias_parts, d_peer = [], [], [], []

        def run_attention(num):
            nonlocal saved, deps
            base, count = groups[num]
            out = attn_forward(base, count, total, own_halves[base // half], base % half, arrived[num], front, tables, saved, deps, head_dim)
            *kept, token = out
            saved, deps = kept, (token,)

        def run_ffn(base, count):
            nonlocal ffn_saved, deps
            *_, hat, rstd, hidden = saved
            *kept, narrow, wide, token = ffn(base, count, hidden, own_cot, hat, rstd, middle, ffn_saved, deps)
            ffn_saved, deps = kept, (token,)
            narrow_parts.append(narrow)
            wide_parts.append(wide)

        def run_backward(base, count):
            nonlocal d_kept, deps
            _, qkv, probs, *_ = saved
            *_, d_resid, d_attn = ffn_saved
            d_emb, d_qkv, d_all, bias_part, token = attn_backward(base, count, total, d_resid, d_attn, qkv, probs, (wqkv_full, wout_full), tables, d_kept, deps, head_dim)
            d_kept, deps = (d_qkv, d_all), (token,)
            bias_parts.append(bias_part)
            d_peer.append(exchange(d_emb))

        def run_outer(left, right, block, shape, slot, previous):
            nonlocal deps
            out, token = outer(left.reshape(-1, left.shape[-1]), right.reshape(-1, right.shape[-1]), block, shape, slot, half_index, previous, deps)
            deps = (token,)
            return out

        for num in range(half + 2):
            run_attention(num)
            if num % 2 and num < half:
                run_ffn(num - 1, 2)
        run_backward(0, half)
        run_ffn(half, half)
        inner, d_gate, d_lin, d_ffn, _, d_attn = ffn_saved
        emb, _, _, context, _, _, hidden = saved
        half_index = tp_index.reshape(1)
        shape = (2, width, 3 * wide_loc)
        step = wide_loc // CHUNK
        grads = run_outer(hidden, d_gate, CHUNK, shape, 0, None)
        grads = run_outer(hidden, d_lin, CHUNK, shape, step, grads)
        grads = run_outer(d_ffn, inner, CHUNK, shape, 2 * step, grads)
        wide_grads = reduce_gradient(grads)
        for base, count in groups_of(half, total, 2):
            run_backward(base, count)
        block = w_out.shape[0]
        shape = (2, width + parts * TILE, qkv_loc + block)
        d_qkv, d_all = d_kept
        grads = run_outer(d_attn, context, block, shape, qkv_loc // block, None)
        grads = run_outer(emb, d_qkv, qkv_loc, shape, 0, grads)

        narrow = jnp.sum(sum(narrow_parts).reshape(5, 8, -1), axis=1).reshape(1, -1)
        d_bwide = jnp.sum(sum(wide_parts).reshape(2, 8, -1), axis=1).reshape(2, 2, -1)
        small = jnp.concatenate([jnp.sum(sum(bias_parts), axis=0).reshape(2, -1), d_bwide[0], d_bwide[1], jnp.concatenate([narrow] * 2)], axis=1)
        used = small.shape[1]
        small = jnp.pad(small, ((0, 0), (0, TILE * (qkv_loc + block) - used))).reshape(2, TILE, -1)
        small = jnp.where(tp_index == 0, small, small[::-1])
        grads = lax.dynamic_update_slice(grads, small, (0, width, 0))
        front_grads = reduce_gradient(grads)

        own_row_ids = jnp.where(own_in, own_ids, vocab_loc)
        peer_row_ids = jnp.where(peer_in, peer_ids, vocab_loc)

        def add_rows(grad, ids, rows):
            return grad.at[ids.reshape(-1)].add(rows.reshape(-1, width), mode='drop')

        d_table = add_rows(jnp.zeros((vocab_loc, width), F32), tie(own_row_ids, *deps), d_all)
        d_table = add_rows(d_table, peer_row_ids, jnp.concatenate(d_peer, axis=0))
        d_table = reduce_table(d_table)

        small = front_grads[width:width + TILE].reshape(-1)
        d_b_qkv = small[:qkv_loc].reshape(b_qkv.shape)
        d_b_gate = small[qkv_loc:qkv_loc + wide_loc]
        d_b_lin = small[qkv_loc + wide_loc:qkv_loc + 2 * wide_loc]
        d_ln2_gain, d_b_down, d_ln1_bias, d_ln1_gain, d_b_out = small[qkv_loc + 2 * wide_loc:used].reshape(5, width)
        d_w_gate, d_w_lin, d_w_down = (wide_grads[:, num * wide_loc:(num + 1) * wide_loc] for num in range(3))
        d_w_qkv, d_w_out = front_grads[:width, :qkv_loc], front_grads[:width, qkv_loc:]
        return (d_table, d_w_qkv, d_b_qkv, d_w_out.T, d_b_out, d_ln1_gain, d_ln1_bias, d_w_gate, d_b_gate, d_w_lin, d_b_lin, d_w_down.T, d_b_down, d_ln2_gain)

    return jax.shard_map(device_step, mesh=mesh, in_specs=in_specs, out_specs=out_specs, check_vma=False)
```

```python
import functools

import jax
import jax.numpy as jnp
from jax import lax
from jax.experimental import pallas as pl
from jax.experimental.pallas import tpu as pltpu
from jax.sharding import PartitionSpec as P


ALPHA = 140.0 ** 0.5
EPS = 1e-5
SHRINK = 0.1
ROPE_BASE = 10000.0
COLS, ROWS, ALL = P(None, 'tp'), P('tp'), P()
WEIGHT_SPECS = (COLS, ROWS, ROWS, ALL, ALL, ALL, COLS, ROWS, COLS, ROWS, ROWS, ALL, ALL)

F32 = jnp.float32
BF16 = jnp.bfloat16
LANES = 128
HALF_Q = 256
CHUNK = 512
FFN_CHUNK = 768
TILE = 8
PIECES = 3
VMEM_LIMIT = 66 * 1024 * 1024 - 512 * 1024
LOG2E = 1.4426950408889634
MASKED = -8e30
NT = (((1,), (1,)), ((), ()))
NN = (((1,), (0,)), ((), ()))
SWAP = ((0, 1), (1, 0))


def dot_nn(left, right):
    return lax.dot_general(left, right, NN, preferred_element_type=F32)


def dot_nt(left, right):
    return lax.dot_general(left, right, NT, preferred_element_type=F32)


def row_sums(values):
    return jnp.sum(values.reshape(-1, TILE, values.shape[1]), axis=0)


def row_mean(values):
    return jnp.mean(values, axis=-1, keepdims=True)


def col_sum(values):
    return jnp.sum(values, axis=0, keepdims=True)


def add_sums(ref, slot, values):
    ref[slot * TILE:(slot + 1) * TILE] += row_sums(values)


def full(ref):
    return ref[...]


def clear(ref):
    ref[...] = jnp.zeros_like(ref)


def normalize(values):
    centered = values - row_mean(values)
    rstd = lax.rsqrt(row_mean(centered * centered) + EPS)
    return centered * rstd, rstd


def normalize_back(d_hat, hat, rstd):
    return rstd * (d_hat - row_mean(d_hat) - hat * row_mean(d_hat * hat))


def rope(values, cos_tab, sin_tab, first_half):
    partner = jnp.where(first_half, pltpu.roll(values, 96, 1), pltpu.roll(values, 32, 1))
    return values * cos_tab + partner * sin_tab


def lane_masks():
    lane = lax.broadcasted_iota(jnp.int32, (1, LANES), 1)
    low = lane < 64
    return low, low.astype(F32).astype(BF16), (1.0 - low.astype(F32)).astype(BF16), (lane % 64) < 32


def attn_forward_kernel(head_dim, alias_count, *refs):
    (own_ref, other_ref, mask_ref, wqkv_ref, bqkv_ref, wo_ref, bo_ref, gain_ref, bias_ref, cos_ref, sin_ref) = refs[:11]
    (emb_ref, qkv_ref, prob_ref, ctx_ref, hat_ref, rstd_ref, hid_ref, token_ref) = refs[11 + alias_count:]
    seq_len, width = own_ref.shape
    clear(token_ref)
    emb_ref[...] = jnp.where(mask_ref[:, :1] > 0, full(own_ref).astype(F32), full(other_ref)).astype(BF16)
    low, mask_low, mask_high, first_half = lane_masks()
    score_scale = head_dim ** -0.5 * LOG2E
    causal = lax.broadcasted_iota(jnp.int32, (HALF_Q, HALF_Q), 0) <= lax.broadcasted_iota(jnp.int32, (HALF_Q, HALF_Q), 1)
    step = 4 * 3 * head_dim

    def quad(index, carry):
        col = pl.multiple_of(index * step, step)
        pre = dot_nn(full(emb_ref), wqkv_ref[:, pl.ds(col, step)]) + bqkv_ref[:, pl.ds(col, step)]
        pre = pre.astype(BF16).astype(F32)
        for half in range(2):
            parts = [pre[:, (half * 3 + part) * LANES:(half * 3 + part + 1) * LANES] for part in range(3)]
            pair = index * 2 + half
            pair_col = pl.multiple_of(pair * LANES, LANES)
            q_pair = jnp.where(low, parts[0], parts[1])
            k_pair = pltpu.roll(jnp.where(low, parts[2], parts[0]), 64, 1)
            v_pair = jnp.where(low, parts[1], parts[2])
            q_rot = rope(q_pair, full(cos_ref), full(sin_ref), first_half).astype(BF16)
            k_rot = rope(k_pair, full(cos_ref), full(sin_ref), first_half).astype(BF16)
            qkv_ref[:, pl.ds(pair_col, LANES)] = q_rot
            qkv_ref[:, pl.ds(width + pair_col, LANES)] = k_rot
            qkv_ref[:, pl.ds(2 * width + pair_col, LANES)] = v_pair.astype(BF16)
            v_trans = v_pair.T.astype(BF16)
            ctx_rows = []
            for head in range(2):
                k_one = k_rot * (mask_low if head == 0 else mask_high)
                v_one = v_trans[head * 64:(head + 1) * 64]
                blocks = []
                for block in range(2):
                    q_block = q_rot[block * HALF_Q:(block + 1) * HALF_Q]
                    diag = jnp.where(causal, dot_nt(k_one[block * HALF_Q:(block + 1) * HALF_Q], q_block), MASKED)
                    pieces = [diag] if block == 0 else [dot_nt(k_one[:HALF_Q], q_block), diag]
                    peak = functools.reduce(jnp.maximum, [jnp.max(piece, axis=0, keepdims=True) for piece in pieces])
                    exps = [jnp.exp2((piece - peak) * score_scale) for piece in pieces]
                    total = functools.reduce(jnp.add, [col_sum(piece) for piece in exps])
                    inverse = 1.0 / total
                    ctx = None
                    for num, piece in enumerate(exps):
                        prob = (piece * inverse).astype(BF16)
                        prob_ref[pair * 2 + head, (block + num) * HALF_Q:(block + num + 1) * HALF_Q, :] = prob
                        term = dot_nn(v_one[:, num * HALF_Q:(num + 1) * HALF_Q], prob)
                        ctx = term if ctx is None else ctx + term
                    blocks.append(ctx)
                ctx_rows.append(jnp.concatenate(blocks, axis=1))
            ctx_pair = jnp.concatenate(ctx_rows, axis=0)
            ctx_ref[:, pl.ds(pair_col, LANES)] = ctx_pair.T.astype(BF16)
        return carry

    lax.fori_loop(0, wqkv_ref.shape[1] // step, quad, 0)
    attn = dot_nt(full(ctx_ref), full(wo_ref)) + full(bo_ref)
    resid = ALPHA * full(emb_ref).astype(F32) + attn
    hat, rstd = normalize(resid)
    hat_ref[...] = hat
    rstd_ref[...] = jnp.broadcast_to(rstd, (seq_len, LANES))
    hid_ref[...] = (hat * full(gain_ref) + full(bias_ref)).astype(BF16)


def ffn_kernel(base, half_ref, hid_ref, cot_ref, hat_ref, rstd_ref, wg_ref, wl_ref, wd_ref, bg_ref, bl_ref, bd_ref, gain1_ref, gain2_ref,
               *refs):
    (inner_out, gate_out, lin_out, dffn_ref, dres_ref, dattn_ref, narrow_ref, wide_ref, token_ref,
     act_buf, slope_buf, inner_buf, gate_buf, lin_buf, acc_buf, sems) = refs[-16:]
    step = pl.program_id(0)
    last = pl.num_programs(0) - 1
    clear(token_ref)
    rows, _ = hid_ref.shape
    chunks = wg_ref.shape[1] // FFN_CHUNK

    def copy_out(buf, out, kind, chunk, block):
        cols = pl.ds(pl.multiple_of(chunk * FFN_CHUNK, FFN_CHUNK), FFN_CHUNK)
        return pltpu.make_async_copy(buf.at[:, cols], out.at[pl.ds((block + base) * rows, rows), cols], sems.at[kind, chunk])

    @pl.when(step == 0)
    def _():
        clear(narrow_ref)
        clear(wide_ref)

    outputs = ((inner_buf, inner_out, 0), (gate_buf, gate_out, 1), (lin_buf, lin_out, 2))

    def drain(copies, block):
        def body(chunk, carry):
            for buf, out, kind in copies:
                copy_out(buf, out, kind, chunk, block).wait()
            return carry

        lax.fori_loop(0, chunks, body, 0)

    @pl.when(step > 0)
    def _():
        drain(outputs, step - 1)

    clear(acc_buf)

    def forward(chunk, carry):
        cols = pl.ds(pl.multiple_of(chunk * FFN_CHUNK, FFN_CHUNK), FFN_CHUNK)
        gate_pre = dot_nn(full(hid_ref), wg_ref[:, cols]) + bg_ref[:, cols]
        lin_pre = dot_nn(full(hid_ref), wl_ref[:, cols]) + bl_ref[:, cols]
        cdf = 0.5 + 0.5 * lax.erf(gate_pre * (0.5 ** 0.5))
        act = gate_pre * cdf
        pdf = jnp.exp2(gate_pre * gate_pre * (-0.5 * LOG2E)) * 0.3989422804014327
        act_buf[:, cols] = act
        slope_buf[:, cols] = lin_pre * (cdf + gate_pre * pdf)

        inner = (act * lin_pre).astype(BF16)
        inner_buf[:, cols] = inner
        acc_buf[...] += dot_nt(inner, wd_ref[:, cols])
        copy_out(inner_buf, inner_out, 0, chunk, step).start()
        return carry

    lax.fori_loop(0, chunks, forward, 0)
    resid = ALPHA * full(hid_ref).astype(F32) + (full(acc_buf) + full(bd_ref))
    hat, rstd = normalize(resid)
    cot = full(cot_ref).astype(F32)
    add_sums(narrow_ref, 0, cot * hat)
    d_hat = cot * full(gain2_ref)
    d_resid = normalize_back(d_hat, hat, rstd)
    add_sums(narrow_ref, 1, d_resid)
    dffn_ref[...] = d_resid.astype(BF16)
    acc_buf[...] = ALPHA * d_resid

    def backward(chunk, carry):
        cols = pl.ds(pl.multiple_of(chunk * FFN_CHUNK, FFN_CHUNK), FFN_CHUNK)
        d_inner = dot_nn(full(dffn_ref), wd_ref[:, cols]).astype(BF16).astype(F32)
        d_gate = d_inner * slope_buf[:, cols]
        d_lin = d_inner * act_buf[:, cols]
        add_sums(wide_ref.at[:, cols], 0, d_gate)
        add_sums(wide_ref.at[:, cols], 1, d_lin)

        d_gate = d_gate.astype(BF16)
        d_lin = d_lin.astype(BF16)
        gate_buf[:, cols] = d_gate
        lin_buf[:, cols] = d_lin
        acc_buf[...] += dot_nt(d_gate, wg_ref[:, cols]) + dot_nt(d_lin, wl_ref[:, cols])
        copy_out(gate_buf, gate_out, 1, chunk, step).start()
        copy_out(lin_buf, lin_out, 2, chunk, step).start()
        return carry

    lax.fori_loop(0, chunks, backward, 0)
    d_hid = full(acc_buf)
    hat = full(hat_ref)
    add_sums(narrow_ref, 2, d_hid)
    add_sums(narrow_ref, 3, d_hid * hat)
    d_hat = d_hid * full(gain1_ref)
    d_resid = normalize_back(d_hat, hat, rstd_ref[:, :1])
    add_sums(narrow_ref, 4, d_resid)
    dres_ref[...] = d_resid
    dattn_ref[...] = d_resid.astype(BF16)

    @pl.when(step == last)
    def _():
        drain(outputs, step)


def attn_backward_kernel(head_dim, alias_count, *refs):
    (dres_ref, dattn_ref, qkv_ref, prob_ref, wqkv_ref, wo_ref, cos_ref, sin_ref) = refs[:8]
    (demb_ref, dqkv_ref, dall_ref, acc_ref, token_ref) = refs[8 + alias_count:]
    clear(token_ref)
    width = dres_ref.shape[1]
    low, mask_low, mask_high, first_half = lane_masks()
    attn_scale = head_dim ** -0.5
    step = 4 * 3 * head_dim

    @pl.when(pl.program_id(0) == 0)
    def _():
        clear(acc_ref)

    def quad(index, carry):
        col = pl.multiple_of(index * step, step)
        ctx_row = pl.multiple_of(index * 4 * head_dim, 4 * head_dim)
        d_ctx_quad = dot_nn(full(dattn_ref), wo_ref[:, pl.ds(ctx_row, 4 * head_dim)]).astype(BF16)
        pieces = []
        for half in range(2):
            pair = index * 2 + half
            pair_col = pl.multiple_of(pair * LANES, LANES)
            d_ctx = d_ctx_quad[:, half * LANES:(half + 1) * LANES]
            q_rot = qkv_ref[:, pl.ds(pair_col, LANES)]
            k_rot = qkv_ref[:, pl.ds(width + pair_col, LANES)]
            v_pair = qkv_ref[:, pl.ds(2 * width + pair_col, LANES)]
            k_trans = k_rot.astype(F32).T.astype(BF16)
            dq_rows, dk_heads, dv_heads = [], [], []
            for head in range(2):
                v_one = v_pair * (mask_low if head == 0 else mask_high)
                k_one = k_trans[head * 64:(head + 1) * 64]
                d_v, d_k, d_q = [None, None], [None, None], []
                for block in range(2):
                    rows = slice(block * HALF_Q, (block + 1) * HALF_Q)
                    keys = range(block + 1)
                    probs = [prob_ref[pair * 2 + head, (block + num) * HALF_Q:(block + num + 1) * HALF_Q, :] for num in keys]
                    d_probs = [dot_nt(v_one[num * HALF_Q:(num + 1) * HALF_Q], d_ctx[rows]) for num in keys]
                    wide = [prob.astype(F32) for prob in probs]
                    inner = functools.reduce(jnp.add, [col_sum(d_prob * prob) for d_prob, prob in zip(d_probs, wide)])
                    d_q_block = None
                    for num in keys:
                        d_score = (wide[num] * (d_probs[num] - inner) * attn_scale).astype(BF16)
                        terms = (dot_nn(probs[num], d_ctx[rows]), dot_nn(d_score, q_rot[rows]), dot_nn(k_one[:, num * HALF_Q:(num + 1) * HALF_Q], d_score))
                        d_v[num] = terms[0] if d_v[num] is None else d_v[num] + terms[0]
                        d_k[num] = terms[1] if d_k[num] is None else d_k[num] + terms[1]
                        d_q_block = terms[2] if d_q_block is None else d_q_block + terms[2]
                    d_q.append(d_q_block)
                dq_rows.append(jnp.concatenate(d_q, axis=1))
                dk_heads.append(jnp.concatenate(d_k, axis=0))
                dv_heads.append(jnp.concatenate(d_v, axis=0))
            d_q = rope(jnp.concatenate(dq_rows, axis=0).T, full(cos_ref), -full(sin_ref), first_half)
            d_k = rope(jnp.where(low, dk_heads[0], dk_heads[1]), full(cos_ref), -full(sin_ref), first_half)
            d_v = jnp.where(low, dv_heads[0], dv_heads[1])
            d_k = pltpu.roll(d_k, 64, 1)
            pieces += [jnp.where(low, d_q, d_k), jnp.where(low, d_v, d_q), jnp.where(low, d_k, d_v)]
        for num, piece in enumerate(pieces):
            lanes = pl.ds(col + num * LANES, LANES)
            acc_ref[:, lanes] += row_sums(piece)
            dqkv_ref[:, lanes] = piece.astype(BF16)
        return carry

    lax.fori_loop(0, wqkv_ref.shape[1] // step, quad, 0)
    d_emb = SHRINK * (ALPHA * full(dres_ref) + dot_nt(full(dqkv_ref), full(wqkv_ref)))
    demb_ref[...] = d_emb
    dall_ref[...] = d_emb


def whole(shape):
    return pl.BlockSpec(shape, lambda i: (0,) * len(shape), pipeline_mode=pl.Buffered(1))


def per_seq(shape, base=0):
    return pl.BlockSpec((None,) + tuple(shape), lambda i: (i + base,) + (0,) * len(shape))


def cost(flops, moved):
    return pl.CostEstimate(flops=flops, bytes_accessed=moved, transcendentals=0)


def params():
    return pltpu.CompilerParams(dimension_semantics=('arbitrary',), vmem_limit_bytes=VMEM_LIMIT)


TOKEN = (8, LANES)
ANYWHERE = pl.BlockSpec(memory_space=pl.ANY)


def token_spec():
    return pl.BlockSpec(TOKEN, lambda i: (0, 0))


def attn_forward(base, count, total, own, own_base, other, mask, weights, tables, previous, deps, head_dim):
    seq_len, width = own.shape[1:]
    wqkv = weights[0]
    heads = width // head_dim
    shapes = [((seq_len, width), BF16), ((seq_len, 3 * width), BF16), ((heads, seq_len * 3 // 2, HALF_Q), BF16), ((seq_len, width), BF16),
              ((seq_len, width), F32), ((seq_len, LANES), F32), ((seq_len, width), BF16)]
    operands = (own, other, mask) + tuple(weights) + tuple(tables)
    specs = [per_seq((seq_len, width), own_base), per_seq((seq_len, width)), per_seq((seq_len, LANES), base)] + [whole(item.shape) for item in operands[3:]]
    extra = tuple(previous) if previous is not None else ()
    specs += [ANYWHERE] * (len(extra) + len(deps))
    flops = count * (2 * seq_len * width * (wqkv.shape[1] + width) + 4 * heads * seq_len * seq_len * 64)
    return pl.pallas_call(
        functools.partial(attn_forward_kernel, head_dim, len(extra) + len(deps)),
        grid=(count,),
        in_specs=specs,
        out_specs=[per_seq(shape, base) for shape, _ in shapes] + [token_spec()],
        out_shape=[jax.ShapeDtypeStruct((total,) + shape, dtype) for shape, dtype in shapes] + [jax.ShapeDtypeStruct(TOKEN, F32)],
        input_output_aliases={len(operands) + num: num for num in range(len(extra))},
        compiler_params=params(),
        cost_estimate=cost(2 * flops, count * 12_000_000),
        name='attn_forward',
    )(*operands, *extra, *deps)


def ffn(base, count, hidden, cotangent, half_index, hat, rstd, weights, previous, deps):
    total, seq_len, width = hidden.shape
    wide = weights[0].shape[1]
    operands = (hidden, cotangent, hat, rstd) + tuple(weights)
    extra = tuple(previous) if previous is not None else ()

    def seq_block(lanes, shift=0):
        return pl.BlockSpec((None, seq_len, lanes), lambda i, half: (i + base + half[0] * shift, 0, 0))

    def fixed(shape, **kwargs):
        return pl.BlockSpec(shape, lambda i, half: (0, 0), **kwargs)

    specs = [seq_block(width), seq_block(width, total), seq_block(width), seq_block(LANES)]
    specs += [fixed(item.shape, pipeline_mode=pl.Buffered(1)) for item in weights] + [ANYWHERE] * (len(extra) + len(deps))
    big = jax.ShapeDtypeStruct((total * seq_len, wide), BF16)
    narrow = jax.ShapeDtypeStruct((total, seq_len, width), BF16)
    sums = ((5 * TILE, width), (2 * TILE, wide), TOKEN)
    grid_spec = pltpu.PrefetchScalarGridSpec(
        num_scalar_prefetch=1,
        grid=(count,),
        in_specs=specs,
        out_specs=[ANYWHERE] * 3 + [seq_block(width)] * 3 + [fixed(shape) for shape in sums],
        scratch_shapes=[pltpu.VMEM((seq_len, wide), F32)] * 2 + [pltpu.VMEM((seq_len, wide), BF16)] * 3
        + [pltpu.VMEM((seq_len, width), F32), pltpu.SemaphoreType.DMA((3, wide // FFN_CHUNK))])
    return pl.pallas_call(
        functools.partial(ffn_kernel, base),
        grid_spec=grid_spec,
        out_shape=[big] * 3 + [narrow, jax.ShapeDtypeStruct((total, seq_len, width), F32), narrow] + [jax.ShapeDtypeStruct(shape, F32) for shape in sums],
        input_output_aliases={1 + len(operands) + num: num for num in range(len(extra))},
        compiler_params=params(),
        cost_estimate=cost(18 * count * seq_len * width * wide, count * 14_000_000),
        name='ffn',
    )(half_index, *operands, *extra, *deps)


def attn_backward(base, count, total, d_resid, d_attn, qkv, probs, weights, tables, previous, deps, head_dim):
    seq_len, width = d_resid.shape[1:]
    wqkv, wout = weights
    heads = width // head_dim
    operands = (d_resid, d_attn, qkv, probs, wqkv, wout) + tuple(tables)
    specs = [per_seq(item.shape[1:], base) for item in operands[:4]] + [whole(item.shape) for item in operands[4:]]
    extra = tuple(previous) if previous is not None else ()
    specs += [ANYWHERE] * (len(extra) + len(deps))
    flops = count * (2 * seq_len * width * (wqkv.shape[1] + width) + 8 * heads * seq_len * seq_len * 64)
    return pl.pallas_call(
        functools.partial(attn_backward_kernel, head_dim, len(extra) + len(deps)),
        grid=(count,),
        in_specs=specs,
        out_specs=[per_seq((seq_len, width)), per_seq((seq_len, wqkv.shape[1]), base), per_seq((seq_len, width), base), pl.BlockSpec((8, wqkv.shape[1]), lambda i: (0, 0)), token_spec()],
        out_shape=[jax.ShapeDtypeStruct((count, seq_len, width), F32), jax.ShapeDtypeStruct((total, seq_len, wqkv.shape[1]), BF16),
                   jax.ShapeDtypeStruct((total, seq_len, width), F32),
                   jax.ShapeDtypeStruct((8, wqkv.shape[1]), F32), jax.ShapeDtypeStruct(TOKEN, F32)],
        input_output_aliases={len(operands) + num: 1 + num for num in range(len(extra))},
        compiler_params=params(),
        cost_estimate=cost(2 * flops, count * 12_000_000),
        name='attn_backward',
    )(*operands, *extra, *deps)


def outer_kernel(left_ref, right_ref, *refs):
    out_ref, token_ref, left_t = refs[-3:]
    clear(token_ref)

    @pl.when(pl.program_id(0) == 0)
    def _():
        def turn(index, carry):
            rows = pl.ds(pl.multiple_of(index * CHUNK, CHUNK), CHUNK)
            left_t[:, rows] = left_ref[rows, :].astype(F32).T.astype(BF16)
            return carry

        lax.fori_loop(0, left_ref.shape[0] // CHUNK, turn, 0)

    out_ref[...] = dot_nn(full(left_t), full(right_ref))


def outer(left, right, block, shape, slot, previous, deps):
    rows, width = left.shape
    wide = right.shape[1]
    per_half = wide // (2 * block)
    half_blocks = shape[1] // (2 * block)
    extra = (previous,) if previous is not None else ()
    return pl.pallas_call(
        outer_kernel,
        grid=(wide // block,),
        in_specs=[whole((rows, width)), pl.BlockSpec((rows, block), lambda i: (0, i))] + [ANYWHERE] * (len(extra) + len(deps)),
        out_specs=[pl.BlockSpec((width, block), lambda i: (0, slot + i % per_half + half_blocks * (i // per_half))), token_spec()],
        out_shape=[jax.ShapeDtypeStruct(shape, F32), jax.ShapeDtypeStruct(TOKEN, F32)],
        input_output_aliases={2 + num: num for num in range(len(extra))},
        scratch_shapes=[pltpu.VMEM((width, rows), BF16)],
        compiler_params=params(),
        cost_estimate=cost(2 * rows * width * wide, 4 * width * wide + 2 * rows * (width + wide)),
        name='outer',
    )(left, right, *extra, *deps)


def groups_of(start, stop, size):
    return [(base, size) for base in range(start, stop, size)]


def join_kernel(plain, peer_ref, *refs):
    owns, outs = refs[:len(refs) // 2], refs[len(refs) // 2:]
    start = 0
    for num, (own_ref, out_ref) in enumerate(zip(owns, outs)):
        half = out_ref.shape[1] // 2
        out_ref[:, :half] = full(own_ref) if num < plain else full(own_ref).astype(F32).T.astype(BF16)
        out_ref[:, half:] = peer_ref[:, start:start + half].astype(BF16)
        start += half


def join(peer, plain, flipped):
    owns = tuple(plain) + tuple(flipped)
    rows = peer.shape[0]
    halves = [item.shape[1] for item in plain] + [item.shape[0] for item in flipped]
    return pl.pallas_call(
        functools.partial(join_kernel, len(plain)),
        grid=(rows // LANES,),
        in_specs=[pl.BlockSpec((LANES, peer.shape[1]), lambda i: (i, 0))] + [pl.BlockSpec((LANES, item.shape[1]), lambda i: (i, 0)) for item in plain]
        + [pl.BlockSpec((item.shape[0], LANES), lambda i: (0, i)) for item in flipped],
        out_specs=[pl.BlockSpec((LANES, 2 * half), lambda i: (i, 0)) for half in halves],
        out_shape=[jax.ShapeDtypeStruct((rows, 2 * half), BF16) for half in halves],
        compiler_params=params(),
        cost_estimate=cost(peer.size * 64, peer.size * 10),
        name='join_weights',
    )(peer, *owns)


def shared_slice(plain, flipped, index, parts):
    rows = plain[0].shape[0] // parts
    pieces = [lax.dynamic_slice_in_dim(item, index * rows, rows, 0) for item in plain]
    pieces += [lax.dynamic_slice_in_dim(item, index * rows, rows, 1).T for item in flipped]
    return jnp.concatenate(pieces, axis=1).astype(F32)


def row_pieces(rows):
    tiles = rows // TILE
    cuts = [num * tiles // PIECES * TILE for num in range(PIECES + 1)]
    return [(first, last - first) for first, last in zip(cuts, cuts[1:])]


def table_kernel(src, out, away, keep, got_one, got_two, stage, load_sems, store_sems, swap_sems, one_sems, two_sems, near_sems, far_sems, back_sems):
    me = lax.axis_index('dp')
    core, col, line = me % 2, me // 2 % 2, me // 4
    partner, x_peer, y_peer = me + 1 - 2 * core, me + 2 - 4 * col, me + 4 - 8 * line
    first_peer = x_peer + core * (y_peer - x_peer)
    second_peer = y_peer + core * (x_peer - y_peer)
    one = col + core * (line - col)
    two = line + core * (col - line)
    eighth = src.shape[0] // 8
    pieces = row_pieces(eighth)
    jobs = [(part, num) for part in range(4) for num in range(PIECES)]

    barrier = pltpu.get_barrier_semaphore()
    for peer in (partner, x_peer, y_peer):
        pl.semaphore_signal(barrier, inc=1, device_id={'dp': peer}, device_id_type=pl.DeviceIdType.MESH)
    pl.semaphore_wait(barrier, 3)

    def send(source, target, sems, slot, peer):
        return pltpu.make_async_remote_copy(src_ref=source, dst_ref=target, send_sem=sems.at[0, slot], recv_sem=sems.at[1, slot],
                                            device_id={'dp': peer}, device_id_type=pl.DeviceIdType.MESH)

    def table_rows(ref, half, quarter, last, num):
        start, size = pieces[num]
        return ref.at[pl.ds(pl.multiple_of((half * 4 + quarter * 2 + last) * eighth + start, TILE), size)]

    def part_rows(ref, half, quarter, last, part, num):
        return table_rows(ref, half, 1 - quarter if part < 2 else quarter, last if part % 2 else 1 - last, num)

    def buffer_rows(ref, part, num):
        start, size = pieces[num]
        return ref.at[pl.ds(part % 2 * eighth + start, size)]

    def holder(part):
        return away if part < 2 else keep

    def add_into(target, part, source, source_part, num):
        start, size = pieces[num]
        to, of = part % 2 * eighth + start, source_part * eighth + start

        def body(index, carry):
            offset = index * TILE
            target[pl.ds(pl.multiple_of(to + offset, TILE), TILE)] += source[pl.ds(pl.multiple_of(of + offset, TILE), TILE)]
            return carry

        lax.fori_loop(0, size // TILE, body, 0)

    swaps = [send(part_rows(src, 1 - core, two, one, part, num), buffer_rows(holder(part), part, num), swap_sems, slot, partner)
             for slot, (part, num) in enumerate(jobs)]
    loads = [pltpu.make_async_copy(part_rows(src, core, one, two, part, num), stage.at[slot % 2, pl.ds(0, pieces[num][1])], load_sems.at[slot % 2])
             for slot, (part, num) in enumerate(jobs)]
    firsts = [send(buffer_rows(away, part, num), buffer_rows(got_one, part, num), one_sems, slot, first_peer)
              for slot, (part, num) in enumerate(jobs[:2 * PIECES])]
    seconds = [send(buffer_rows(keep, 0, num), buffer_rows(got_two, 0, num), two_sems, num, second_peer) for num in range(PIECES)]

    for copy in swaps:
        copy.start()
    loads[0].start()
    for slot, (part, num) in enumerate(jobs):
        if slot + 1 < len(jobs):
            loads[slot + 1].start()
        loads[slot].wait()
        swaps[slot].wait_recv()
        start, size = pieces[num]
        target, held, to = holder(part), stage.at[slot % 2], part % 2 * eighth + start

        def body(index, carry, target=target, held=held, to=to):
            offset = index * TILE
            target[pl.ds(pl.multiple_of(to + offset, TILE), TILE)] += held[pl.ds(pl.multiple_of(offset, TILE), TILE)]
            return carry

        lax.fori_loop(0, size // TILE, body, 0)
        if 0 < slot <= len(firsts):
            firsts[slot - 1].start()

    for slot in range(2 * PIECES):
        firsts[slot].wait_recv()
        add_into(keep, slot // PIECES, got_one, slot // PIECES, slot % PIECES)
        if 0 < slot <= PIECES:
            seconds[slot - 1].start()

    done = []

    def publish(num):
        mine = buffer_rows(keep, 1, num)
        place = table_rows(out, core, one, two, num)
        copies = [pltpu.make_async_copy(mine, place, store_sems.at[num]), send(mine, place, near_sems, num, second_peer),
                  send(mine, place, far_sems, num, first_peer), send(mine, place, back_sems, num, partner)]
        for copy in copies:
            copy.start()
        done.append(copies)

    for num in range(PIECES):
        seconds[num].wait_recv()
        add_into(keep, 1, got_two, 0, num)
        if num:
            publish(num - 1)
    publish(PIECES - 1)

    def forward(quarter, last, num, sems, slot, peer, start=True):
        place = table_rows(out, core, quarter, last, num)
        copy = send(place, place, sems, slot, peer)
        if start:
            copy.start()
        return copy

    relays = []
    for num in range(PIECES):
        forward(one, 1 - two, num, near_sems, num, second_peer, False).wait_recv()
        relays.append(forward(one, 1 - two, num, far_sems, PIECES + num, first_peer))
        relays.append(forward(one, 1 - two, num, back_sems, PIECES + num, partner))
        forward(1 - one, two, num, far_sems, num, first_peer, False).wait_recv()
        relays.append(forward(1 - one, two, num, back_sems, 2 * PIECES + num, partner))
    for num in range(PIECES):
        forward(1 - one, 1 - two, num, far_sems, PIECES + num, first_peer, False).wait_recv()
        relays.append(forward(1 - one, 1 - two, num, back_sems, 3 * PIECES + num, partner))
    for slot, (part, num) in enumerate(jobs):
        place = table_rows(out, 1 - core, two if part < 2 else 1 - two, 1 - one if part % 2 else one, num)
        send(place, place, back_sems, slot, partner).wait_recv()
    for copy in swaps + firsts + seconds + relays:
        copy.wait_send()
    for local, *remote in done:
        local.wait()
        for copy in remote:
            copy.wait_send()


def reduce_table(table):
    rows, width = table.shape
    eighth = rows // 8
    largest = max(size for _, size in row_pieces(eighth))
    buffers = [pltpu.VMEM((count * eighth, width), F32) for count in (2, 2, 2, 1)]
    counts = (4 * PIECES, 2 * PIECES, PIECES, PIECES, 2 * PIECES, 4 * PIECES)
    return pl.pallas_call(
        table_kernel,
        in_specs=[ANYWHERE],
        out_specs=ANYWHERE,
        out_shape=jax.ShapeDtypeStruct(table.shape, F32),
        scratch_shapes=buffers + [pltpu.VMEM((2, largest, width), F32), pltpu.SemaphoreType.DMA((2,)), pltpu.SemaphoreType.DMA((PIECES,))]
        + [pltpu.SemaphoreType.DMA((2, count)) for count in counts],
        compiler_params=pltpu.CompilerParams(collective_id=0, has_side_effects=True, vmem_limit_bytes=VMEM_LIMIT),
        cost_estimate=cost(400_000_000_000, rows * width * 8),
        name='reduce_table',
    )(table)


def reduce_gradient(grad):
    piece = lax.psum_scatter(grad, 'dp', scatter_dimension=0, tiled=True)
    half = piece.shape[1] // 2
    other = lax.ppermute(piece[:, half:], 'tp', SWAP)
    return lax.all_gather(piece[:, :half] + other, 'dp', axis=0, tiled=True)


def tie(value, token):
    return lax.optimization_barrier((value, token))[0]


def solution(mesh):
    in_specs = (P('dp'), P('dp'), ROWS) + WEIGHT_SPECS
    out_specs = (ROWS,) + WEIGHT_SPECS
    parts = mesh.shape['dp']

    def device_step(tokens, cotangent, emb_table, *weights):
        (w_qkv, b_qkv, w_out, b_out, ln1_gain, ln1_bias, w_gate, b_gate, w_lin, b_lin, w_down, b_down, ln2_gain) = weights
        tp_index, dp_index = lax.axis_index('tp'), lax.axis_index('dp')
        vocab_loc, width = emb_table.shape
        head_dim = b_qkv.shape[1] // 3
        seq_len = tokens.shape[1]
        total = tokens.shape[0] // 2

        local_ids = tokens - tp_index * vocab_loc
        in_shard = (local_ids >= 0) & (local_ids < vocab_loc)
        own_ids = lax.dynamic_slice_in_dim(local_ids, tp_index * total, total)
        own_in = lax.dynamic_slice_in_dim(in_shard, tp_index * total, total)
        peer_ids = lax.dynamic_slice_in_dim(local_ids, (1 - tp_index) * total, total)
        peer_in = lax.dynamic_slice_in_dim(in_shard, (1 - tp_index) * total, total)

        own_mask = jnp.broadcast_to(own_in.astype(F32)[:, :, None], own_in.shape + (LANES,))

        def rows_of(part, head):
            ids = jnp.concatenate([peer_ids[part], own_ids[part]])
            rows = jnp.take(emb_table, tie(jnp.clip(ids, 0, vocab_loc - 1), head), axis=0, mode='clip')
            return rows

        def exchange(value):
            return lax.ppermute(value, 'tp', SWAP)

        def collect(value):
            value = exchange(value)
            return lax.all_gather(value, 'dp', axis=0, tiled=True)

        def row_of(vector):
            return vector.astype(F32).reshape(1, -1)

        half = total // 2
        qkv_loc, wide_loc = b_qkv.size, b_gate.shape[0]
        groups = [(num, 1) for num in range(half)] + groups_of(half, total, 2)

        first_rows = rows_of(slice(half), tp_index)
        halves = (first_rows, rows_of(slice(half, total), first_rows))
        front_peer = collect(shared_slice((w_qkv,), (w_out,), dp_index, parts))
        own_bias = jnp.concatenate([row_of(b_qkv), row_of(b_gate), row_of(b_lin)], axis=1)
        biases = jnp.concatenate([own_bias, exchange(own_bias)])
        wide_peer = collect(shared_slice((w_gate, w_lin), (w_down,), dp_index, parts))

        def send_rows(base, count):
            return exchange(halves[base // half][base % half:base % half + count].astype(F32))

        arrived = [send_rows(*group) for group in groups[:half]]
        halves = (first_rows, tie(halves[1], arrived[0]))
        arrived += [send_rows(*group) for group in groups[half:]]
        bqkv_full = biases[:, :qkv_loc].reshape(1, -1)
        bgate_full = biases[:, qkv_loc:qkv_loc + wide_loc].reshape(1, -1)
        blin_full = biases[:, qkv_loc + wide_loc:].reshape(1, -1)
        wqkv_full, wout_full = join(front_peer, (w_qkv,), (w_out,))
        wide_full = join(wide_peer, (w_gate, w_lin), (w_down,))

        half_dim = head_dim // 2
        inv_freq = ROPE_BASE ** (-2.0 * jnp.arange(half_dim, dtype=F32) / head_dim)
        angles = jnp.arange(seq_len, dtype=F32)[:, None] * inv_freq[None, :]
        cos_half, sin_half = jnp.cos(angles), jnp.sin(angles)
        tables = (jnp.concatenate([cos_half] * 4, axis=1), jnp.concatenate([-sin_half, sin_half] * 2, axis=1))

        front = (wqkv_full, bqkv_full, wout_full, row_of(b_out), row_of(ln1_gain), row_of(ln1_bias))
        middle = tuple(wide_full) + (bgate_full, blin_full, row_of(b_down), row_of(ln1_gain), row_of(ln2_gain))
        saved, ffn_saved, d_kept, deps = None, None, None, ()
        narrow_parts, wide_parts, bias_parts, d_peer = [], [], [], []

        def run_attention(num):
            nonlocal saved, deps
            base, count = groups[num]
            out = attn_forward(base, count, total, halves[base // half], half + base % half, arrived[num], own_mask, front, tables, saved, deps, head_dim)
            *kept, token = out
            saved, deps = kept, (token,)

        def run_ffn(base, count):
            nonlocal ffn_saved, deps
            *_, hat, rstd, hidden = saved
            *kept, narrow, wide, token = ffn(base, count, hidden, cotangent, tp_index.reshape(1), hat, rstd, middle, ffn_saved, deps)
            ffn_saved, deps = kept, (token,)
            narrow_parts.append(narrow)
            wide_parts.append(wide)

        def run_backward(base, count):
            nonlocal d_kept, deps
            _, qkv, probs, *_ = saved
            *_, d_resid, d_attn = ffn_saved
            d_emb, d_qkv, d_all, bias_part, token = attn_backward(base, count, total, d_resid, d_attn, qkv, probs, (wqkv_full, wout_full), tables, d_kept, deps, head_dim)
            d_kept, deps = (d_qkv, d_all), (token,)
            bias_parts.append(bias_part)
            d_peer.append(exchange(d_emb))

        def run_outer(left, right, block, shape, slot, previous):
            nonlocal deps
            out, token = outer(left.reshape(-1, left.shape[-1]), right.reshape(-1, right.shape[-1]), block, shape, slot, previous, deps)
            deps = (token,)
            return out

        for num in range(half + 2):
            run_attention(num)
            if num % 2 and num < half:
                run_ffn(num - 1, 2)
        run_backward(0, half)
        run_ffn(half, half)
        inner, d_gate, d_lin, d_ffn, _, d_attn = ffn_saved
        emb, _, _, context, _, _, hidden = saved
        shape = (width, 6 * wide_loc)
        step = wide_loc // CHUNK
        grads = run_outer(hidden, d_gate, CHUNK, shape, 0, None)
        grads = run_outer(hidden, d_lin, CHUNK, shape, step, grads)
        grads = run_outer(d_ffn, inner, CHUNK, shape, 2 * step, grads)
        wide_grads = reduce_gradient(grads)
        for base, count in groups_of(half, total, 2):
            run_backward(base, count)
        block = w_out.shape[0]
        shape = (width + parts * TILE, 2 * (qkv_loc + block))
        d_qkv, d_all = d_kept
        grads = run_outer(d_attn, context, block, shape, qkv_loc // block, None)
        grads = run_outer(emb, d_qkv, block, shape, 0, grads)

        narrow = jnp.sum(sum(narrow_parts).reshape(5, 8, -1), axis=1).reshape(1, -1)
        d_bwide = jnp.sum(sum(wide_parts).reshape(2, 8, -1), axis=1).reshape(2, 2, -1)
        small = jnp.concatenate([jnp.sum(sum(bias_parts), axis=0).reshape(2, -1), d_bwide[0], d_bwide[1], jnp.concatenate([narrow] * 2)], axis=1)
        used = small.shape[1]
        small = jnp.pad(small, ((0, 0), (0, TILE * (qkv_loc + block) - used))).reshape(2, TILE, -1)
        grads = lax.dynamic_update_slice(grads, jnp.concatenate([small[0], small[1]], axis=1), (width, 0))
        front_grads = reduce_gradient(grads)

        own_row_ids = jnp.where(own_in, own_ids, vocab_loc)
        peer_row_ids = jnp.where(peer_in, peer_ids, vocab_loc)

        def add_rows(grad, ids, rows):
            return grad.at[ids.reshape(-1)].add(rows.reshape(-1, width), mode='drop')

        d_table = add_rows(jnp.zeros((vocab_loc, width), F32), tie(own_row_ids, *deps), d_all)
        d_table = add_rows(d_table, peer_row_ids, jnp.concatenate(d_peer, axis=0))
        d_table = reduce_table(d_table)

        small = front_grads[width:width + TILE].reshape(-1)
        d_b_qkv = small[:qkv_loc].reshape(b_qkv.shape)
        d_b_gate = small[qkv_loc:qkv_loc + wide_loc]
        d_b_lin = small[qkv_loc + wide_loc:qkv_loc + 2 * wide_loc]
        d_ln2_gain, d_b_down, d_ln1_bias, d_ln1_gain, d_b_out = small[qkv_loc + 2 * wide_loc:used].reshape(5, width)
        d_w_gate, d_w_lin, d_w_down = (wide_grads[:, num * wide_loc:(num + 1) * wide_loc] for num in range(3))
        d_w_qkv, d_w_out = front_grads[:width, :qkv_loc], front_grads[:width, qkv_loc:]
        return (d_table, d_w_qkv, d_b_qkv, d_w_out.T, d_b_out, d_ln1_gain, d_ln1_bias, d_w_gate, d_b_gate, d_w_lin, d_b_lin, d_w_down.T, d_b_down, d_ln2_gain)

    return jax.shard_map(device_step, mesh=mesh, in_specs=in_specs, out_specs=out_specs, check_vma=False)
```
